32 devices in a mesh: col: 4 (over z), row: 8 (over y, x, core).
Axes of the slice: x: 2, y: 2, z: 4, core: 2. Of those that a mesh axis runs over, the one named last changes fastest.
Arguments:
- vel_u: float32 [31, 512, 2048], P(None, 'row', 'col')
- vel_v: float32 [31, 512, 2048], P(None, 'row', 'col')
- temperature: float32 [31, 512, 2048], P(None, 'row', 'col')
- salinity: float32 [31, 512, 2048], P(None, 'row', 'col')
- sea_level: float32 [512, 2048], P('row', 'col')
- trans_u: float32 [512, 2048], P('row', 'col')
- trans_v: float32 [512, 2048], P('row', 'col')
- bathymetry: float32 [512, 2048], P('row', 'col')
- kmt_levels: int32 [512, 2048], P('row', 'col')
- tide_force: float32 [30, 2], replicated
Outputs:
- output 1: float32 [512, 2048], P('row', 'col')
- output 2: float32 [512, 2048], P('row', 'col')
- output 3: float32 [512, 2048], P('row', 'col')
- output 4: float32 [31, 512, 2048], P(None, 'row', 'col')
- output 5: float32 [31, 512, 2048], P(None, 'row', 'col')
- output 6: float32 [31, 512, 2048], P(None, 'row', 'col')
- output 7: float32 [31, 512, 2048], P(None, 'row', 'col')
All inputs are finite; a program needn't handle non-finite values.
Results may differ from the reference program's by a relative error of at most 0.001.
Values sent between devices are 32-bit elements.
A program may use at most 1 GiB of HBM per device.

```python
import jax
import jax.numpy as jnp
from jax import lax

LEVELS = 31
SUBCYCLES = 30
GRID_NY = 512
GRID_NX = 2048

GRAVITY = 1.0
GRID_DX = 1.0
TIME_STEP = 4.0
ALPHA_T = 0.02
BETA_S = 0.015
T_REF = 1.0
S_REF = 1.0
VISC_KV = 0.001
DIFF_KT = 0.0005


def pad_halo(field):
    wrapped = jnp.concatenate([field[..., -1:], field, field[..., :1]], axis=-1)
    walls = jnp.zeros_like(wrapped[..., :1, :])
    return jnp.concatenate([walls, wrapped, walls], axis=-2)


def level_mask(count, n_levels):
    levels = jnp.arange(n_levels, dtype=jnp.int32)[:, None, None]
    return (levels < count[None]).astype(jnp.float32)


def interface_coef(count, thick, kappa, n_levels):
    levels = jnp.arange(n_levels - 1, dtype=jnp.int32)[:, None, None]
    active = (levels + 1 < count[None]).astype(jnp.float32)
    safe = jnp.where(count > 0, thick, 1.0)
    return active * (TIME_STEP * kappa / (safe * safe))[None]


def column_solve(source, couple):
    edge = jnp.zeros_like(source[:1])
    upper = jnp.concatenate([couple, edge], axis=0)
    lower = jnp.concatenate([edge, couple], axis=0)
    diag = 1.0 + upper + lower

    def forward(carry, slab):
        gain_prev, part_prev = carry
        lower_k, diag_k, upper_k, source_k = slab
        pivot = diag_k - lower_k * gain_prev
        gain = upper_k / pivot
        part = (source_k + lower_k * part_prev) / pivot
        return (gain, part), (gain, part)

    start = (jnp.zeros_like(source[0]), jnp.zeros_like(source[0]))
    _, (gains, parts) = lax.scan(forward, start, (lower, diag, upper, source))

    def backward(below, slab):
        gain, part = slab
        here = part + gain * below
        return here, here

    _, profile = lax.scan(backward, jnp.zeros_like(source[0]), (gains, parts), reverse=True)
    return profile


def geometry(kmt_ext, depth_ext):
    kmt_cell = kmt_ext[1:-1, 1:-1]
    thick_ext = depth_ext / jnp.maximum(kmt_ext, 1).astype(jnp.float32)
    thick_cell = thick_ext[1:-1, 1:-1]
    return {"k_cell": kmt_cell, "k_u": jnp.minimum(kmt_cell, kmt_ext[1:-1, 2:]), "k_v": jnp.minimum(kmt_cell, kmt_ext[2:, 1:-1]), "dz_cell": thick_cell, "dz_u": 0.5 * (thick_cell + thick_ext[1:-1, 2:]), "dz_v": 0.5 * (thick_cell + thick_ext[2:, 1:-1])}


def surface_fields(layout):
    k_faces = jnp.stack([layout["k_u"], layout["k_v"]])
    face_depth = k_faces.astype(jnp.float32) * jnp.stack([layout["dz_u"], layout["dz_v"]])
    face_wet = (k_faces > 0).astype(jnp.float32)
    wet_cell = (layout["k_cell"] > 0).astype(jnp.float32)
    return face_depth, face_wet, wet_cell


def momentum_tend(u_ext, v_ext, p_ext):
    cen_u = 0.5 * (u_ext[:, 1:-1, :-1] + u_ext[:, 1:-1, 1:])
    corner_v = 0.5 * (v_ext[:, :-1, 1:-1] + v_ext[:, :-1, 2:])
    corner_u = 0.5 * (u_ext[:, :-1, 1:-1] + u_ext[:, 1:, 1:-1])
    flux_uu = cen_u * cen_u
    flux_vu = corner_v * corner_u
    tend_u = -(flux_uu[:, :, 1:] - flux_uu[:, :, :-1] + flux_vu[:, 1:, :] - flux_vu[:, :-1, :] + p_ext[:, 1:-1, 2:] - p_ext[:, 1:-1, 1:-1]) / GRID_DX
    cen_v = 0.5 * (v_ext[:, :-1, 1:-1] + v_ext[:, 1:, 1:-1])
    side_u = 0.5 * (u_ext[:, 1:-1, :-1] + u_ext[:, 2:, :-1])
    side_v = 0.5 * (v_ext[:, 1:-1, :-1] + v_ext[:, 1:-1, 1:])
    flux_vv = cen_v * cen_v
    flux_uv = side_u * side_v
    tend_v = -(flux_vv[:, 1:, :] - flux_vv[:, :-1, :] + flux_uv[:, :, 1:] - flux_uv[:, :, :-1] + p_ext[:, 2:, 1:-1] - p_ext[:, 1:-1, 1:-1]) / GRID_DX
    return tend_u, tend_v


def baroclinic_predict(vel_u, vel_v, temperature, salinity, layout, halo_fn):
    n_levels = vel_u.shape[0]
    mask_c = level_mask(layout["k_cell"], n_levels)
    mask_u = level_mask(layout["k_u"], n_levels)
    mask_v = level_mask(layout["k_v"], n_levels)
    vel_um = vel_u * mask_u
    vel_vm = vel_v * mask_v
    density = mask_c * (BETA_S * (salinity - S_REF) - ALPHA_T * (temperature - T_REF))
    pressure = GRAVITY * layout["dz_cell"] * (jnp.cumsum(density, axis=0) - 0.5 * density)
    cell_coef = interface_coef(layout["k_cell"], layout["dz_cell"], DIFF_KT, n_levels)
    temp_mix = column_solve(temperature * mask_c, cell_coef)
    salt_mix = column_solve(salinity * mask_c, cell_coef)
    edges = halo_fn(jnp.stack([vel_um, vel_vm, pressure, temp_mix, salt_mix]))
    tend_u, tend_v = momentum_tend(edges[0], edges[1], edges[2])
    u_star = column_solve(mask_u * (vel_um + TIME_STEP * tend_u), interface_coef(layout["k_u"], layout["dz_u"], VISC_KV, n_levels))
    v_star = column_solve(mask_v * (vel_vm + TIME_STEP * tend_v), interface_coef(layout["k_v"], layout["dz_v"], VISC_KV, n_levels))
    forcing = jnp.stack([jnp.sum(layout["dz_u"] * (u_star - vel_um), axis=0), jnp.sum(layout["dz_v"] * (v_star - vel_vm), axis=0)]) / TIME_STEP
    return u_star, v_star, forcing, edges[3:], (mask_c, mask_u, mask_v)


def barotropic(eta_start, trans_start, face_depth, face_wet, wet_cell, forcing, tide_force, halo_fn):
    n_sub = tide_force.shape[0]
    dt_sub = TIME_STEP / n_sub
    weight_norm = 6.0 / (n_sub * (n_sub + 1) * (n_sub + 2))

    def substep(step, carry):
        eta_now, trans_now, trans_avg = carry
        trans_ext = halo_fn(trans_now)
        divergence = (trans_now[0] - trans_ext[0, 1:-1, :-2] + trans_now[1] - trans_ext[1, :-2, 1:-1]) / GRID_DX
        eta_next = wet_cell * (eta_now - dt_sub * divergence)
        eta_ext = halo_fn(eta_next)
        slope = jnp.stack([eta_ext[1:-1, 2:] - eta_next, eta_ext[2:, 1:-1] - eta_next]) / GRID_DX
        tide_now = lax.dynamic_index_in_dim(tide_force, step, 0, keepdims=False)
        trans_next = face_wet * (trans_now + dt_sub * (face_depth * (tide_now[:, None, None] - GRAVITY * slope) + forcing))
        weight = weight_norm * ((step + 1) * (n_sub - step)).astype(jnp.float32)
        return eta_next, trans_next, trans_avg + weight * trans_next

    return lax.fori_loop(0, n_sub, substep, (eta_start, trans_start, jnp.zeros_like(trans_start)))


def correct_velocity(star, dz_face, depth_face, mean_trans, mask):
    safe = jnp.where(depth_face > 0, depth_face, 1.0)
    return mask * (star + ((mean_trans - jnp.sum(dz_face * star, axis=0)) / safe)[None])


def advect_tracers(tracer_ext, flow_ext, mask_c):
    flux_x = flow_ext[0, :, 1:-1, :-1] * (0.5 * (tracer_ext[..., 1:-1, :-1] + tracer_ext[..., 1:-1, 1:]))
    flux_y = flow_ext[1, :, :-1, 1:-1] * (0.5 * (tracer_ext[..., :-1, 1:-1] + tracer_ext[..., 1:, 1:-1]))
    divergence = (flux_x[..., 1:] - flux_x[..., :-1] + flux_y[..., 1:, :] - flux_y[..., :-1, :]) / GRID_DX
    return mask_c * (tracer_ext[..., 1:-1, 1:-1] - TIME_STEP * divergence)


def baroclinic_finish(u_star, v_star, trans_avg, face_depth, layout, tracer_ext, masks, halo_fn):
    mask_c, mask_u, mask_v = masks
    vel_uc = correct_velocity(u_star, layout["dz_u"], face_depth[0], trans_avg[0], mask_u)
    vel_vc = correct_velocity(v_star, layout["dz_v"], face_depth[1], trans_avg[1], mask_v)
    flows = halo_fn(jnp.stack([vel_uc, vel_vc]))
    tracers = advect_tracers(tracer_ext, flows, mask_c)
    return vel_uc, vel_vc, tracers[0], tracers[1]


def ocean_step(vel_u, vel_v, temperature, salinity, sea_level, trans_u, trans_v, bathymetry, kmt_levels, tide_force, halo_fn):
    layout = geometry(halo_fn(kmt_levels), halo_fn(bathymetry))
    u_star, v_star, forcing, tracer_ext, masks = baroclinic_predict(vel_u, vel_v, temperature, salinity, layout, halo_fn)
    face_depth, face_wet, wet_cell = surface_fields(layout)
    eta_new, trans_new, trans_avg = barotropic(wet_cell * sea_level, face_wet * jnp.stack([trans_u, trans_v]), face_depth, face_wet, wet_cell, forcing, tide_force, halo_fn)
    vel_uc, vel_vc, temp_new, salt_new = baroclinic_finish(u_star, v_star, trans_avg, face_depth, layout, tracer_ext, masks, halo_fn)
    return eta_new, trans_new[0], trans_new[1], vel_uc, vel_vc, temp_new, salt_new


def draw_levels(key):
    key_count, key_land = jax.random.split(key)
    counts = jax.random.randint(key_count, (GRID_NY, GRID_NX), (LEVELS + 2) // 3, LEVELS + 1)
    land = jax.random.randint(key_land, (GRID_NY, GRID_NX), 0, 12) == 0
    levels = jnp.where(land, 0, counts).astype(jnp.int32)
    return levels.at[0, 0].set(0).at[GRID_NY - 1, GRID_NX - 1].set(LEVELS)


def setup_inputs(seed: int = 0) -> dict:
    keys = jax.random.split(jax.random.key(seed), 10)
    shape_cube = (LEVELS, GRID_NY, GRID_NX)
    shape_plane = (GRID_NY, GRID_NX)
    depth_frac = jnp.arange(LEVELS, dtype=jnp.float32)[:, None, None] / LEVELS
    return {
        "vel_u": 0.1 * jax.random.normal(keys[0], shape_cube, jnp.float32),
        "vel_v": 0.1 * jax.random.normal(keys[1], shape_cube, jnp.float32),
        "temperature": 2.0 * (1.0 - depth_frac) + 0.5 * jax.random.normal(keys[2], shape_cube, jnp.float32),
        "salinity": 1.0 + depth_frac + 0.3 * jax.random.normal(keys[3], shape_cube, jnp.float32),
        "sea_level": 0.05 * jax.random.normal(keys[4], shape_plane, jnp.float32),
        "trans_u": 0.05 * jax.random.normal(keys[5], shape_plane, jnp.float32),
        "trans_v": 0.05 * jax.random.normal(keys[6], shape_plane, jnp.float32),
        "bathymetry": 0.6 + 0.8 * jax.random.uniform(keys[7], shape_plane, jnp.float32),
        "kmt_levels": draw_levels(keys[8]),
        "tide_force": 0.01 + 0.01 * jax.random.normal(keys[9], (SUBCYCLES, 2), jnp.float32),
    }


def reference(vel_u, vel_v, temperature, salinity, sea_level, trans_u, trans_v, bathymetry, kmt_levels, tide_force):
    return ocean_step(vel_u, vel_v, temperature, salinity, sea_level, trans_u, trans_v, bathymetry, kmt_levels, tide_force, pad_halo)
```

```python
import jax
import jax.numpy as jnp
from jax import lax
from jax.experimental import pallas as pl
from jax.experimental.pallas import tpu as pltpu
from jax.sharding import PartitionSpec as P

GRAVITY = 1.0
TIME_STEP = 4.0
ALPHA_T = 0.02
BETA_S = 0.015
T_REF = 1.0
S_REF = 1.0
VISC_KV = 0.001
DIFF_KT = 0.0005

LANES = 128
HALO = 32
PAD = 8
F32 = jnp.float32
NORTH, SOUTH, EAST, WEST = (1, 0), (-1, 0), (0, 1), (0, -1)
NORTH_EAST, NORTH_WEST, SOUTH_EAST, SOUTH_WEST = (1, 1), (1, -1), (-1, 1), (-1, -1)
COMPASS = (NORTH, SOUTH, EAST, WEST, NORTH_EAST, NORTH_WEST, SOUTH_EAST, SOUTH_WEST)
SLOT = 32
BLOCK = 16
CROSS_ROWS = 8
FLOW_ROWS = 8
SOLVE_ROWS = 32
SUB_ROWS = 16
BACK_ROWS = 8
MIB = 2**20


def kernels(mesh, levels, rows, cols, n_sub):
    n_cols, n_rows = mesh.shape["col"], mesh.shape["row"]
    tiles = cols // LANES
    ring = tiles + 1
    halo_tile = tiles
    ext_rows = rows + 2 * PAD
    flat_rows = rows + 2 * HALO + 2 * PAD
    core = PAD + HALO
    top = core + rows
    body_rows = pl.ds(PAD, rows)
    own = pl.ds(core, rows)
    dt_sub = TIME_STEP / n_sub
    weight_norm = 6.0 / (n_sub * (n_sub + 1) * (n_sub + 2))

    def lane_iota(n):
        return lax.broadcasted_iota(jnp.int32, (n, LANES), 1)

    def roll(x, shift):
        return pltpu.roll(x, shift, 1)

    def east(parts):
        last = lane_iota(parts[0].shape[0]) == LANES - 1
        moved = [roll(x, LANES - 1) for x in parts]
        return [jnp.where(last, moved[(c + 1) % ring], moved[c]) for c in range(ring)]

    def west(parts):
        first = lane_iota(parts[0].shape[0]) == 0
        moved = [roll(x, 1) for x in parts]
        return [jnp.where(first, moved[(c - 1) % ring], moved[c]) for c in range(ring)]

    def split(ref):
        return [ref.at[f] for f in range(ref.shape[0])]

    def scaled(factor, x):
        return x if factor == 1.0 else factor * x

    def blank():
        return jnp.zeros((rows, LANES), F32)

    def neighbour(way):
        d_row, d_col = way
        row = lax.rem(lax.axis_index("row") + (d_row + n_rows), n_rows)
        col = lax.rem(lax.axis_index("col") + (d_col + n_cols), n_cols)
        return {"row": row, "col": col}

    def remote(sems, *routes):
        sent, arrived = split(sems)
        return [
            pltpu.make_async_remote_copy(
                src_ref=src,
                dst_ref=dst,
                send_sem=sent.at[index],
                recv_sem=arrived.at[index],
                device_id=neighbour(way),
                device_id_type=pl.DeviceIdType.MESH,
            )
            for index, (src, dst, way) in enumerate(routes)
        ]

    def start_all(copies):
        for copy in copies:
            copy.start()

    def wait_all(copies):
        for copy in copies:
            copy.wait()

    def rim_pack(maps, pack_east, pack_west):
        slot = lane_iota(rows) // HALO
        last, first = blank(), blank()
        for f, ref in enumerate(maps):
            last = jnp.where(slot == f, roll(ref[tiles - 1, own, :], (HALO * f + HALO) % LANES), last)
            first = jnp.where(slot == f, roll(ref[0, own, :], HALO * f), first)
        pack_east[...] = last
        pack_west[...] = first

    def rim_copies(main, pack_east, pack_west, from_west, from_east, sems):
        inner = pl.ds(0, tiles)
        low, high = pl.ds(core, HALO), pl.ds(top - HALO, HALO)
        p_low, p_all, p_high = pl.ds(0, HALO), pl.ds(0, rows), pl.ds(rows - HALO, HALO)
        d_low, d_all, d_high = pl.ds(0, HALO), pl.ds(HALO, rows), pl.ds(HALO + rows, HALO)
        every = pl.ds(0, main.shape[0])
        return remote(
            sems,
            (main.at[every, inner, high, :], main.at[every, inner, pl.ds(PAD, HALO), :], NORTH),
            (main.at[every, inner, low, :], main.at[every, inner, pl.ds(top, HALO), :], SOUTH),
            (pack_east.at[p_all, :], from_west.at[d_all, :], EAST),
            (pack_west.at[p_all, :], from_east.at[d_all, :], WEST),
            (pack_east.at[p_high, :], from_west.at[d_low, :], NORTH_EAST),
            (pack_west.at[p_high, :], from_east.at[d_low, :], NORTH_WEST),
            (pack_east.at[p_low, :], from_west.at[d_high, :], SOUTH_EAST),
            (pack_west.at[p_low, :], from_east.at[d_high, :], SOUTH_WEST),
        )

    def rim_unpack(maps, from_west, from_east):
        n = rows + 2 * HALO
        easterly = lane_iota(n) < LANES // 2
        for f, ref in enumerate(maps):
            e = roll(from_east[...], (LANES - HALO * f) % LANES)
            w = roll(from_west[...], LANES - HALO - HALO * f)
            ref[halo_tile, pl.ds(PAD, n), :] = jnp.where(easterly, e, w)

    def front(
        u_hbm, v_hbm, t_hbm, s_hbm, eta_hbm, tu_hbm, tv_hbm, depth_hbm, kmt_hbm, tide,
        us, vs, tm, sm, baro_out, corr, counts,
        u, v, p, gain_a, gain_b, cross, kmt_int, geo, thick, baro, force, coef, mean, depth_sum,
        pk_e, pk_w, rim_w, rim_e, first_col, last_col, first_row, last_row,
        col_e, col_w, row_n, row_s, corner_nw, corner_se,
        col_e4, col_w4, row_n4, row_s4, first_col4, last_col4, first_row4, last_row4,
        load_sems, plane_sems, sem1a, sem1b, sem2, sem3, sem4,
    ):
        k_map, depth_map = split(geo)
        eta_map, tu_map, tv_map = split(baro)
        dz_map, dzu_map, dzv_map = split(thick)
        k_out, ku_map, kv_map = split(counts)
        wet_map, hu_map, hv_map = split(coef)
        fu_map, fv_map = split(force)
        mu_map, mv_map = split(mean)
        su_map, sv_map = split(depth_sum)
        pk_e1, pk_e2, pk_e3 = split(pk_e)
        pk_w1, pk_w2, pk_w3 = split(pk_w)
        rim_e1, rim_e2, rim_e3 = split(rim_e)
        rim_w1, rim_w2, rim_w3 = split(rim_w)
        zero = blank()
        lane = lane_iota(rows)

        barrier = pltpu.get_barrier_semaphore()
        for way in COMPASS:
            pl.semaphore_signal(barrier, device_id=neighbour(way), device_id_type=pl.DeviceIdType.MESH)

        def plane_load(sems, src, dst):
            return [
                pltpu.make_async_copy(src.at[:, pl.ds(c * LANES, LANES)], dst(c), sems.at[c]) for c in range(tiles)
            ]

        def cube_load(sems, src, dst):
            return [
                pltpu.make_async_copy(
                    src.at[:, :, pl.ds(c * LANES, LANES)], dst.at[c, :, body_rows, :], sems.at[c]
                )
                for c in range(tiles)
            ]

        sem_k, sem_h, sem_e, sem_tu, sem_tv = split(plane_sems)
        sem_t, sem_s, sem_u, sem_v = split(load_sems)
        geo_load = plane_load(sem_k, kmt_hbm, lambda c: kmt_int.at[c]) + plane_load(
            sem_h, depth_hbm, lambda c: depth_map.at[c, own, :]
        )
        baro_load = (
            plane_load(sem_e, eta_hbm, lambda c: eta_map.at[c, own, :])
            + plane_load(sem_tu, tu_hbm, lambda c: tu_map.at[c, own, :])
            + plane_load(sem_tv, tv_hbm, lambda c: tv_map.at[c, own, :])
        )
        tracer_load = cube_load(sem_t, t_hbm, tm) + cube_load(sem_s, s_hbm, sm)
        flow_load = cube_load(sem_u, u_hbm, u) + cube_load(sem_v, v_hbm, v)
        start_all(geo_load + baro_load + tracer_load + flow_load)

        zero_rows = jnp.zeros((PAD, LANES), F32)
        for ref in (k_map, depth_map, dz_map, eta_map, tu_map, tv_map):
            for c in range(ring):
                ref[c, pl.ds(0, PAD), :] = zero_rows
                ref[c, pl.ds(flat_rows - PAD, PAD), :] = zero_rows
        for ref in (mu_map, mv_map):
            for c in range(ring):
                ref[c] = jnp.zeros((flat_rows, LANES), F32)

        wait_all(geo_load)
        for c in range(tiles):
            k_map[c, own, :] = kmt_int[c].astype(F32)
        rim_pack((k_map, depth_map), pk_e1, pk_w1)
        pl.semaphore_wait(barrier, len(COMPASS))
        ex1a = rim_copies(geo, pk_e1, pk_w1, rim_w1, rim_e1, sem1a)
        start_all(ex1a)
        wait_all(baro_load)
        rim_pack((eta_map, tu_map, tv_map), pk_e2, pk_w2)
        ex1b = rim_copies(baro, pk_e2, pk_w2, rim_w2, rim_e2, sem1b)
        start_all(ex1b)

        wait_all(tracer_load)
        rho_s, rho_t = 0.5 * BETA_S, 0.5 * ALPHA_T
        rho_0 = rho_t * T_REF - rho_s * S_REF

        def pressure_tile(c, _):
            k_cell = k_map[c, own, :]
            scale = (TIME_STEP * GRAVITY) * (depth_map[c, own, :] / jnp.maximum(k_cell, 1.0))

            def level(k, total):
                half = (rho_s * sm[c, k, body_rows, :] - rho_t * tm[c, k, body_rows, :]) + rho_0
                half = jnp.where(k.astype(F32) < k_cell, half, zero)
                middle = total + half
                p[c, k, body_rows, :] = scale * middle
                return middle + half

            lax.fori_loop(0, levels, level, zero)
            return _

        lax.fori_loop(0, tiles, pressure_tile, 0)

        def tracer_tile(c, _):
            k_cell = k_map[c, own, :]
            dz = depth_map[c, own, :] / jnp.maximum(k_cell, 1.0)
            safe = jnp.where(k_cell > 0, dz, 1.0)
            couple = (TIME_STEP * DIFF_KT) / (safe * safe)

            def down(k, carry):
                lower, keep, part_t, part_s = carry
                kf = k.astype(F32)
                wet = kf < k_cell
                upper = jnp.where(kf + 1.0 < k_cell, couple, zero)
                turn = 1.0 + lower * keep
                inv = 1.0 / (turn + upper)
                gain_a[k] = upper * inv
                part_t = (jnp.where(wet, tm[c, k, body_rows, :], zero) + lower * part_t) * inv
                part_s = (jnp.where(wet, sm[c, k, body_rows, :], zero) + lower * part_s) * inv
                tm[c, k, body_rows, :] = part_t
                sm[c, k, body_rows, :] = part_s
                return upper, turn * inv, part_t, part_s

            lax.fori_loop(0, levels, down, (zero, zero, zero, zero))

            def up(i, carry):
                below_t, below_s = carry
                k = levels - 1 - i
                gain = gain_a[k]
                below_t = tm[c, k, body_rows, :] + gain * below_t
                below_s = sm[c, k, body_rows, :] + gain * below_s
                tm[c, k, body_rows, :] = below_t
                sm[c, k, body_rows, :] = below_s
                return below_t, below_s

            lax.fori_loop(0, levels, up, (zero, zero))
            return _

        lax.fori_loop(0, tiles // 2, tracer_tile, 0)

        wait_all(ex1a)
        rim_unpack((k_map, depth_map), rim_w1, rim_e1)
        row_index = lax.axis_index("row")
        south_rim, north_rim = pl.ds(PAD, HALO), pl.ds(top, HALO)
        for inside, rim in ((row_index > 0, south_rim), (row_index < n_rows - 1, north_rim)):
            factor = jnp.where(inside, 1.0, 0.0).astype(F32)
            for c in range(ring):
                k_map[c, rim, :] = k_map[c, rim, :] * factor

        n_blocks = (rows + 2 * HALO) // BLOCK

        def block(i):
            return pl.multiple_of(PAD + BLOCK * i, PAD)

        def thickness(i, _):
            here = pl.ds(block(i), BLOCK)
            for c in range(ring):
                dz_map[c, here, :] = depth_map[c, here, :] / jnp.maximum(k_map[c, here, :], 1.0)
            return _

        lax.fori_loop(0, n_blocks, thickness, 0)

        def faces(i, _):
            here, north = pl.ds(block(i), BLOCK), pl.ds(block(i) + 1, BLOCK)
            k_cell = [k_map[c, here, :] for c in range(ring)]
            dz = [dz_map[c, here, :] for c in range(ring)]
            k_east, dz_east = east(k_cell), east(dz)
            for c in range(ring):
                k_u = jnp.minimum(k_cell[c], k_east[c])
                k_v = jnp.minimum(k_cell[c], k_map[c, north, :])
                dz_u = 0.5 * (dz[c] + dz_east[c])
                dz_v = 0.5 * (dz[c] + dz_map[c, north, :])
                k_out[c, here, :] = k_cell[c]
                ku_map[c, here, :] = k_u
                kv_map[c, here, :] = k_v
                dzu_map[c, here, :] = dz_u
                dzv_map[c, here, :] = dz_v
                wet_map[c, here, :] = jnp.where(k_cell[c] > 0, dt_sub, 0.0)
                hu_map[c, here, :] = dt_sub * (k_u * dz_u)
                hv_map[c, here, :] = dt_sub * (k_v * dz_v)
            return _

        lax.fori_loop(0, n_blocks, faces, 0)

        wait_all(flow_load)

        def mask_tile(c, _):
            for ref, count in ((u, ku_map), (v, kv_map)):
                k_face = count[c, own, :]

                def level(k, done, ref=ref, k_face=k_face):
                    ref[c, k, body_rows, :] = jnp.where(k.astype(F32) < k_face, ref[c, k, body_rows, :], zero)
                    return done

                lax.fori_loop(0, levels, level, 0)
            return _

        lax.fori_loop(0, tiles, mask_tile, 0)

        def edges(firsts, lasts, top_rows, bottom_rows):
            def level(k, carry):
                first, last = carry
                row = pl.ds(k, 1)
                for f, ref in firsts:
                    first = jnp.where(lane == SLOT * f + k, roll(ref[0, k, body_rows, :], SLOT * f + k), first)
                for f, ref in lasts:
                    x = roll(ref[tiles - 1, k, body_rows, :], SLOT * f + k + 1)
                    last = jnp.where(lane == SLOT * f + k, x, last)
                for c in range(tiles):
                    for ref, out in top_rows:
                        out[c, row, :] = ref[c, k, pl.ds(PAD, 1), :]
                    for ref, out in bottom_rows:
                        out[c, row, :] = ref[c, k, pl.ds(PAD + rows - 1, 1), :]
                return first, last

            return lax.fori_loop(0, levels, level, (zero, zero))

        fr_u, fr_v, fr_p = split(first_row)
        lr_u, lr_v = split(last_row)
        flows = ((0, u), (1, v))
        first, last = edges(
            flows + ((2, p),), flows, ((u, fr_u), (v, fr_v), (p, fr_p)), ((u, lr_u), (v, lr_v))
        )
        first_col[...] = first
        last_col[...] = last
        ex2 = remote(
            sem2,
            (first_col, col_e, WEST),
            (last_col, col_w, EAST),
            (first_row, row_n, SOUTH),
            (last_row, row_s, NORTH),
            (last_col.at[pl.ds(0, PAD), :], corner_nw, SOUTH_EAST),
            (first_col.at[pl.ds(rows - PAD, PAD), :], corner_se, NORTH_WEST),
        )
        start_all(ex2)

        wait_all(ex1b)
        rim_unpack((eta_map, tu_map, tv_map), rim_w2, rim_e2)

        def start_fields(i, _):
            here = pl.ds(block(i), BLOCK)
            for ref, count in ((eta_map, k_out), (tu_map, ku_map), (tv_map, kv_map)):
                for c in range(ring):
                    ref[c, here, :] = jnp.where(count[c, here, :] > 0, ref[c, here, :], 0.0)
            return _

        lax.fori_loop(0, n_blocks, start_fields, 0)
        wait_all(ex2)

        def fill(west_east, east_only, west_only, norths, souths):
            def level(k, _):
                here = (halo_tile, k, body_rows, slice(None))
                for ref, f, src_e, src_w in west_east:
                    e = roll(src_e[...], lax.rem(2 * LANES - SLOT * f - k, LANES))
                    w = roll(src_w[...], LANES - 1 - SLOT * f - k)
                    ref[here] = jnp.where(lane < LANES // 2, e, w)
                for ref, f, src in east_only:
                    ref[here] = roll(src[...], LANES - SLOT * f - k)
                for ref, f, src in west_only:
                    ref[here] = roll(src[...], LANES - 1 - SLOT * f - k)
                row = pl.ds(k, 1)
                for c in range(tiles):
                    for ref, src in norths:
                        ref[c, k, pl.ds(PAD + rows, 1), :] = src[c, row, :]
                    for ref, src in souths:
                        ref[c, k, pl.ds(PAD - 1, 1), :] = src[c, row, :]
                return _

            lax.fori_loop(0, levels, level, 0)

        rn_u, rn_v, rn_p = split(row_n)
        rs_u, rs_v = split(row_s)
        fill(
            ((u, 0, col_e, col_w), (v, 1, col_e, col_w)), ((p, 2, col_e),), (),
            ((u, rn_u), (v, rn_v), (p, rn_p)), ((u, rs_u), (v, rs_v)),
        )

        def corners(k, _):
            u[halo_tile, k, pl.ds(PAD + rows, PAD), :] = roll(corner_nw[...], LANES - 1 - k)
            v[halo_tile, k, pl.ds(0, PAD), :] = roll(corner_se[...], LANES - SLOT - k)
            return _

        lax.fori_loop(0, levels, corners, 0)

        quarter = 0.25 * TIME_STEP

        def momentum(k, _):
            for r in range(0, PAD + rows, CROSS_ROWS):
                here, north = pl.ds(r, CROSS_ROWS), pl.ds(r + 1, CROSS_ROWS)
                vv = [v[c, k, here, :] for c in range(ring)]
                v_east = east(vv)
                for c in range(ring):
                    cross[c, here, :] = (vv[c] + v_east[c]) * (u[c, k, here, :] + u[c, k, north, :])
            for r in range(PAD, PAD + rows, FLOW_ROWS):
                here, north, south = pl.ds(r, FLOW_ROWS), pl.ds(r + 1, FLOW_ROWS), pl.ds(r - 1, FLOW_ROWS)
                uu = [u[c, k, here, :] for c in range(ring)]
                square = [x + y for x, y in zip(uu, east(uu))]
                square = [x * x for x in square]
                square_west = west(square)
                xx = [cross[c, here, :] for c in range(ring)]
                x_west = west(xx)
                pp = [p[c, k, here, :] for c in range(ring)]
                p_east = east(pp)
                for c in range(tiles):
                    push = (square[c] - square_west[c]) + (xx[c] - cross[c, south, :])
                    us[c, k, here, :] = uu[c] - (scaled(quarter, push) + (p_east[c] - pp[c]))
                    vv = v[c, k, here, :]
                    b_here = vv + v[c, k, north, :]
                    b_south = vv + v[c, k, south, :]
                    push = (b_here * b_here - b_south * b_south) + (xx[c] - x_west[c])
                    vs[c, k, here, :] = vv - (scaled(quarter, push) + (p[c, k, north, :] - pp[c]))
            return _

        lax.fori_loop(0, levels, momentum, 0)

        nil = jnp.zeros((SOLVE_ROWS, LANES), F32)
        parts = rows // SOLVE_ROWS

        def solve_tile(i, _):
            c, r = i // parts, pl.multiple_of((i % parts) * SOLVE_ROWS, PAD)
            flat, here = pl.ds(core + r, SOLVE_ROWS), pl.ds(PAD + r, SOLVE_ROWS)
            faces = []
            for count, dz in ((ku_map, dzu_map), (kv_map, dzv_map)):
                k_face = count[c, flat, :]
                safe = jnp.where(k_face > 0, dz[c, flat, :], 1.0)
                faces.append((k_face, (TIME_STEP * VISC_KV) / (safe * safe)))

            def down(k, carry):
                kf = k.astype(F32)
                out = []
                for face, ref, gain, state in zip(faces, (us, vs), (gain_a, gain_b), carry):
                    k_face, couple = face
                    lower, keep, part = state
                    upper = jnp.where(kf + 1.0 < k_face, couple, nil)
                    turn = 1.0 + lower * keep
                    inv = 1.0 / (turn + upper)
                    gain[k, pl.ds(0, SOLVE_ROWS), :] = upper * inv
                    part = (jnp.where(kf < k_face, ref[c, k, here, :], nil) + lower * part) * inv
                    ref[c, k, here, :] = part
                    out.append((upper, turn * inv, part))
                return tuple(out)

            lax.fori_loop(0, levels, down, ((nil,) * 3,) * 2)

            def up(j, carry):
                k = levels - 1 - j
                out = []
                for ref, old, gain, state in zip((us, vs), (u, v), (gain_a, gain_b), carry):
                    below, total, change = state
                    below = ref[c, k, here, :] + gain[k, pl.ds(0, SOLVE_ROWS), :] * below
                    ref[c, k, here, :] = below
                    out.append((below, total + below, change + (below - old[c, k, here, :])))
                return tuple(out)

            sums = lax.fori_loop(0, levels, up, ((nil,) * 3,) * 2)
            for dz, total_map, force_map, state in zip((dzu_map, dzv_map), (su_map, sv_map), (fu_map, fv_map), sums):
                _, total, change = state
                total_map[c, flat, :] = dz[c, flat, :] * total
                force_map[c, flat, :] = dz[c, flat, :] * change * (1.0 / TIME_STEP)
            return i

        lax.fori_loop(0, tiles * parts, solve_tile, 0)

        rim_pack((fu_map, fv_map), pk_e3, pk_w3)
        ex3 = rim_copies(force, pk_e3, pk_w3, rim_w3, rim_e3, sem3)
        start_all(ex3)

        lax.fori_loop(tiles // 2, tiles, tracer_tile, 0)

        fr_t4, fr_s4 = split(first_row4)
        lr_v4, lr_t4, lr_s4 = split(last_row4)
        mixed = ((1, tm), (2, sm))
        first, last = edges(
            mixed, ((0, us),) + mixed, ((tm, fr_t4), (sm, fr_s4)), ((vs, lr_v4), (tm, lr_t4), (sm, lr_s4))
        )
        first_col4[...] = first
        last_col4[...] = jnp.where(lane == levels, roll(su_map[tiles - 1, own, :], levels + 1), last)
        for c in range(tiles):
            lr_v4[c, pl.ds(levels, 1), :] = sv_map[c, pl.ds(top - 1, 1), :]
        ex4 = remote(
            sem4,
            (first_col4, col_e4, WEST),
            (last_col4, col_w4, EAST),
            (first_row4, row_n4, SOUTH),
            (last_row4, row_s4, NORTH),
        )
        start_all(ex4)

        wait_all(ex3)
        rim_unpack((fu_map, fv_map), rim_w3, rim_e3)

        def force_fields(i, _):
            here = pl.ds(block(i), BLOCK)
            for ref, count in ((fu_map, ku_map), (fv_map, kv_map)):
                for c in range(ring):
                    ref[c, here, :] = jnp.where(count[c, here, :] > 0, dt_sub * ref[c, here, :], 0.0)
            return _

        lax.fori_loop(0, n_blocks, force_fields, 0)

        def subcycle(low, high):
            def body(n, _):
                tide_u, tide_v = tide[n, 0], tide[n, 1]
                weight = weight_norm * ((n + 1) * (n_sub - n)).astype(F32)
                for r in range(low, high, SUB_ROWS):
                    here, south = pl.ds(r, SUB_ROWS), pl.ds(r - 1, SUB_ROWS)
                    tu = [tu_map[c, here, :] for c in range(ring)]
                    tu_west = west(tu)
                    for c in range(ring):
                        spread = (tu[c] - tu_west[c]) + (tv_map[c, here, :] - tv_map[c, south, :])
                        eta_map[c, here, :] = eta_map[c, here, :] - wet_map[c, here, :] * spread
                for r in range(low, high, SUB_ROWS):
                    here, north = pl.ds(r, SUB_ROWS), pl.ds(r + 1, SUB_ROWS)
                    eta = [eta_map[c, here, :] for c in range(ring)]
                    eta_east = east(eta)
                    averaged = r + SUB_ROWS > core - 1 and r < top
                    for c in range(ring):
                        drive = hu_map[c, here, :] * (tide_u - scaled(GRAVITY, eta_east[c] - eta[c]))
                        tu = tu_map[c, here, :] + (drive + fu_map[c, here, :])
                        tu_map[c, here, :] = tu
                        drive = hv_map[c, here, :] * (tide_v - scaled(GRAVITY, eta_map[c, north, :] - eta[c]))
                        tv = tv_map[c, here, :] + (drive + fv_map[c, here, :])
                        tv_map[c, here, :] = tv
                        if averaged:
                            mu_map[c, here, :] = mu_map[c, here, :] + weight * tu
                            if c < tiles:
                                mv_map[c, here, :] = mv_map[c, here, :] + weight * tv
                return _

            return body

        begin, margin = 0, 0
        while begin < n_sub:
            end = n_sub if margin + PAD >= HALO else min(n_sub, n_sub - (HALO - margin - PAD))
            if end > begin:
                lax.fori_loop(begin, end, subcycle(PAD + margin, flat_rows - PAD - margin), 0)
                begin = end
            margin += PAD

        for ref, out in zip((eta_map, tu_map, tv_map), split(baro_out)):
            for c in range(tiles):
                out[c] = ref[c, own, :]

        wait_all(ex4)
        rn_t4, rn_s4 = split(row_n4)
        rs_v4, rs_t4, rs_s4 = split(row_s4)
        fill(
            ((tm, 1, col_e4, col_w4), (sm, 2, col_e4, col_w4)), (), ((us, 0, col_w4),),
            ((tm, rn_t4), (sm, rn_s4)), ((vs, rs_v4), (tm, rs_t4), (sm, rs_s4)),
        )
        su_map[halo_tile, own, :] = roll(col_w4[...], LANES - 1 - levels)
        for c in range(tiles):
            sv_map[c, pl.ds(core - 1, 1), :] = rs_v4[c, pl.ds(levels, 1), :]
        cu_map, cv_map = split(corr)
        for out, mean_map, total_map, count, dz, n, here in (
            (cu_map, mu_map, su_map, ku_map, dzu_map, ring, own),
            (cv_map, mv_map, sv_map, kv_map, dzv_map, tiles, pl.ds(core - PAD, rows + PAD)),
        ):
            for c in range(n):
                depth = count[c, here, :] * dz[c, here, :]
                safe = jnp.where(depth > 0, depth, 1.0)
                out[c, here, :] = (mean_map[c, here, :] - total_map[c, here, :]) / safe

    group = 4

    def back(us, vs, tm, sm, baro_in, corr, counts, eta_o, tu_o, tv_o, u_o, v_o, t_o, s_o, flux):
        k_map, ku_map, kv_map = split(counts)
        cu_map, cv_map = split(corr)
        fluxes = split(flux)
        for ref, out in zip(split(baro_in), (eta_o, tu_o, tv_o)):
            for c in range(tiles):
                out[:, pl.ds(c * LANES, LANES)] = ref[c]
        half = 0.5 * TIME_STEP

        def level(i, _):
            k = jnp.minimum(pl.program_id(0) * group + i, levels - 1)
            kf = k.astype(F32)
            for r in range(0, PAD + rows, BACK_ROWS):
                here, north = pl.ds(r, BACK_ROWS), pl.ds(r + 1, BACK_ROWS)
                flat = pl.ds(r + core - PAD, BACK_ROWS)
                for c in range(tiles):
                    vv = jnp.where(kf < kv_map[c, flat, :], vs[c, k, here, :] + cv_map[c, flat, :], 0.0)
                    if r >= PAD:
                        v_o[i, pl.ds(r - PAD, BACK_ROWS), pl.ds(c * LANES, LANES)] = vv
                    vv = half * vv
                    for ref, store in zip((tm, sm), fluxes):
                        store[c, here, :] = vv * (ref[c, k, here, :] + ref[c, k, north, :])
            for r in range(PAD, PAD + rows, BACK_ROWS):
                here, south = pl.ds(r, BACK_ROWS), pl.ds(r - 1, BACK_ROWS)
                flat = pl.ds(r - PAD + core, BACK_ROWS)
                out_rows = pl.ds(r - PAD, BACK_ROWS)
                uu = []
                for c in range(ring):
                    x = jnp.where(kf < ku_map[c, flat, :], us[c, k, here, :] + cu_map[c, flat, :], 0.0)
                    if c < tiles:
                        u_o[i, out_rows, pl.ds(c * LANES, LANES)] = x
                    uu.append(half * x)
                for ref, store, out in zip((tm, sm), fluxes, (t_o, s_o)):
                    tt = [ref[c, k, here, :] for c in range(ring)]
                    fx = [x * (y + z) for x, y, z in zip(uu, tt, east(tt))]
                    fx_west = west(fx)
                    for c in range(tiles):
                        spread = (fx[c] - fx_west[c]) + (store[c, here, :] - store[c, south, :])
                        new = jnp.where(kf < k_map[c, flat, :], tt[c] - spread, 0.0)
                        out[i, out_rows, pl.ds(c * LANES, LANES)] = new
            return _

        lax.fori_loop(0, group, level, 0)

    vmem = lambda *shape: pltpu.VMEM(shape, F32)
    flat = lambda n: vmem(n, ring, flat_rows, LANES)
    line = lambda n: vmem(n, tiles, SLOT, LANES)
    cube_buf = vmem(ring, levels, ext_rows, LANES)
    gain_buf = vmem(levels, rows, LANES)
    pack_buf = vmem(3, rows, LANES)
    rim_buf = vmem(3, rows + 2 * HALO, LANES)
    col_buf, corner_buf = vmem(rows, LANES), vmem(PAD, LANES)
    dma = lambda *shape: pltpu.SemaphoreType.DMA(shape)
    shared = [cube_buf, cube_buf, cube_buf, cube_buf, vmem(3, tiles, rows, LANES), flat(2), flat(3)]
    routes = len(COMPASS)
    any_spec = pl.BlockSpec(memory_space=pl.ANY)
    vmem_spec = pl.BlockSpec(memory_space=pltpu.VMEM)
    front_call = pl.pallas_call(
        front,
        name="front",
        out_shape=shared,
        in_specs=[any_spec] * 9 + [pl.BlockSpec(memory_space=pltpu.SMEM)],
        out_specs=[vmem_spec] * len(shared),
        scratch_shapes=[
            cube_buf, cube_buf, cube_buf, gain_buf, gain_buf,
            vmem(ring, ext_rows, LANES), pltpu.VMEM((tiles, rows, LANES), jnp.int32),
            flat(2), flat(3), flat(3), flat(2), flat(3), flat(2), flat(2),
            pack_buf, pack_buf, rim_buf, rim_buf,
            col_buf, col_buf, line(3), line(2),
            col_buf, col_buf, line(3), line(2), corner_buf, corner_buf,
            col_buf, col_buf, line(2), line(3),
            col_buf, col_buf, line(2), line(3),
            dma(4, tiles), dma(5, tiles), dma(2, routes), dma(2, routes), dma(2, routes), dma(2, routes), dma(2, routes),
        ],
        compiler_params=pltpu.CompilerParams(
            collective_id=0, has_side_effects=True, vmem_limit_bytes=31 * MIB
        ),
    )
    plane_out = pl.BlockSpec((rows, cols), lambda i: (0, 0))
    cube_out = pl.BlockSpec((group, rows, cols), lambda i: (i, 0, 0))
    plane_shape = jax.ShapeDtypeStruct((rows, cols), F32)
    cube_shape = jax.ShapeDtypeStruct((levels, rows, cols), F32)
    back_call = pl.pallas_call(
        back,
        name="back",
        grid=(pl.cdiv(levels, group),),
        out_shape=[plane_shape] * 3 + [cube_shape] * 4,
        in_specs=[vmem_spec] * len(shared),
        out_specs=[plane_out] * 3 + [cube_out] * 4,
        scratch_shapes=[vmem(2, tiles, ext_rows, LANES)],
        compiler_params=pltpu.CompilerParams(vmem_limit_bytes=8 * MIB),
    )
    return front_call, back_call


def solution(mesh):
    def local_step(vel_u, vel_v, temperature, salinity, sea_level, trans_u, trans_v, bathymetry, kmt_levels, tide_force):
        levels, rows, cols = vel_u.shape
        front_call, back_call = kernels(mesh, levels, rows, cols, tide_force.shape[0])
        shared = front_call(
            vel_u, vel_v, temperature, salinity, sea_level, trans_u, trans_v, bathymetry, kmt_levels, tide_force
        )
        return tuple(back_call(*shared))

    spec_cube = P(None, "row", "col")
    spec_plane = P("row", "col")
    return jax.shard_map(
        local_step,
        mesh=mesh,
        in_specs=(spec_cube,) * 4 + (spec_plane,) * 5 + (P(None, None),),
        out_specs=(spec_plane,) * 3 + (spec_cube,) * 4,
        check_vma=False,
    )
```

```python
import jax
import jax.numpy as jnp
from jax import lax
from jax.experimental import pallas as pl
from jax.experimental.pallas import tpu as pltpu
from jax.sharding import PartitionSpec as P

GRAVITY = 1.0
TIME_STEP = 4.0
ALPHA_T = 0.02
BETA_S = 0.015
T_REF = 1.0
S_REF = 1.0
VISC_KV = 0.001
DIFF_KT = 0.0005

LANES = 128
HALO = 32
PAD = 8
NEAR = 16
F32 = jnp.float32
NORTH, SOUTH, EAST, WEST = (1, 0), (-1, 0), (0, 1), (0, -1)
NORTH_EAST, NORTH_WEST, SOUTH_EAST, SOUTH_WEST = (1, 1), (1, -1), (-1, 1), (-1, -1)
COMPASS = (NORTH, SOUTH, EAST, WEST, NORTH_EAST, NORTH_WEST, SOUTH_EAST, SOUTH_WEST)
SLOT = 32
BLOCK = 16
CROSS_ROWS = 72
FLOW_ROWS = 64
SOLVE_ROWS = 32
SUB_ROWS = 16
BACK_ROWS = 16
MIB = 2**20


def kernels(mesh, levels, rows, cols, n_sub):
    n_cols, n_rows = mesh.shape["col"], mesh.shape["row"]
    tiles = cols // LANES
    ring = tiles + 1
    halo_tile = tiles
    ext_rows = rows + 2 * PAD
    flat_rows = rows + 2 * HALO + 2 * PAD
    core = PAD + HALO
    top = core + rows
    body_rows = pl.ds(PAD, rows)
    own = pl.ds(core, rows)
    dt_sub = TIME_STEP / n_sub
    weight_norm = 6.0 / (n_sub * (n_sub + 1) * (n_sub + 2))

    def lane_iota(n):
        return lax.broadcasted_iota(jnp.int32, (n, LANES), 1)

    def roll(x, shift):
        return pltpu.roll(x, shift, 1)

    def east(parts):
        last = lane_iota(parts[0].shape[0]) == LANES - 1
        moved = [roll(x, LANES - 1) for x in parts]
        return [jnp.where(last, moved[(c + 1) % ring], moved[c]) for c in range(ring)]

    def west(parts):
        first = lane_iota(parts[0].shape[0]) == 0
        moved = [roll(x, 1) for x in parts]
        return [jnp.where(first, moved[(c - 1) % ring], moved[c]) for c in range(ring)]

    def split(ref):
        return [ref.at[f] for f in range(ref.shape[0])]

    def scaled(factor, x):
        return x if factor == 1.0 else factor * x

    def blank():
        return jnp.zeros((rows, LANES), F32)

    def neighbour(way):
        d_row, d_col = way
        row = lax.rem(lax.axis_index("row") + (d_row + n_rows), n_rows)
        col = lax.rem(lax.axis_index("col") + (d_col + n_cols), n_cols)
        return {"row": row, "col": col}

    def remote(sems, *routes):
        sent, arrived = split(sems)
        return [
            pltpu.make_async_remote_copy(
                src_ref=src,
                dst_ref=dst,
                send_sem=sent.at[index],
                recv_sem=arrived.at[index],
                device_id=neighbour(way),
                device_id_type=pl.DeviceIdType.MESH,
            )
            for index, (src, dst, way) in enumerate(routes)
        ]

    def start_all(copies):
        for copy in copies:
            copy.start()

    def wait_all(copies):
        for copy in copies:
            copy.wait()

    def rim_pack(maps, pack_east, pack_west):
        slot = lane_iota(rows) // HALO
        last, first = blank(), blank()
        for f, ref in enumerate(maps):
            last = jnp.where(slot == f, roll(ref[tiles - 1, own, :], (HALO * f + HALO) % LANES), last)
            first = jnp.where(slot == f, roll(ref[0, own, :], HALO * f), first)
        pack_east[...] = last
        pack_west[...] = first

    def row_rims(main, sems, reach, skip=0):
        every, inner, n = pl.ds(0, main.shape[0]), pl.ds(0, tiles), reach - skip
        return remote(
            sems,
            (main.at[every, inner, pl.ds(top - reach, n), :], main.at[every, inner, pl.ds(core - reach, n), :], NORTH),
            (main.at[every, inner, pl.ds(core + skip, n), :], main.at[every, inner, pl.ds(top + skip, n), :], SOUTH),
        )

    def column_rims(pack_east, pack_west, from_west, from_east, sems):
        own_rows = pl.ds(HALO, rows)
        return remote(sems, (pack_east, from_west.at[own_rows, :], EAST), (pack_west, from_east.at[own_rows, :], WEST))

    def corner_rims(pack_east, pack_west, from_west, from_east, sems, reach, skip=0):
        n = reach - skip
        p_high, p_low = pl.ds(rows - reach, n), pl.ds(skip, n)
        d_low, d_high = pl.ds(HALO - reach, n), pl.ds(HALO + rows + skip, n)
        return remote(
            sems,
            (pack_east.at[p_high, :], from_west.at[d_low, :], NORTH_EAST),
            (pack_west.at[p_high, :], from_east.at[d_low, :], NORTH_WEST),
            (pack_east.at[p_low, :], from_west.at[d_high, :], SOUTH_EAST),
            (pack_west.at[p_low, :], from_east.at[d_high, :], SOUTH_WEST),
        )

    def rim_unpack(maps, from_west, from_east, start, n):
        easterly = lane_iota(n) < LANES // 2
        here = pl.ds(start - PAD, n)
        for f, ref in enumerate(maps):
            e = roll(from_east[here, :], (LANES - HALO * f) % LANES)
            w = roll(from_west[here, :], LANES - HALO - HALO * f)
            ref[halo_tile, pl.ds(start, n), :] = jnp.where(easterly, e, w)

    def front(
        u_hbm, v_hbm, t_hbm, s_hbm, eta_hbm, tu_hbm, tv_hbm, depth_hbm, kmt_hbm, tide_hbm,
        us, vs, tm, sm, baro_out, corr, counts,
        u, v, p, gain_a, gain_b, cross, kmt_int, geo, thick, baro, force, coef, mean, depth_sum,
        pk_e, pk_w, rim_w, rim_e, cols, cols_e, cols_w, cols_in, first_row, last_row,
        row_n, row_s, corner_nw, corner_se, first_row4, last_row4, row_n4, row_s4, tide,
        load_sems, plane_sems, tide_sem, sem_near, sem_far, sem_baro, sem_uvp, sem_ts, sem_force, sem_star,
    ):
        k_map, depth_map = split(geo)
        eta_map, tu_map, tv_map = split(baro)
        dz_map, dzu_map, dzv_map = split(thick)
        k_out, ku_map, kv_map = split(counts)
        wet_map, hu_map, hv_map = split(coef)
        fu_map, fv_map = split(force)
        mu_map, mv_map = split(mean)
        su_map, sv_map = split(depth_sum)
        pk_e1, pk_e2, pk_e3 = split(pk_e)
        pk_w1, pk_w2, pk_w3 = split(pk_w)
        rim_e1, rim_e2, rim_e3 = split(rim_e)
        rim_w1, rim_w2, rim_w3 = split(rim_w)
        zero = blank()
        lane = lane_iota(rows)

        barrier = pltpu.get_barrier_semaphore()
        for way in COMPASS:
            pl.semaphore_signal(barrier, device_id=neighbour(way), device_id_type=pl.DeviceIdType.MESH)

        def plane_load(sems, src, dst):
            return [
                pltpu.make_async_copy(src.at[:, pl.ds(c * LANES, LANES)], dst(c), sems.at[c]) for c in range(tiles)
            ]

        def cube_load(sems, src, dst):
            return [
                pltpu.make_async_copy(
                    src.at[:, :, pl.ds(c * LANES, LANES)], dst.at[c, :, body_rows, :], sems.at[c]
                )
                for c in range(tiles)
            ]

        sem_k, sem_h, sem_e, sem_tu, sem_tv = split(plane_sems)
        sem_t, sem_s, sem_u, sem_v = split(load_sems)
        geo_load = plane_load(sem_k, kmt_hbm, lambda c: kmt_int.at[c]) + plane_load(
            sem_h, depth_hbm, lambda c: depth_map.at[c, own, :]
        )
        baro_load = (
            plane_load(sem_e, eta_hbm, lambda c: eta_map.at[c, own, :])
            + plane_load(sem_tu, tu_hbm, lambda c: tu_map.at[c, own, :])
            + plane_load(sem_tv, tv_hbm, lambda c: tv_map.at[c, own, :])
        )
        tracer_load = cube_load(sem_t, t_hbm, tm) + cube_load(sem_s, s_hbm, sm)
        flow_load = cube_load(sem_u, u_hbm, u) + cube_load(sem_v, v_hbm, v)
        tide_load = pltpu.make_async_copy(tide_hbm, tide, tide_sem)
        start_all(geo_load)
        start_all(tracer_load)
        start_all(flow_load)
        start_all(baro_load)
        tide_load.start()

        zero_rows = jnp.zeros((PAD, LANES), F32)
        for ref in (k_map, depth_map, dz_map, eta_map, tu_map, tv_map):
            for c in range(ring):
                ref[c, pl.ds(0, PAD), :] = zero_rows
                ref[c, pl.ds(flat_rows - PAD, PAD), :] = zero_rows
        for ref in (mu_map, mv_map):
            for c in range(ring):
                ref[c] = jnp.zeros((flat_rows, LANES), F32)

        wait_all(geo_load)
        for c in range(tiles):
            k_map[c, own, :] = kmt_int[c].astype(F32)
        rim_pack((k_map, depth_map), pk_e1, pk_w1)
        pl.semaphore_wait(barrier, len(COMPASS))
        near_rows, near_cols, near_corners = split(sem_near)
        near = row_rims(geo, near_rows, NEAR)
        near += column_rims(pk_e1, pk_w1, rim_w1, rim_e1, near_cols)
        near += corner_rims(pk_e1, pk_w1, rim_w1, rim_e1, near_corners, NEAR)
        start_all(near)

        rho_s, rho_t = 0.5 * BETA_S, 0.5 * ALPHA_T
        rho_0 = rho_t * T_REF - rho_s * S_REF

        def pressure_tile(c, _):
            k_cell = k_map[c, own, :]
            scale = (TIME_STEP * GRAVITY) * (depth_map[c, own, :] / jnp.maximum(k_cell, 1.0))

            def level(k, total):
                half = (rho_s * sm[c, k, body_rows, :] - rho_t * tm[c, k, body_rows, :]) + rho_0
                half = jnp.where(k.astype(F32) < k_cell, half, zero)
                middle = total + half
                p[c, k, body_rows, :] = scale * middle
                return middle + half

            lax.fori_loop(0, levels, level, zero)
            return _

        for c in range(tiles):
            wait_all([tracer_load[c], tracer_load[tiles + c]])
            pressure_tile(c, 0)

        def edges(columns, top_rows, bottom_rows):
            def level(k, packed):
                row = pl.ds(k, 1)
                out = []
                for pair, acc in zip(columns, packed):
                    for f, ref in pair:
                        slot = SLOT * f + k
                        both = jnp.where(lane < LANES // 2, ref[0, k, body_rows, :], ref[tiles - 1, k, body_rows, :])
                        acc = jnp.where(lane // 2 == slot, roll(both, 2 * slot + 1), acc)
                    out.append(acc)
                for c in range(tiles):
                    for ref, dst in top_rows:
                        dst[c, row, :] = ref[c, k, pl.ds(PAD, 1), :]
                    for ref, dst in bottom_rows:
                        dst[c, row, :] = ref[c, k, pl.ds(PAD + rows - 1, 1), :]
                return tuple(out)

            return lax.fori_loop(0, levels, level, (zero,) * len(columns))

        wait_all(flow_load)
        cols_uv, cols_p, cols_ts, cols_us = split(cols)
        east_uv, east_p, east_ts = split(cols_e)
        west_uv, west_ts, west_us = split(cols_w)
        fr_u, fr_v, fr_p = split(first_row)
        lr_u, lr_v = split(last_row)
        cols_uv[...], cols_p[...] = edges(
            (((0, u), (1, v)), ((0, p),)), ((u, fr_u), (v, fr_v), (p, fr_p)), ((u, lr_u), (v, lr_v))
        )
        ex_uvp = remote(
            sem_uvp,
            (cols_uv, east_uv, WEST),
            (cols_p, east_p, WEST),
            (cols_uv, west_uv, EAST),
            (first_row, row_n, SOUTH),
            (last_row, row_s, NORTH),
            (cols_uv.at[pl.ds(0, PAD), :], corner_nw, SOUTH_EAST),
            (cols_uv.at[pl.ds(rows - PAD, PAD), :], corner_se, NORTH_WEST),
        )
        start_all(ex_uvp)

        wait_all(baro_load)
        rim_pack((eta_map, tu_map, tv_map), pk_e2, pk_w2)
        far_rows, far_corners = split(sem_far)
        baro_rows, baro_cols, baro_corners = split(sem_baro)
        far = row_rims(geo, far_rows, HALO, NEAR)
        far += corner_rims(pk_e1, pk_w1, rim_w1, rim_e1, far_corners, HALO, NEAR)
        far += row_rims(baro, baro_rows, HALO)
        far += column_rims(pk_e2, pk_w2, rim_w2, rim_e2, baro_cols)
        far += corner_rims(pk_e2, pk_w2, rim_w2, rim_e2, baro_corners, HALO)
        start_all(far)

        def tracer_tile(c, _):
            k_cell = k_map[c, own, :]
            dz = depth_map[c, own, :] / jnp.maximum(k_cell, 1.0)
            safe = jnp.where(k_cell > 0, dz, 1.0)
            couple = (TIME_STEP * DIFF_KT) / (safe * safe)

            def down(k, carry):
                lower, keep, part_t, part_s = carry
                kf = k.astype(F32)
                wet = kf < k_cell
                upper = jnp.where(kf + 1.0 < k_cell, couple, zero)
                turn = 1.0 + lower * keep
                inv = 1.0 / (turn + upper)
                gain_a[k] = upper * inv
                part_t = (jnp.where(wet, tm[c, k, body_rows, :], zero) + lower * part_t) * inv
                part_s = (jnp.where(wet, sm[c, k, body_rows, :], zero) + lower * part_s) * inv
                tm[c, k, body_rows, :] = part_t
                sm[c, k, body_rows, :] = part_s
                return upper, turn * inv, part_t, part_s

            lax.fori_loop(0, levels, down, (zero, zero, zero, zero))

            def up(i, carry):
                below_t, below_s = carry
                k = levels - 1 - i
                gain = gain_a[k]
                below_t = tm[c, k, body_rows, :] + gain * below_t
                below_s = sm[c, k, body_rows, :] + gain * below_s
                tm[c, k, body_rows, :] = below_t
                sm[c, k, body_rows, :] = below_s
                return below_t, below_s

            lax.fori_loop(0, levels, up, (zero, zero))
            return _

        lax.fori_loop(0, tiles, tracer_tile, 0)
        fr_t4, fr_s4 = split(first_row4)
        lr_t4, lr_s4, lr_v4 = split(last_row4)
        rn_t4, rn_s4 = split(row_n4)
        rs_t4, rs_s4, rs_v4 = split(row_s4)
        (packed,) = edges((((0, tm), (1, sm)),), ((tm, fr_t4), (sm, fr_s4)), ((tm, lr_t4), (sm, lr_s4)))
        cols_ts[...] = packed
        two = pl.ds(0, 2)
        ex_ts = remote(
            sem_ts,
            (cols_ts, east_ts, WEST),
            (cols_ts, west_ts, EAST),
            (first_row4, row_n4, SOUTH),
            (last_row4.at[two], row_s4.at[two], NORTH),
        )
        start_all(ex_ts)

        row_index = lax.axis_index("row")

        def wall(low, n, inside):
            @pl.when(jnp.logical_not(inside))
            def _():
                for c in range(ring):
                    k_map[c, pl.ds(low, n), :] = jnp.zeros((n, LANES), F32)

        def thickness(start, n):
            here = pl.ds(start, n)
            for c in range(ring):
                dz_map[c, here, :] = depth_map[c, here, :] / jnp.maximum(k_map[c, here, :], 1.0)

        def faces(start, n):
            here, north = pl.ds(start, n), pl.ds(start + 1, n)
            k_cell = [k_map[c, here, :] for c in range(ring)]
            dz = [dz_map[c, here, :] for c in range(ring)]
            k_east, dz_east = east(k_cell), east(dz)
            for c in range(ring):
                k_u = jnp.minimum(k_cell[c], k_east[c])
                k_v = jnp.minimum(k_cell[c], k_map[c, north, :])
                dz_u = 0.5 * (dz[c] + dz_east[c])
                dz_v = 0.5 * (dz[c] + dz_map[c, north, :])
                k_out[c, here, :] = k_cell[c]
                ku_map[c, here, :] = k_u
                kv_map[c, here, :] = k_v
                dzu_map[c, here, :] = dz_u
                dzv_map[c, here, :] = dz_v
                wet_map[c, here, :] = jnp.where(k_cell[c] > 0, dt_sub, 0.0)
                hu_map[c, here, :] = dt_sub * (k_u * dz_u)
                hv_map[c, here, :] = dt_sub * (k_v * dz_v)

        def in_blocks(work, start, n, size=BLOCK):
            lax.fori_loop(0, n // size, lambda i, _: (work(pl.multiple_of(start + size * i, PAD), size), _)[1], 0)

        far_low, far_high, far_n = PAD, top + NEAR, HALO - NEAR
        wait_all(near)
        rim_unpack((k_map, depth_map), rim_w1, rim_e1, core - NEAR, rows + 2 * NEAR)
        wall(core - NEAR, NEAR, row_index > 0)
        wall(top, NEAR, row_index < n_rows - 1)
        in_blocks(thickness, core - NEAR, rows + 2 * NEAR)
        in_blocks(faces, core - PAD, rows + 2 * PAD)

        def mask_tile(c, _):
            for ref, count in ((u, ku_map), (v, kv_map)):
                k_face = count[c, own, :]

                def level(k, done, ref=ref, k_face=k_face):
                    ref[c, k, body_rows, :] = jnp.where(k.astype(F32) < k_face, ref[c, k, body_rows, :], zero)
                    return done

                lax.fori_loop(0, levels, level, 0)
            return _

        lax.fori_loop(0, tiles, mask_tile, 0)

        def fill(columns, norths, souths):
            def masked(x, k, count, tile, here):
                return x if count is None else jnp.where(k.astype(F32) < count[tile, here, :], x, 0.0)

            def level(k, _):
                for ref, f, src, count in columns:
                    x = roll(src[...], LANES - 1 - 2 * (SLOT * f + k))
                    ref[halo_tile, k, body_rows, :] = masked(x, k, count, halo_tile, own)
                row = pl.ds(k, 1)
                for c in range(tiles):
                    for ref, src, count in norths:
                        x = masked(src[c, row, :], k, count, c, pl.ds(top, 1))
                        ref[c, k, pl.ds(PAD + rows, 1), :] = x
                    for ref, src, count in souths:
                        x = masked(src[c, row, :], k, count, c, pl.ds(core - 1, 1))
                        ref[c, k, pl.ds(PAD - 1, 1), :] = x
                return _

            lax.fori_loop(0, levels, level, 0)

        odd = lane % 2 == 1
        in_uv, in_ts = split(cols_in)
        wait_all(ex_uvp)
        in_uv[...] = jnp.where(odd, east_uv[...], west_uv[...])
        rn_u, rn_v, rn_p = split(row_n)
        rs_u, rs_v = split(row_s)
        fill(
            ((u, 0, in_uv, ku_map), (v, 1, in_uv, kv_map), (p, 0, east_p, None)),
            ((u, rn_u, ku_map), (v, rn_v, kv_map), (p, rn_p, None)),
            ((u, rs_u, ku_map), (v, rs_v, kv_map)),
        )

        def corners(k, _):
            kf = k.astype(F32)
            x = roll(corner_nw[...], LANES - 1 - 2 * k)
            u[halo_tile, k, pl.ds(PAD + rows, PAD), :] = jnp.where(kf < ku_map[halo_tile, pl.ds(top, PAD), :], x, 0.0)
            x = roll(corner_se[...], LANES - 1 - 2 * (SLOT + k))
            v[halo_tile, k, pl.ds(0, PAD), :] = jnp.where(kf < kv_map[halo_tile, pl.ds(core - PAD, PAD), :], x, 0.0)
            return _

        lax.fori_loop(0, levels, corners, 0)

        quarter = 0.25 * TIME_STEP

        def momentum(k, _):
            for r in range(0, PAD + rows, CROSS_ROWS):
                here, north = pl.ds(r, CROSS_ROWS), pl.ds(r + 1, CROSS_ROWS)
                vv = [v[c, k, here, :] for c in range(ring)]
                v_east = east(vv)
                for c in range(ring):
                    cross[c, here, :] = (vv[c] + v_east[c]) * (u[c, k, here, :] + u[c, k, north, :])
            for r in range(PAD, PAD + rows, FLOW_ROWS):
                here, north, south = pl.ds(r, FLOW_ROWS), pl.ds(r + 1, FLOW_ROWS), pl.ds(r - 1, FLOW_ROWS)
                uu = [u[c, k, here, :] for c in range(ring)]
                square = [x + y for x, y in zip(uu, east(uu))]
                square = [x * x for x in square]
                square_west = west(square)
                xx = [cross[c, here, :] for c in range(ring)]
                x_west = west(xx)
                pp = [p[c, k, here, :] for c in range(ring)]
                p_east = east(pp)
                for c in range(tiles):
                    push = (square[c] - square_west[c]) + (xx[c] - cross[c, south, :])
                    us[c, k, here, :] = uu[c] - (scaled(quarter, push) + (p_east[c] - pp[c]))
                    vv = v[c, k, here, :]
                    b_here = vv + v[c, k, north, :]
                    b_south = vv + v[c, k, south, :]
                    push = (b_here * b_here - b_south * b_south) + (xx[c] - x_west[c])
                    vs[c, k, here, :] = vv - (scaled(quarter, push) + (p[c, k, north, :] - pp[c]))
            return _

        lax.fori_loop(0, levels, momentum, 0)

        nil = jnp.zeros((SOLVE_ROWS, LANES), F32)
        parts = rows // SOLVE_ROWS

        def solve_part(c, i):
            r = pl.multiple_of(i * SOLVE_ROWS, PAD)
            flat, here = pl.ds(core + r, SOLVE_ROWS), pl.ds(PAD + r, SOLVE_ROWS)
            faces = []
            for count, dz in ((ku_map, dzu_map), (kv_map, dzv_map)):
                k_face = count[c, flat, :]
                safe = jnp.where(k_face > 0, dz[c, flat, :], 1.0)
                faces.append((k_face, (TIME_STEP * VISC_KV) / (safe * safe)))

            def down(k, carry):
                kf = k.astype(F32)
                out = []
                for face, ref, gain, state in zip(faces, (us, vs), (gain_a, gain_b), carry):
                    k_face, couple = face
                    lower, keep, part = state
                    upper = jnp.where(kf + 1.0 < k_face, couple, nil)
                    turn = 1.0 + lower * keep
                    inv = 1.0 / (turn + upper)
                    gain[k, pl.ds(0, SOLVE_ROWS), :] = upper * inv
                    part = (jnp.where(kf < k_face, ref[c, k, here, :], nil) + lower * part) * inv
                    ref[c, k, here, :] = part
                    out.append((upper, turn * inv, part))
                return tuple(out)

            lax.fori_loop(0, levels, down, ((nil,) * 3,) * 2)

            def up(j, carry):
                k = levels - 1 - j
                out = []
                for ref, old, gain, state in zip((us, vs), (u, v), (gain_a, gain_b), carry):
                    below, total, change = state
                    below = ref[c, k, here, :] + gain[k, pl.ds(0, SOLVE_ROWS), :] * below
                    ref[c, k, here, :] = below
                    out.append((below, total + below, change + (below - old[c, k, here, :])))
                return tuple(out)

            sums = lax.fori_loop(0, levels, up, ((nil,) * 3,) * 2)
            for dz, total_map, force_map, state in zip((dzu_map, dzv_map), (su_map, sv_map), (fu_map, fv_map), sums):
                _, total, change = state
                total_map[c, flat, :] = dz[c, flat, :] * total
                force_map[c, flat, :] = dz[c, flat, :] * change * (1.0 / TIME_STEP)

        force_rows, force_cols, force_corners = split(sem_force)
        ex3 = []
        for step, c in enumerate((0, tiles - 1) + tuple(range(1, tiles - 1))):
            lax.fori_loop(0, parts, lambda i, _: (solve_part(c, i), _)[1], 0)
            low, high, every = pl.ds(core, HALO), pl.ds(top - HALO, HALO), pl.ds(0, 2)
            sent = remote(
                force_rows.at[pl.ds(0, 2), pl.ds(2 * step, 2)],
                (force.at[every, c, high, :], force.at[every, c, pl.ds(PAD, HALO), :], NORTH),
                (force.at[every, c, low, :], force.at[every, c, pl.ds(top, HALO), :], SOUTH),
            )
            if step == 1:
                rim_pack((fu_map, fv_map), pk_e3, pk_w3)
                sent += column_rims(pk_e3, pk_w3, rim_w3, rim_e3, force_cols)
                sent += corner_rims(pk_e3, pk_w3, rim_w3, rim_e3, force_corners, HALO)
            start_all(sent)
            ex3 += sent

        (packed,) = edges((((0, us),),), (), ((vs, lr_v4),))
        cols_us[...] = jnp.where(lane // 2 == levels, roll(su_map[tiles - 1, own, :], 2 * levels + 1), packed)
        for c in range(tiles):
            lr_v4[c, pl.ds(levels, 1), :] = sv_map[c, pl.ds(top - 1, 1), :]
        ex_star = remote(sem_star, (cols_us, west_us, EAST), (lr_v4, rs_v4, NORTH))
        start_all(ex_star)

        wait_all(ex_ts)
        in_ts[...] = jnp.where(odd, east_ts[...], west_ts[...])
        fill(
            ((tm, 0, in_ts, None), (sm, 1, in_ts, None)),
            ((tm, rn_t4, None), (sm, rn_s4, None)),
            ((tm, rs_t4, None), (sm, rs_s4, None)),
        )

        wait_all(far)
        for start in (far_low, far_high):
            rim_unpack((k_map, depth_map), rim_w1, rim_e1, start, far_n)
        wall(far_low, far_n, row_index > 0)
        wall(far_high, far_n, row_index < n_rows - 1)
        in_blocks(thickness, far_low, far_n, PAD)
        in_blocks(thickness, far_high, far_n, PAD)
        in_blocks(faces, PAD, HALO - PAD, PAD)
        in_blocks(faces, top + PAD, HALO - PAD, PAD)
        full_n = rows + 2 * HALO
        rim_unpack((eta_map, tu_map, tv_map), rim_w2, rim_e2, PAD, full_n)

        def start_fields(start, n):
            here = pl.ds(start, n)
            for ref, count in ((eta_map, k_out), (tu_map, ku_map), (tv_map, kv_map)):
                for c in range(ring):
                    ref[c, here, :] = jnp.where(count[c, here, :] > 0, ref[c, here, :], 0.0)

        in_blocks(start_fields, PAD, full_n)
        tide_load.wait()

        wait_all(ex3)
        rim_unpack((fu_map, fv_map), rim_w3, rim_e3, PAD, full_n)

        def force_fields(start, n):
            here = pl.ds(start, n)
            for ref, count in ((fu_map, ku_map), (fv_map, kv_map)):
                for c in range(ring):
                    ref[c, here, :] = jnp.where(count[c, here, :] > 0, dt_sub * ref[c, here, :], 0.0)

        in_blocks(force_fields, PAD, full_n)

        def subcycle(low, high):
            def body(n, _):
                tide_u, tide_v = tide[n, 0], tide[n, 1]
                weight = weight_norm * ((n + 1) * (n_sub - n)).astype(F32)
                for r in range(low, high, SUB_ROWS):
                    here, south = pl.ds(r, SUB_ROWS), pl.ds(r - 1, SUB_ROWS)
                    tu = [tu_map[c, here, :] for c in range(ring)]
                    tu_west = west(tu)
                    for c in range(ring):
                        spread = (tu[c] - tu_west[c]) + (tv_map[c, here, :] - tv_map[c, south, :])
                        eta_map[c, here, :] = eta_map[c, here, :] - wet_map[c, here, :] * spread
                for r in range(low, high, SUB_ROWS):
                    here, north = pl.ds(r, SUB_ROWS), pl.ds(r + 1, SUB_ROWS)
                    eta = [eta_map[c, here, :] for c in range(ring)]
                    eta_east = east(eta)
                    averaged = r + SUB_ROWS > core - 1 and r < top
                    for c in range(ring):
                        drive = hu_map[c, here, :] * (tide_u - scaled(GRAVITY, eta_east[c] - eta[c]))
                        tu = tu_map[c, here, :] + (drive + fu_map[c, here, :])
                        tu_map[c, here, :] = tu
                        drive = hv_map[c, here, :] * (tide_v - scaled(GRAVITY, eta_map[c, north, :] - eta[c]))
                        tv = tv_map[c, here, :] + (drive + fv_map[c, here, :])
                        tv_map[c, here, :] = tv
                        if averaged:
                            mu_map[c, here, :] = mu_map[c, here, :] + weight * tu
                            if c < tiles:
                                mv_map[c, here, :] = mv_map[c, here, :] + weight * tv
                return _

            return body

        begin, margin = 0, 0
        while begin < n_sub:
            end = n_sub if margin + PAD >= HALO else min(n_sub, n_sub - (HALO - margin - PAD))
            if end > begin:
                lax.fori_loop(begin, end, subcycle(PAD + margin, flat_rows - PAD - margin), 0)
                begin = end
            margin += PAD

        for ref, out in zip((eta_map, tu_map, tv_map), split(baro_out)):
            for c in range(tiles):
                out[c] = ref[c, own, :]

        wait_all(ex_star)
        fill(((us, 0, west_us, None),), (), ((vs, rs_v4, None),))
        su_map[halo_tile, own, :] = roll(west_us[...], LANES - 1 - 2 * levels)
        for c in range(tiles):
            sv_map[c, pl.ds(core - 1, 1), :] = rs_v4[c, pl.ds(levels, 1), :]
        cu_map, cv_map = split(corr)
        for out, mean_map, total_map, count, dz, n, here in (
            (cu_map, mu_map, su_map, ku_map, dzu_map, ring, own),
            (cv_map, mv_map, sv_map, kv_map, dzv_map, tiles, pl.ds(core - PAD, rows + PAD)),
        ):
            for c in range(n):
                depth = count[c, here, :] * dz[c, here, :]
                safe = jnp.where(depth > 0, depth, 1.0)
                out[c, here, :] = (mean_map[c, here, :] - total_map[c, here, :]) / safe

    group = 4

    def back(us, vs, tm, sm, baro_in, corr, counts, eta_o, tu_o, tv_o, u_o, v_o, t_o, s_o, flux):
        k_map, ku_map, kv_map = split(counts)
        cu_map, cv_map = split(corr)
        fluxes = split(flux)
        for ref, out in zip(split(baro_in), (eta_o, tu_o, tv_o)):
            for c in range(tiles):
                out[:, pl.ds(c * LANES, LANES)] = ref[c]
        half = 0.5 * TIME_STEP

        def level(i, _):
            k = jnp.minimum(pl.program_id(0) * group + i, levels - 1)
            kf = k.astype(F32)
            for r in range(0, PAD + rows, PAD):
                here, north = pl.ds(r, PAD), pl.ds(r + 1, PAD)
                flat = pl.ds(r + core - PAD, PAD)
                for c in range(tiles):
                    vv = jnp.where(kf < kv_map[c, flat, :], vs[c, k, here, :] + cv_map[c, flat, :], 0.0)
                    if r >= PAD:
                        v_o[i, pl.ds(r - PAD, PAD), pl.ds(c * LANES, LANES)] = vv
                    vv = half * vv
                    for ref, store in zip((tm, sm), fluxes):
                        store[c, here, :] = vv * (ref[c, k, here, :] + ref[c, k, north, :])
            for r in range(PAD, PAD + rows, BACK_ROWS):
                here, south = pl.ds(r, BACK_ROWS), pl.ds(r - 1, BACK_ROWS)
                flat = pl.ds(r - PAD + core, BACK_ROWS)
                out_rows = pl.ds(r - PAD, BACK_ROWS)
                uu = []
                for c in range(ring):
                    x = jnp.where(kf < ku_map[c, flat, :], us[c, k, here, :] + cu_map[c, flat, :], 0.0)
                    if c < tiles:
                        u_o[i, out_rows, pl.ds(c * LANES, LANES)] = x
                    uu.append(half * x)
                for ref, store, out in zip((tm, sm), fluxes, (t_o, s_o)):
                    tt = [ref[c, k, here, :] for c in range(ring)]
                    fx = [x * (y + z) for x, y, z in zip(uu, tt, east(tt))]
                    fx_west = west(fx)
                    for c in range(tiles):
                        spread = (fx[c] - fx_west[c]) + (store[c, here, :] - store[c, south, :])
                        new = jnp.where(kf < k_map[c, flat, :], tt[c] - spread, 0.0)
                        out[i, out_rows, pl.ds(c * LANES, LANES)] = new
            return _

        lax.fori_loop(0, group, level, 0)

    vmem = lambda *shape: pltpu.VMEM(shape, F32)
    flat = lambda n: vmem(n, ring, flat_rows, LANES)
    line = lambda n: vmem(n, tiles, SLOT, LANES)
    cube_buf = vmem(ring, levels, ext_rows, LANES)
    gain_buf = vmem(levels, rows, LANES)
    pack_buf = vmem(3, rows, LANES)
    rim_buf = vmem(3, rows + 2 * HALO, LANES)
    col_buf, corner_buf = vmem(rows, LANES), vmem(PAD, LANES)
    dma = lambda *shape: pltpu.SemaphoreType.DMA(shape)
    shared = [cube_buf, cube_buf, cube_buf, cube_buf, vmem(3, tiles, rows, LANES), flat(2), flat(3)]
    routes = 7
    any_spec = pl.BlockSpec(memory_space=pl.ANY)
    vmem_spec = pl.BlockSpec(memory_space=pltpu.VMEM)
    front_call = pl.pallas_call(
        front,
        name="front",
        out_shape=shared,
        in_specs=[any_spec] * 10,
        out_specs=[vmem_spec] * len(shared),
        scratch_shapes=[
            cube_buf, cube_buf, cube_buf, gain_buf, gain_buf,
            vmem(ring, ext_rows, LANES), pltpu.VMEM((tiles, rows, LANES), jnp.int32),
            flat(2), flat(3), flat(3), flat(2), flat(3), flat(2), flat(2),
            pack_buf, pack_buf, rim_buf, rim_buf,
            vmem(4, rows, LANES), pack_buf, pack_buf, vmem(2, rows, LANES), line(3), line(2),
            line(3), line(2), corner_buf, corner_buf, line(2), line(3), line(2), line(3),
            pltpu.SMEM((n_sub, 2), F32),
            dma(4, tiles), dma(5, tiles), pltpu.SemaphoreType.DMA,
            dma(3, 2, 4), dma(2, 2, 4), dma(3, 2, 4), dma(2, routes), dma(2, 4), dma(3, 2, 2 * tiles), dma(2, 2),
        ],
        compiler_params=pltpu.CompilerParams(
            collective_id=0, has_side_effects=True, vmem_limit_bytes=31 * MIB
        ),
    )
    plane_out = pl.BlockSpec((rows, cols), lambda i: (0, 0))
    cube_out = pl.BlockSpec((group, rows, cols), lambda i: (i, 0, 0))
    plane_shape = jax.ShapeDtypeStruct((rows, cols), F32)
    cube_shape = jax.ShapeDtypeStruct((levels, rows, cols), F32)
    back_call = pl.pallas_call(
        back,
        name="back",
        grid=(pl.cdiv(levels, group),),
        out_shape=[plane_shape] * 3 + [cube_shape] * 4,
        in_specs=[vmem_spec] * len(shared),
        out_specs=[plane_out] * 3 + [cube_out] * 4,
        scratch_shapes=[vmem(2, tiles, ext_rows, LANES)],
        compiler_params=pltpu.CompilerParams(vmem_limit_bytes=8 * MIB),
    )
    return front_call, back_call


def solution(mesh):
    def local_step(vel_u, vel_v, temperature, salinity, sea_level, trans_u, trans_v, bathymetry, kmt_levels, tide_force):
        levels, rows, cols = vel_u.shape
        front_call, back_call = kernels(mesh, levels, rows, cols, tide_force.shape[0])
        shared = front_call(
            vel_u, vel_v, temperature, salinity, sea_level, trans_u, trans_v, bathymetry, kmt_levels, tide_force
        )
        return tuple(back_call(*shared))

    spec_cube = P(None, "row", "col")
    spec_plane = P("row", "col")
    return jax.shard_map(
        local_step,
        mesh=mesh,
        in_specs=(spec_cube,) * 4 + (spec_plane,) * 5 + (P(None, None),),
        out_specs=(spec_plane,) * 3 + (spec_cube,) * 4,
        check_vma=False,
    )
```

```python
import jax
import jax.numpy as jnp
from jax import lax
from jax.experimental import pallas as pl
from jax.experimental.pallas import tpu as pltpu
from jax.sharding import PartitionSpec as P

GRAVITY = 1.0
TIME_STEP = 4.0
ALPHA_T = 0.02
BETA_S = 0.015
T_REF = 1.0
S_REF = 1.0
VISC_KV = 0.001
DIFF_KT = 0.0005

LANES = 128
HALO = 32
PAD = 8
NEAR = 16
F32 = jnp.float32
NORTH, SOUTH, EAST, WEST = (1, 0), (-1, 0), (0, 1), (0, -1)
NORTH_EAST, NORTH_WEST, SOUTH_EAST, SOUTH_WEST = (1, 1), (1, -1), (-1, 1), (-1, -1)
COMPASS = (NORTH, SOUTH, EAST, WEST, NORTH_EAST, NORTH_WEST, SOUTH_EAST, SOUTH_WEST)
SLOT = 32
BLOCK = 16
SOLVE_ROWS = 32
SUB_ROWS = 32
BACK_ROWS = 16
UNROLL = 2
EDGE_UNROLL = 3
MIB = 2**20


def kernels(mesh, levels, rows, cols, n_sub):
    n_cols, n_rows = mesh.shape["col"], mesh.shape["row"]
    tiles = cols // LANES
    ring = tiles + 1
    halo_tile = tiles
    ext_rows = rows + 2 * PAD
    flat_rows = rows + 2 * HALO + 2 * PAD
    core = PAD + HALO
    top = core + rows
    body_rows = pl.ds(PAD, rows)
    own = pl.ds(core, rows)
    dt_sub = TIME_STEP / n_sub
    weight_norm = 6.0 / (n_sub * (n_sub + 1) * (n_sub + 2))

    def lane_iota(n):
        return lax.broadcasted_iota(jnp.int32, (n, LANES), 1)

    def roll(x, shift):
        return pltpu.roll(x, shift, 1)

    def east(parts):
        last = lane_iota(parts[0].shape[0]) == LANES - 1
        moved = [roll(x, LANES - 1) for x in parts]
        return [pick(last, moved[(c + 1) % ring], moved[c]) for c in range(ring)]

    def west(parts):
        first = lane_iota(parts[0].shape[0]) == 0
        moved = [roll(x, 1) for x in parts]
        return [pick(first, moved[(c - 1) % ring], moved[c]) for c in range(ring)]

    def split(ref):
        return [ref.at[f] for f in range(ref.shape[0])]

    def scaled(factor, x):
        return x if factor == 1.0 else factor * x

    def real(k):
        return float(k) if isinstance(k, int) else k.astype(F32)

    def over_levels(body, carry, unroll=UNROLL):
        def trip(i, carry):
            for j in range(unroll):
                carry = body(unroll * i + j, carry)
            return carry

        carry = lax.fori_loop(0, levels // unroll, trip, carry)
        for k in range(levels - levels % unroll, levels):
            carry = body(k, carry)
        return carry

    def pick(condition, x, other):
        if jnp.ndim(condition) == 0:
            return jnp.where(condition, x, other)
        shape = condition.shape
        x = x if jnp.ndim(x) else jnp.full(shape, x, F32)
        other = other if jnp.ndim(other) else jnp.full(shape, other, F32)
        return lax.select(condition, x, other)

    def blank():
        return jnp.zeros((rows, LANES), F32)

    def neighbour(way):
        d_row, d_col = way
        row = lax.rem(lax.axis_index("row") + (d_row + n_rows), n_rows)
        col = lax.rem(lax.axis_index("col") + (d_col + n_cols), n_cols)
        return {"row": row, "col": col}

    def remote(sems, *routes):
        sent, arrived = split(sems)
        return [
            pltpu.make_async_remote_copy(
                src_ref=src,
                dst_ref=dst,
                send_sem=sent.at[index],
                recv_sem=arrived.at[index],
                device_id=neighbour(way),
                device_id_type=pl.DeviceIdType.MESH,
            )
            for index, (src, dst, way) in enumerate(routes)
        ]

    def start_all(copies):
        for copy in copies:
            copy.start()

    def wait_all(copies):
        for copy in copies:
            copy.wait()

    def rim_pack(maps, pack_east, pack_west):
        slot = lane_iota(rows) // HALO
        last, first = blank(), blank()
        for f, ref in enumerate(maps):
            last = pick(slot == f, roll(ref[tiles - 1, own, :], (HALO * f + HALO) % LANES), last)
            first = pick(slot == f, roll(ref[0, own, :], HALO * f), first)
        pack_east[...] = last
        pack_west[...] = first

    def row_rims(main, sems, reach, skip=0):
        every, inner, n = pl.ds(0, main.shape[0]), pl.ds(0, tiles), reach - skip
        return remote(
            sems,
            (main.at[every, inner, pl.ds(top - reach, n), :], main.at[every, inner, pl.ds(core - reach, n), :], NORTH),
            (main.at[every, inner, pl.ds(core + skip, n), :], main.at[every, inner, pl.ds(top + skip, n), :], SOUTH),
        )

    def column_rims(pack_east, pack_west, from_west, from_east, sems):
        own_rows = pl.ds(HALO, rows)
        return remote(sems, (pack_east, from_west.at[own_rows, :], EAST), (pack_west, from_east.at[own_rows, :], WEST))

    def corner_rims(pack_east, pack_west, from_west, from_east, sems, reach, skip=0):
        n = reach - skip
        p_high, p_low = pl.ds(rows - reach, n), pl.ds(skip, n)
        d_low, d_high = pl.ds(HALO - reach, n), pl.ds(HALO + rows + skip, n)
        return remote(
            sems,
            (pack_east.at[p_high, :], from_west.at[d_low, :], NORTH_EAST),
            (pack_west.at[p_high, :], from_east.at[d_low, :], NORTH_WEST),
            (pack_east.at[p_low, :], from_west.at[d_high, :], SOUTH_EAST),
            (pack_west.at[p_low, :], from_east.at[d_high, :], SOUTH_WEST),
        )

    def rim_unpack(maps, from_west, from_east, start, n):
        easterly = lane_iota(n) < LANES // 2
        here = pl.ds(start - PAD, n)
        for f, ref in enumerate(maps):
            e = roll(from_east[here, :], (LANES - HALO * f) % LANES)
            w = roll(from_west[here, :], LANES - HALO - HALO * f)
            ref[halo_tile, pl.ds(start, n), :] = pick(easterly, e, w)

    def front(
        u_hbm, v_hbm, t_hbm, s_hbm, eta_hbm, tu_hbm, tv_hbm, depth_hbm, kmt_hbm, tide_hbm,
        us, vs, tm, sm, baro_out, corr, counts,
        u, v, p, gain_a, gain_b, cross, kmt_int, geo, thick, baro, force, coef, mean, depth_sum,
        pk_e, pk_w, rim_w, rim_e, cols, cols_e, cols_w, cols_in, first_row, last_row,
        row_n, row_s, corner_nw, corner_se, first_row4, last_row4, row_n4, row_s4, tide,
        load_sems, plane_sems, tide_sem, sem_near, sem_far, sem_baro, sem_uvp, sem_ts, sem_force, sem_star,
    ):
        k_map, depth_map = split(geo)
        eta_map, tu_map, tv_map = split(baro)
        dz_map, dzu_map, dzv_map = split(thick)
        k_out, ku_map, kv_map = split(counts)
        wet_map, hu_map, hv_map = split(coef)
        fu_map, fv_map = split(force)
        mu_map, mv_map = split(mean)
        su_map, sv_map = split(depth_sum)
        pk_e1, pk_e2, pk_e3 = split(pk_e)
        pk_w1, pk_w2, pk_w3 = split(pk_w)
        rim_e1, rim_e2, rim_e3 = split(rim_e)
        rim_w1, rim_w2, rim_w3 = split(rim_w)
        zero = blank()
        lane = lane_iota(rows)
        low_half = lane < LANES // 2
        pair_of_lane, odd = lane // 2, lane % 2 == 1

        barrier = pltpu.get_barrier_semaphore()
        for way in COMPASS:
            pl.semaphore_signal(barrier, device_id=neighbour(way), device_id_type=pl.DeviceIdType.MESH)

        def plane_load(sems, src, dst):
            return [
                pltpu.make_async_copy(src.at[:, pl.ds(c * LANES, LANES)], dst(c), sems.at[c]) for c in range(tiles)
            ]

        def cube_load(sems, src, dst):
            return [
                pltpu.make_async_copy(
                    src.at[:, :, pl.ds(c * LANES, LANES)], dst.at[c, :, body_rows, :], sems.at[c]
                )
                for c in range(tiles)
            ]

        sem_k, sem_h, sem_e, sem_tu, sem_tv = split(plane_sems)
        sem_t, sem_s, sem_u, sem_v = split(load_sems)
        geo_load = plane_load(sem_k, kmt_hbm, lambda c: kmt_int.at[c]) + plane_load(
            sem_h, depth_hbm, lambda c: depth_map.at[c, own, :]
        )
        baro_load = (
            plane_load(sem_e, eta_hbm, lambda c: eta_map.at[c, own, :])
            + plane_load(sem_tu, tu_hbm, lambda c: tu_map.at[c, own, :])
            + plane_load(sem_tv, tv_hbm, lambda c: tv_map.at[c, own, :])
        )
        tracer_load = cube_load(sem_t, t_hbm, tm) + cube_load(sem_s, s_hbm, sm)
        flow_load = cube_load(sem_u, u_hbm, u) + cube_load(sem_v, v_hbm, v)
        tide_load = pltpu.make_async_copy(tide_hbm, tide, tide_sem)
        start_all(geo_load)
        start_all(tracer_load)
        start_all(flow_load)
        start_all(baro_load)
        tide_load.start()

        zero_rows = jnp.zeros((PAD, LANES), F32)
        for ref in (k_map, depth_map, dz_map, eta_map, tu_map, tv_map):
            for c in range(ring):
                ref[c, pl.ds(0, PAD), :] = zero_rows
                ref[c, pl.ds(flat_rows - PAD, PAD), :] = zero_rows
        for ref in (mu_map, mv_map):
            for c in range(ring):
                ref[c] = jnp.zeros((flat_rows, LANES), F32)

        wait_all(geo_load)
        for c in range(tiles):
            k_map[c, own, :] = kmt_int[c].astype(F32)
        rim_pack((k_map, depth_map), pk_e1, pk_w1)
        pl.semaphore_wait(barrier, len(COMPASS))
        near_rows, near_cols, near_corners = split(sem_near)
        near = row_rims(geo, near_rows, NEAR)
        near += column_rims(pk_e1, pk_w1, rim_w1, rim_e1, near_cols)
        near += corner_rims(pk_e1, pk_w1, rim_w1, rim_e1, near_corners, NEAR)
        start_all(near)

        rho_s, rho_t = 0.5 * BETA_S, 0.5 * ALPHA_T
        rho_0 = rho_t * T_REF - rho_s * S_REF

        def pressure_tile(c, _):
            k_cell = k_map[c, own, :]
            scale = (TIME_STEP * GRAVITY) * (depth_map[c, own, :] / jnp.maximum(k_cell, 1.0))

            def level(k, total):
                half = (rho_s * sm[c, k, body_rows, :] - rho_t * tm[c, k, body_rows, :]) + rho_0
                half = pick(real(k) < k_cell, half, zero)
                middle = total + half
                p[c, k, body_rows, :] = scale * middle
                return middle + half

            over_levels(level, zero)
            return _

        wait_all(tracer_load)
        lax.fori_loop(0, tiles, pressure_tile, 0)

        def tracer_tile(c, _):
            k_cell = k_map[c, own, :]
            dz = depth_map[c, own, :] / jnp.maximum(k_cell, 1.0)
            safe = pick(k_cell > 0, dz, 1.0)
            couple = (TIME_STEP * DIFF_KT) / (safe * safe)

            def down(k, carry):
                lower, keep, part_t, part_s = carry
                kf = real(k)
                wet = kf < k_cell
                upper = pick(kf + 1.0 < k_cell, couple, zero)
                turn = 1.0 + lower * keep
                inv = 1.0 / (turn + upper)
                gain_a[k] = upper * inv
                part_t = (pick(wet, tm[c, k, body_rows, :], zero) + lower * part_t) * inv
                part_s = (pick(wet, sm[c, k, body_rows, :], zero) + lower * part_s) * inv
                tm[c, k, body_rows, :] = part_t
                sm[c, k, body_rows, :] = part_s
                return upper, turn * inv, part_t, part_s

            over_levels(down, (zero, zero, zero, zero))

            def up(i, carry):
                below_t, below_s = carry
                k = levels - 1 - i
                gain = gain_a[k]
                below_t = tm[c, k, body_rows, :] + gain * below_t
                below_s = sm[c, k, body_rows, :] + gain * below_s
                tm[c, k, body_rows, :] = below_t
                sm[c, k, body_rows, :] = below_s
                return below_t, below_s

            over_levels(up, (zero, zero))
            return _

        def edges(columns, top_rows, bottom_rows):
            def level(k, packed):
                row = pl.ds(k, 1)
                out = []
                for pair, acc in zip(columns, packed):
                    for f, ref in pair:
                        slot = SLOT * f + k
                        both = pick(low_half, ref[0, k, body_rows, :], ref[tiles - 1, k, body_rows, :])
                        acc = pick(pair_of_lane == slot, roll(both, 2 * slot + 1), acc)
                    out.append(acc)
                for c in range(tiles):
                    for ref, dst in top_rows:
                        dst[c, row, :] = ref[c, k, pl.ds(PAD, 1), :]
                    for ref, dst in bottom_rows:
                        dst[c, row, :] = ref[c, k, pl.ds(PAD + rows - 1, 1), :]
                return tuple(out)

            return over_levels(level, (zero,) * len(columns), EDGE_UNROLL)

        wait_all(flow_load)
        cols_uv, cols_p, cols_ts, cols_us = split(cols)
        east_uv, east_p, east_ts = split(cols_e)
        west_uv, west_ts, west_us = split(cols_w)
        fr_u, fr_v, fr_p = split(first_row)
        lr_u, lr_v = split(last_row)
        cols_uv[...], cols_p[...] = edges(
            (((0, u), (1, v)), ((0, p),)), ((u, fr_u), (v, fr_v), (p, fr_p)), ((u, lr_u), (v, lr_v))
        )
        ex_uvp = remote(
            sem_uvp,
            (cols_uv, east_uv, WEST),
            (cols_p, east_p, WEST),
            (cols_uv, west_uv, EAST),
            (first_row, row_n, SOUTH),
            (last_row, row_s, NORTH),
            (cols_uv.at[pl.ds(0, PAD), :], corner_nw, SOUTH_EAST),
            (cols_uv.at[pl.ds(rows - PAD, PAD), :], corner_se, NORTH_WEST),
        )
        start_all(ex_uvp)

        wait_all(baro_load)
        rim_pack((eta_map, tu_map, tv_map), pk_e2, pk_w2)
        far_rows, far_corners = split(sem_far)
        baro_rows, baro_cols, baro_corners = split(sem_baro)
        far = row_rims(geo, far_rows, HALO, NEAR)
        far += corner_rims(pk_e1, pk_w1, rim_w1, rim_e1, far_corners, HALO, NEAR)
        far += row_rims(baro, baro_rows, HALO)
        far += column_rims(pk_e2, pk_w2, rim_w2, rim_e2, baro_cols)
        far += corner_rims(pk_e2, pk_w2, rim_w2, rim_e2, baro_corners, HALO)
        start_all(far)

        lax.fori_loop(0, tiles, tracer_tile, 0)
        fr_t4, fr_s4 = split(first_row4)
        lr_t4, lr_s4, lr_v4 = split(last_row4)
        rn_t4, rn_s4 = split(row_n4)
        rs_t4, rs_s4, rs_v4 = split(row_s4)
        (packed,) = edges((((0, tm), (1, sm)),), ((tm, fr_t4), (sm, fr_s4)), ((tm, lr_t4), (sm, lr_s4)))
        cols_ts[...] = packed
        two = pl.ds(0, 2)
        ex_ts = remote(
            sem_ts,
            (cols_ts, east_ts, WEST),
            (cols_ts, west_ts, EAST),
            (first_row4, row_n4, SOUTH),
            (last_row4.at[two], row_s4.at[two], NORTH),
        )
        start_all(ex_ts)

        row_index = lax.axis_index("row")

        def wall(low, n, inside):
            @pl.when(jnp.logical_not(inside))
            def _():
                for c in range(ring):
                    k_map[c, pl.ds(low, n), :] = jnp.zeros((n, LANES), F32)

        def thickness(start, n):
            here = pl.ds(start, n)
            for c in range(ring):
                dz_map[c, here, :] = depth_map[c, here, :] / jnp.maximum(k_map[c, here, :], 1.0)

        def faces(start, n):
            here, north = pl.ds(start, n), pl.ds(start + 1, n)
            k_cell = [k_map[c, here, :] for c in range(ring)]
            dz = [dz_map[c, here, :] for c in range(ring)]
            k_east, dz_east = east(k_cell), east(dz)
            for c in range(ring):
                k_u = jnp.minimum(k_cell[c], k_east[c])
                k_v = jnp.minimum(k_cell[c], k_map[c, north, :])
                dz_u = 0.5 * (dz[c] + dz_east[c])
                dz_v = 0.5 * (dz[c] + dz_map[c, north, :])
                k_out[c, here, :] = k_cell[c]
                ku_map[c, here, :] = k_u
                kv_map[c, here, :] = k_v
                dzu_map[c, here, :] = dz_u
                dzv_map[c, here, :] = dz_v
                wet_map[c, here, :] = pick(k_cell[c] > 0, dt_sub, 0.0)
                hu_map[c, here, :] = dt_sub * (k_u * dz_u)
                hv_map[c, here, :] = dt_sub * (k_v * dz_v)

        def in_blocks(work, start, n, size=BLOCK):
            lax.fori_loop(0, n // size, lambda i, _: (work(pl.multiple_of(start + size * i, PAD), size), _)[1], 0)

        far_low, far_high, far_n = PAD, top + NEAR, HALO - NEAR
        wait_all(near)
        rim_unpack((k_map, depth_map), rim_w1, rim_e1, core - NEAR, rows + 2 * NEAR)
        wall(core - NEAR, NEAR, row_index > 0)
        wall(top, NEAR, row_index < n_rows - 1)
        in_blocks(thickness, core - NEAR, rows + 2 * NEAR)
        in_blocks(faces, core - PAD, rows + 2 * PAD)

        def mask_tile(c, _):
            for ref, count in ((u, ku_map), (v, kv_map)):
                k_face = count[c, own, :]

                def level(k, done, ref=ref, k_face=k_face):
                    ref[c, k, body_rows, :] = pick(real(k) < k_face, ref[c, k, body_rows, :], zero)
                    return done

                over_levels(level, 0)
            return _

        lax.fori_loop(0, tiles, mask_tile, 0)

        def fill(columns, norths, souths):
            def masked(x, k, count, tile, here):
                return x if count is None else pick(real(k) < count[tile, here, :], x, 0.0)

            def level(k, _):
                for ref, f, src, count in columns:
                    x = roll(src[...], LANES - 1 - 2 * (SLOT * f + k))
                    ref[halo_tile, k, body_rows, :] = masked(x, k, count, halo_tile, own)
                row = pl.ds(k, 1)
                for c in range(tiles):
                    for ref, src, count in norths:
                        x = masked(src[c, row, :], k, count, c, pl.ds(top, 1))
                        ref[c, k, pl.ds(PAD + rows, 1), :] = x
                    for ref, src, count in souths:
                        x = masked(src[c, row, :], k, count, c, pl.ds(core - 1, 1))
                        ref[c, k, pl.ds(PAD - 1, 1), :] = x
                return _

            over_levels(level, 0, EDGE_UNROLL)

        in_uv, in_ts = split(cols_in)
        wait_all(ex_uvp)
        in_uv[...] = pick(odd, east_uv[...], west_uv[...])
        rn_u, rn_v, rn_p = split(row_n)
        rs_u, rs_v = split(row_s)
        fill(
            ((u, 0, in_uv, ku_map), (v, 1, in_uv, kv_map), (p, 0, east_p, None)),
            ((u, rn_u, ku_map), (v, rn_v, kv_map), (p, rn_p, None)),
            ((u, rs_u, ku_map), (v, rs_v, kv_map)),
        )

        def corners(k, _):
            kf = real(k)
            x = roll(corner_nw[...], LANES - 1 - 2 * k)
            u[halo_tile, k, pl.ds(PAD + rows, PAD), :] = pick(kf < ku_map[halo_tile, pl.ds(top, PAD), :], x, 0.0)
            x = roll(corner_se[...], LANES - 1 - 2 * (SLOT + k))
            v[halo_tile, k, pl.ds(0, PAD), :] = pick(kf < kv_map[halo_tile, pl.ds(core - PAD, PAD), :], x, 0.0)
            return _

        over_levels(corners, 0, EDGE_UNROLL)

        quarter = 0.25 * TIME_STEP

        def momentum(k, _):
            tall, tall_north = pl.ds(0, PAD + rows), pl.ds(1, PAD + rows)
            here, north, south = body_rows, pl.ds(PAD + 1, rows), pl.ds(PAD - 1, rows)
            vv = [v[c, k, tall, :] for c in range(ring)]
            v_east = east(vv)
            for c in range(ring):
                cross[c, tall, :] = (vv[c] + v_east[c]) * (u[c, k, tall, :] + u[c, k, tall_north, :])
            uu = [u[c, k, here, :] for c in range(ring)]
            pp = [p[c, k, here, :] for c in range(ring)]
            centre = [x + y for x, y in zip(uu, west(uu))]
            centre = [scaled(quarter, x * x) + y for x, y in zip(centre, pp)]
            centre_east = east(centre)
            xx = [cross[c, here, :] for c in range(ring)]
            x_west = west(xx)
            for c in range(tiles):
                us[c, k, here, :] = uu[c] - (
                    (centre_east[c] - centre[c]) + scaled(quarter, xx[c] - cross[c, south, :])
                )
                vv = v[c, k, here, :]
                b_here = vv + v[c, k, north, :]
                b_south = vv + v[c, k, south, :]
                push = (b_here * b_here - b_south * b_south) + (xx[c] - x_west[c])
                vs[c, k, here, :] = vv - (scaled(quarter, push) + (p[c, k, north, :] - pp[c]))
            return _

        over_levels(momentum, 0)

        nil = jnp.zeros((SOLVE_ROWS, LANES), F32)
        parts = rows // SOLVE_ROWS

        def solve_part(c, i):
            r = pl.multiple_of(i * SOLVE_ROWS, PAD)
            flat, here = pl.ds(core + r, SOLVE_ROWS), pl.ds(PAD + r, SOLVE_ROWS)
            faces = []
            for count, dz in ((ku_map, dzu_map), (kv_map, dzv_map)):
                k_face = count[c, flat, :]
                safe = pick(k_face > 0, dz[c, flat, :], 1.0)
                faces.append((k_face, (TIME_STEP * VISC_KV) / (safe * safe)))

            def down(k, carry):
                kf = real(k)
                out = []
                for face, ref, gain, state in zip(faces, (us, vs), (gain_a, gain_b), carry):
                    k_face, couple = face
                    lower, keep, part = state
                    upper = pick(kf + 1.0 < k_face, couple, nil)
                    turn = 1.0 + lower * keep
                    inv = 1.0 / (turn + upper)
                    gain[k, pl.ds(0, SOLVE_ROWS), :] = upper * inv
                    part = (pick(kf < k_face, ref[c, k, here, :], nil) + lower * part) * inv
                    ref[c, k, here, :] = part
                    out.append((upper, turn * inv, part))
                return tuple(out)

            over_levels(down, ((nil,) * 3,) * 2)

            def up(j, carry):
                k = levels - 1 - j
                out = []
                for ref, old, gain, state in zip((us, vs), (u, v), (gain_a, gain_b), carry):
                    below, total, change = state
                    below = ref[c, k, here, :] + gain[k, pl.ds(0, SOLVE_ROWS), :] * below
                    ref[c, k, here, :] = below
                    out.append((below, total + below, change + (below - old[c, k, here, :])))
                return tuple(out)

            sums = over_levels(up, ((nil,) * 3,) * 2)
            for dz, total_map, force_map, state in zip((dzu_map, dzv_map), (su_map, sv_map), (fu_map, fv_map), sums):
                _, total, change = state
                total_map[c, flat, :] = dz[c, flat, :] * total
                force_map[c, flat, :] = dz[c, flat, :] * change * (1.0 / TIME_STEP)

        force_rows, force_cols, force_corners = split(sem_force)
        low, high, both = pl.ds(core, HALO), pl.ds(top - HALO, HALO), pl.ds(0, 2)

        def solve_tiles(first, step):
            def work(i, done):
                solve_part(first + step * (i // parts), i % parts)
                return done

            lax.fori_loop(0, 2 * parts, work, 0)
            sent = []
            for c in (first, first + step):
                sent += remote(
                    force_rows.at[both, pl.ds(2 * c, 2)],
                    (force.at[both, c, high, :], force.at[both, c, pl.ds(PAD, HALO), :], NORTH),
                    (force.at[both, c, low, :], force.at[both, c, pl.ds(top, HALO), :], SOUTH),
                )
            return sent

        ex3 = solve_tiles(0, tiles - 1)
        rim_pack((fu_map, fv_map), pk_e3, pk_w3)
        ex3 += column_rims(pk_e3, pk_w3, rim_w3, rim_e3, force_cols)
        ex3 += corner_rims(pk_e3, pk_w3, rim_w3, rim_e3, force_corners, HALO)
        start_all(ex3)
        late = solve_tiles(1, 1)
        start_all(late)
        ex3 += late

        (packed,) = edges((((0, us),),), (), ((vs, lr_v4),))
        cols_us[...] = pick(pair_of_lane == levels, roll(su_map[tiles - 1, own, :], 2 * levels + 1), packed)
        for c in range(tiles):
            lr_v4[c, pl.ds(levels, 1), :] = sv_map[c, pl.ds(top - 1, 1), :]
        ex_star = remote(sem_star, (cols_us, west_us, EAST), (lr_v4, rs_v4, NORTH))
        start_all(ex_star)

        wait_all(ex_ts)
        in_ts[...] = pick(odd, east_ts[...], west_ts[...])
        fill(
            ((tm, 0, in_ts, None), (sm, 1, in_ts, None)),
            ((tm, rn_t4, None), (sm, rn_s4, None)),
            ((tm, rs_t4, None), (sm, rs_s4, None)),
        )

        wait_all(far)
        for start in (far_low, far_high):
            rim_unpack((k_map, depth_map), rim_w1, rim_e1, start, far_n)
        wall(far_low, far_n, row_index > 0)
        wall(far_high, far_n, row_index < n_rows - 1)
        in_blocks(thickness, far_low, far_n, PAD)
        in_blocks(thickness, far_high, far_n, PAD)
        in_blocks(faces, PAD, HALO - PAD, PAD)
        in_blocks(faces, top + PAD, HALO - PAD, PAD)
        full_n = rows + 2 * HALO
        rim_unpack((eta_map, tu_map, tv_map), rim_w2, rim_e2, PAD, full_n)

        def start_fields(start, n):
            here = pl.ds(start, n)
            for ref, count in ((eta_map, k_out), (tu_map, ku_map), (tv_map, kv_map)):
                for c in range(ring):
                    ref[c, here, :] = pick(count[c, here, :] > 0, ref[c, here, :], 0.0)

        in_blocks(start_fields, PAD, full_n)
        tide_load.wait()

        wait_all(ex3)
        rim_unpack((fu_map, fv_map), rim_w3, rim_e3, PAD, full_n)

        def force_fields(start, n):
            here = pl.ds(start, n)
            for ref, count in ((fu_map, ku_map), (fv_map, kv_map)):
                for c in range(ring):
                    ref[c, here, :] = pick(count[c, here, :] > 0, dt_sub * ref[c, here, :], 0.0)

        in_blocks(force_fields, PAD, full_n)

        def subcycle(low, high):
            chunks = [(r, min(SUB_ROWS, high - r)) for r in range(low, high, SUB_ROWS)]

            def body(n, _):
                tide_u, tide_v = tide[0, n], tide[1, n]
                weight = weight_norm * ((n + 1) * (n_sub - n)).astype(F32)
                for r, n_r in chunks:
                    here, south = pl.ds(r, n_r), pl.ds(r - 1, n_r)
                    tu = [tu_map[c, here, :] for c in range(ring)]
                    tu_west = west(tu)
                    for c in range(ring):
                        spread = (tu[c] - tu_west[c]) + (tv_map[c, here, :] - tv_map[c, south, :])
                        eta_map[c, here, :] = eta_map[c, here, :] - wet_map[c, here, :] * spread
                for r, n_r in chunks:
                    here, north = pl.ds(r, n_r), pl.ds(r + 1, n_r)
                    eta = [eta_map[c, here, :] for c in range(ring)]
                    eta_east = east(eta)
                    averaged = r + n_r > core - 1 and r < top
                    for c in range(ring):
                        drive = hu_map[c, here, :] * (tide_u - scaled(GRAVITY, eta_east[c] - eta[c]))
                        tu = tu_map[c, here, :] + (drive + fu_map[c, here, :])
                        tu_map[c, here, :] = tu
                        drive = hv_map[c, here, :] * (tide_v - scaled(GRAVITY, eta_map[c, north, :] - eta[c]))
                        tv = tv_map[c, here, :] + (drive + fv_map[c, here, :])
                        tv_map[c, here, :] = tv
                        if averaged:
                            mu_map[c, here, :] = mu_map[c, here, :] + weight * tu
                            if c < tiles:
                                mv_map[c, here, :] = mv_map[c, here, :] + weight * tv
                return _

            return body

        begin, margin = 0, 0
        while begin < n_sub:
            end = n_sub if margin + PAD >= HALO else min(n_sub, n_sub - (HALO - margin - PAD))
            if end > begin:
                lax.fori_loop(begin, end, subcycle(PAD + margin, flat_rows - PAD - margin), 0)
                begin = end
            margin += PAD

        for ref, out in zip((eta_map, tu_map, tv_map), split(baro_out)):
            for c in range(tiles):
                out[c] = ref[c, own, :]

        wait_all(ex_star)
        fill(((us, 0, west_us, None),), (), ((vs, rs_v4, None),))
        su_map[halo_tile, own, :] = roll(west_us[...], LANES - 1 - 2 * levels)
        for c in range(tiles):
            sv_map[c, pl.ds(core - 1, 1), :] = rs_v4[c, pl.ds(levels, 1), :]
        cu_map, cv_map = split(corr)
        for out, mean_map, total_map, count, dz, n, here in (
            (cu_map, mu_map, su_map, ku_map, dzu_map, ring, own),
            (cv_map, mv_map, sv_map, kv_map, dzv_map, tiles, pl.ds(core - PAD, rows + PAD)),
        ):
            for c in range(n):
                depth = count[c, here, :] * dz[c, here, :]
                safe = pick(depth > 0, depth, 1.0)
                out[c, here, :] = (mean_map[c, here, :] - total_map[c, here, :]) / safe

    group = 4

    def back(us, vs, tm, sm, baro_in, corr, counts, eta_o, tu_o, tv_o, u_o, v_o, t_o, s_o, flux):
        k_map, ku_map, kv_map = split(counts)
        cu_map, cv_map = split(corr)
        fluxes = split(flux)
        for ref, out in zip(split(baro_in), (eta_o, tu_o, tv_o)):
            for c in range(tiles):
                out[:, pl.ds(c * LANES, LANES)] = ref[c]
        half = 0.5 * TIME_STEP

        def level(i, _):
            k = jnp.minimum(pl.program_id(0) * group + i, levels - 1)
            kf = k.astype(F32)
            for r in range(0, PAD + rows, PAD):
                here, north = pl.ds(r, PAD), pl.ds(r + 1, PAD)
                flat = pl.ds(r + core - PAD, PAD)
                for c in range(tiles):
                    vv = pick(kf < kv_map[c, flat, :], vs[c, k, here, :] + cv_map[c, flat, :], 0.0)
                    if r >= PAD:
                        v_o[i, pl.ds(r - PAD, PAD), pl.ds(c * LANES, LANES)] = vv
                    vv = half * vv
                    for ref, store in zip((tm, sm), fluxes):
                        store[c, here, :] = vv * (ref[c, k, here, :] + ref[c, k, north, :])
            for r in range(PAD, PAD + rows, BACK_ROWS):
                here, south = pl.ds(r, BACK_ROWS), pl.ds(r - 1, BACK_ROWS)
                flat = pl.ds(r - PAD + core, BACK_ROWS)
                out_rows = pl.ds(r - PAD, BACK_ROWS)
                uu = []
                for c in range(ring):
                    x = pick(kf < ku_map[c, flat, :], us[c, k, here, :] + cu_map[c, flat, :], 0.0)
                    if c < tiles:
                        u_o[i, out_rows, pl.ds(c * LANES, LANES)] = x
                    uu.append(half * x)
                for ref, store, out in zip((tm, sm), fluxes, (t_o, s_o)):
                    tt = [ref[c, k, here, :] for c in range(ring)]
                    fx = [x * (y + z) for x, y, z in zip(uu, tt, east(tt))]
                    fx_west = west(fx)
                    for c in range(tiles):
                        spread = (fx[c] - fx_west[c]) + (store[c, here, :] - store[c, south, :])
                        new = pick(kf < k_map[c, flat, :], tt[c] - spread, 0.0)
                        out[i, out_rows, pl.ds(c * LANES, LANES)] = new
            return _

        for i in range(group):
            level(i, 0)

    vmem = lambda *shape: pltpu.VMEM(shape, F32)
    flat = lambda n: vmem(n, ring, flat_rows, LANES)
    line = lambda n: vmem(n, tiles, SLOT, LANES)
    cube_buf = vmem(ring, levels, ext_rows, LANES)
    gain_buf = vmem(levels, rows, LANES)
    pack_buf = vmem(3, rows, LANES)
    rim_buf = vmem(3, rows + 2 * HALO, LANES)
    col_buf, corner_buf = vmem(rows, LANES), vmem(PAD, LANES)
    dma = lambda *shape: pltpu.SemaphoreType.DMA(shape)
    shared = [cube_buf, vmem(tiles, levels, ext_rows, LANES), cube_buf, cube_buf, vmem(3, tiles, rows, LANES), flat(2), flat(3)]
    routes = 7
    any_spec = pl.BlockSpec(memory_space=pl.ANY)
    vmem_spec = pl.BlockSpec(memory_space=pltpu.VMEM)
    front_call = pl.pallas_call(
        front,
        name="front",
        out_shape=shared,
        in_specs=[any_spec] * 10,
        out_specs=[vmem_spec] * len(shared),
        scratch_shapes=[
            cube_buf, cube_buf, cube_buf, gain_buf, vmem(levels, SOLVE_ROWS, LANES),
            vmem(ring, ext_rows, LANES), pltpu.VMEM((tiles, rows, LANES), jnp.int32),
            flat(2), flat(3), flat(3), flat(2), flat(3), flat(2), flat(2),
            pack_buf, pack_buf, rim_buf, rim_buf,
            vmem(4, rows, LANES), pack_buf, pack_buf, vmem(2, rows, LANES), line(3), line(2),
            line(3), line(2), corner_buf, corner_buf, line(2), line(3), line(2), line(3),
            pltpu.SMEM((2, n_sub), F32),
            dma(4, tiles), dma(5, tiles), pltpu.SemaphoreType.DMA,
            dma(3, 2, 4), dma(2, 2, 4), dma(3, 2, 4), dma(2, routes), dma(2, 4), dma(3, 2, 2 * tiles), dma(2, 2),
        ],
        compiler_params=pltpu.CompilerParams(
            collective_id=0, has_side_effects=True, vmem_limit_bytes=32 * MIB
        ),
    )
    plane_out = pl.BlockSpec((rows, cols), lambda i: (0, 0))
    cube_out = pl.BlockSpec((group, rows, cols), lambda i: (i, 0, 0))
    plane_shape = jax.ShapeDtypeStruct((rows, cols), F32)
    cube_shape = jax.ShapeDtypeStruct((levels, rows, cols), F32)
    back_call = pl.pallas_call(
        back,
        name="back",
        grid=(pl.cdiv(levels, group),),
        out_shape=[plane_shape] * 3 + [cube_shape] * 4,
        in_specs=[vmem_spec] * len(shared),
        out_specs=[plane_out] * 3 + [cube_out] * 4,
        scratch_shapes=[vmem(2, tiles, ext_rows, LANES)],
        compiler_params=pltpu.CompilerParams(vmem_limit_bytes=8 * MIB),
    )
    return front_call, back_call


def solution(mesh):
    def local_step(vel_u, vel_v, temperature, salinity, sea_level, trans_u, trans_v, bathymetry, kmt_levels, tide_force):
        levels, rows, cols = vel_u.shape
        front_call, back_call = kernels(mesh, levels, rows, cols, tide_force.shape[0])
        shared = front_call(
            vel_u, vel_v, temperature, salinity, sea_level, trans_u, trans_v, bathymetry, kmt_levels, tide_force.T
        )
        return tuple(back_call(*shared))

    spec_cube = P(None, "row", "col")
    spec_plane = P("row", "col")
    return jax.shard_map(
        local_step,
        mesh=mesh,
        in_specs=(spec_cube,) * 4 + (spec_plane,) * 5 + (P(None, None),),
        out_specs=(spec_plane,) * 3 + (spec_cube,) * 4,
        check_vma=False,
    )
```

```python
import jax
import jax.numpy as jnp
from jax import lax
from jax.experimental import pallas as pl
from jax.experimental.pallas import tpu as pltpu
from jax.sharding import PartitionSpec as P

GRAVITY = 1.0
TIME_STEP = 4.0
ALPHA_T = 0.02
BETA_S = 0.015
T_REF = 1.0
S_REF = 1.0
VISC_KV = 0.001
DIFF_KT = 0.0005

LANES = 128
HALO = 32
PAD = 8
NEAR = 16
F32 = jnp.float32
NORTH, SOUTH, EAST, WEST = (1, 0), (-1, 0), (0, 1), (0, -1)
NORTH_EAST, NORTH_WEST, SOUTH_EAST, SOUTH_WEST = (1, 1), (1, -1), (-1, 1), (-1, -1)
COMPASS = (NORTH, SOUTH, EAST, WEST, NORTH_EAST, NORTH_WEST, SOUTH_EAST, SOUTH_WEST)
SLOT = 32
BLOCK = 16
SOLVE_ROWS = 32
SUB_ROWS = 32
BACK_ROWS = 16
UNROLL = 2
EDGE_UNROLL = 3
MIB = 2**20


def kernels(mesh, levels, rows, cols, n_sub):
    n_cols, n_rows = mesh.shape["col"], mesh.shape["row"]
    tiles = cols // LANES
    ring = tiles + 1
    halo_tile = tiles
    ext_rows = rows + 2 * PAD
    flat_rows = rows + 2 * HALO + 2 * PAD
    core = PAD + HALO
    top = core + rows
    body_rows = pl.ds(PAD, rows)
    own = pl.ds(core, rows)
    dt_sub = TIME_STEP / n_sub
    weight_norm = 6.0 / (n_sub * (n_sub + 1) * (n_sub + 2))

    def lane_iota(n):
        return lax.broadcasted_iota(jnp.int32, (n, LANES), 1)

    def roll(x, shift):
        return pltpu.roll(x, shift, 1)

    def east(parts):
        last = lane_iota(parts[0].shape[0]) == LANES - 1
        moved = [roll(x, LANES - 1) for x in parts]
        return [pick(last, moved[(c + 1) % ring], moved[c]) for c in range(ring)]

    def west(parts):
        first = lane_iota(parts[0].shape[0]) == 0
        moved = [roll(x, 1) for x in parts]
        return [pick(first, moved[(c - 1) % ring], moved[c]) for c in range(ring)]

    def split(ref):
        return [ref.at[f] for f in range(ref.shape[0])]

    def scaled(factor, x):
        return x if factor == 1.0 else factor * x

    def real(k):
        return float(k) if isinstance(k, int) else k.astype(F32)

    def over_levels(body, carry, unroll=UNROLL):
        def trip(i, carry):
            for j in range(unroll):
                carry = body(unroll * i + j, carry)
            return carry

        carry = lax.fori_loop(0, levels // unroll, trip, carry)
        for k in range(levels - levels % unroll, levels):
            carry = body(k, carry)
        return carry

    def pick(condition, x, other):
        if jnp.ndim(condition) == 0:
            return jnp.where(condition, x, other)
        shape = condition.shape
        x = x if jnp.ndim(x) else jnp.full(shape, x, F32)
        other = other if jnp.ndim(other) else jnp.full(shape, other, F32)
        return lax.select(condition, x, other)

    def blank():
        return jnp.zeros((rows, LANES), F32)

    def neighbour(way):
        d_row, d_col = way
        row = lax.rem(lax.axis_index("row") + (d_row + n_rows), n_rows)
        col = lax.rem(lax.axis_index("col") + (d_col + n_cols), n_cols)
        return {"row": row, "col": col}

    def remote(sems, *routes):
        sent, arrived = split(sems)
        return [
            pltpu.make_async_remote_copy(
                src_ref=src,
                dst_ref=dst,
                send_sem=sent.at[index],
                recv_sem=arrived.at[index],
                device_id=neighbour(way),
                device_id_type=pl.DeviceIdType.MESH,
            )
            for index, (src, dst, way) in enumerate(routes)
        ]

    def start_all(copies):
        for copy in copies:
            copy.start()

    def wait_all(copies):
        for copy in copies:
            copy.wait()

    def rim_pack(maps, pack_east, pack_west):
        slot = lane_iota(rows) // HALO
        last, first = blank(), blank()
        for f, ref in enumerate(maps):
            last = pick(slot == f, roll(ref[tiles - 1, own, :], (HALO * f + HALO) % LANES), last)
            first = pick(slot == f, roll(ref[0, own, :], HALO * f), first)
        pack_east[...] = last
        pack_west[...] = first

    def row_rims(main, sems, reach, skip=0):
        every, inner, n = pl.ds(0, main.shape[0]), pl.ds(0, tiles), reach - skip
        return remote(
            sems,
            (main.at[every, inner, pl.ds(top - reach, n), :], main.at[every, inner, pl.ds(core - reach, n), :], NORTH),
            (main.at[every, inner, pl.ds(core + skip, n), :], main.at[every, inner, pl.ds(top + skip, n), :], SOUTH),
        )

    def column_rims(pack_east, pack_west, from_west, from_east, sems):
        own_rows = pl.ds(HALO, rows)
        return remote(sems, (pack_east, from_west.at[own_rows, :], EAST), (pack_west, from_east.at[own_rows, :], WEST))

    def corner_rims(pack_east, pack_west, from_west, from_east, sems, reach, skip=0):
        n = reach - skip
        p_high, p_low = pl.ds(rows - reach, n), pl.ds(skip, n)
        d_low, d_high = pl.ds(HALO - reach, n), pl.ds(HALO + rows + skip, n)
        return remote(
            sems,
            (pack_east.at[p_high, :], from_west.at[d_low, :], NORTH_EAST),
            (pack_west.at[p_high, :], from_east.at[d_low, :], NORTH_WEST),
            (pack_east.at[p_low, :], from_west.at[d_high, :], SOUTH_EAST),
            (pack_west.at[p_low, :], from_east.at[d_high, :], SOUTH_WEST),
        )

    def rim_unpack(maps, from_west, from_east, start, n):
        easterly = lane_iota(n) < LANES // 2
        here = pl.ds(start - PAD, n)
        for f, ref in enumerate(maps):
            e = roll(from_east[here, :], (LANES - HALO * f) % LANES)
            w = roll(from_west[here, :], LANES - HALO - HALO * f)
            ref[halo_tile, pl.ds(start, n), :] = pick(easterly, e, w)

    def front(
        u_hbm, v_hbm, t_hbm, s_hbm, eta_hbm, tu_hbm, tv_hbm, depth_hbm, kmt_hbm, tide_hbm,
        us, vs, tm, sm, baro_out, corr, counts,
        u, v, p, gain_a, gain_b, cross, kmt_int, geo, thick, baro, force, coef, mean, depth_sum,
        pk_e, pk_w, rim_w, rim_e, cols, cols_e, cols_w, cols_in, first_row, last_row,
        row_n, row_s, corner_nw, corner_se, first_row4, last_row4, row_n4, row_s4, tide,
        load_sems, plane_sems, tide_sem, sem_near, sem_far, sem_baro, sem_uv, sem_p, sem_ts, sem_force, sem_star,
    ):
        k_map, depth_map = split(geo)
        eta_map, tu_map, tv_map = split(baro)
        dz_map, dzu_map, dzv_map = split(thick)
        k_out, ku_map, kv_map = split(counts)
        wet_map, hu_map, hv_map = split(coef)
        fu_map, fv_map = split(force)
        mu_map, mv_map = split(mean)
        su_map, sv_map = split(depth_sum)
        pk_e1, pk_e2, pk_e3 = split(pk_e)
        pk_w1, pk_w2, pk_w3 = split(pk_w)
        rim_e1, rim_e2, rim_e3 = split(rim_e)
        rim_w1, rim_w2, rim_w3 = split(rim_w)
        zero = blank()
        lane = lane_iota(rows)
        low_half = lane < LANES // 2
        pair_of_lane, odd = lane // 2, lane % 2 == 1

        barrier = pltpu.get_barrier_semaphore()
        for way in COMPASS:
            pl.semaphore_signal(barrier, device_id=neighbour(way), device_id_type=pl.DeviceIdType.MESH)

        def plane_load(sems, src, dst):
            return [
                pltpu.make_async_copy(src.at[:, pl.ds(c * LANES, LANES)], dst(c), sems.at[c]) for c in range(tiles)
            ]

        def cube_load(sems, src, dst):
            return [
                pltpu.make_async_copy(
                    src.at[:, :, pl.ds(c * LANES, LANES)], dst.at[c, :, body_rows, :], sems.at[c]
                )
                for c in range(tiles)
            ]

        sem_k, sem_h, sem_e, sem_tu, sem_tv = split(plane_sems)
        sem_t, sem_s, sem_u, sem_v = split(load_sems)
        geo_load = plane_load(sem_k, kmt_hbm, lambda c: kmt_int.at[c]) + plane_load(
            sem_h, depth_hbm, lambda c: depth_map.at[c, own, :]
        )
        baro_load = (
            plane_load(sem_e, eta_hbm, lambda c: eta_map.at[c, own, :])
            + plane_load(sem_tu, tu_hbm, lambda c: tu_map.at[c, own, :])
            + plane_load(sem_tv, tv_hbm, lambda c: tv_map.at[c, own, :])
        )
        tracer_load = cube_load(sem_t, t_hbm, tm) + cube_load(sem_s, s_hbm, sm)
        flow_load = cube_load(sem_u, u_hbm, u) + cube_load(sem_v, v_hbm, v)
        tide_load = pltpu.make_async_copy(tide_hbm, tide, tide_sem)
        start_all(geo_load)
        start_all(flow_load)
        start_all(tracer_load)
        start_all(baro_load)
        tide_load.start()

        zero_rows = jnp.zeros((PAD, LANES), F32)
        for ref in (k_map, depth_map, dz_map, eta_map, tu_map, tv_map):
            for c in range(ring):
                ref[c, pl.ds(0, PAD), :] = zero_rows
                ref[c, pl.ds(flat_rows - PAD, PAD), :] = zero_rows
        for ref in (mu_map, mv_map):
            for c in range(ring):
                ref[c] = jnp.zeros((flat_rows, LANES), F32)

        wait_all(geo_load)
        for c in range(tiles):
            k_map[c, own, :] = kmt_int[c].astype(F32)
        rim_pack((k_map, depth_map), pk_e1, pk_w1)
        pl.semaphore_wait(barrier, len(COMPASS))
        near_rows, near_cols, near_corners = split(sem_near)
        near = row_rims(geo, near_rows, NEAR)
        near += column_rims(pk_e1, pk_w1, rim_w1, rim_e1, near_cols)
        near += corner_rims(pk_e1, pk_w1, rim_w1, rim_e1, near_corners, NEAR)
        start_all(near)

        def tracer_tile(c, _):
            k_cell = k_map[c, own, :]
            dz = depth_map[c, own, :] / jnp.maximum(k_cell, 1.0)
            safe = pick(k_cell > 0, dz, 1.0)
            couple = (TIME_STEP * DIFF_KT) / (safe * safe)

            def down(k, carry):
                lower, keep, part_t, part_s = carry
                kf = real(k)
                wet = kf < k_cell
                upper = pick(kf + 1.0 < k_cell, couple, zero)
                turn = 1.0 + lower * keep
                inv = 1.0 / (turn + upper)
                gain_a[k] = upper * inv
                part_t = (pick(wet, tm[c, k, body_rows, :], zero) + lower * part_t) * inv
                part_s = (pick(wet, sm[c, k, body_rows, :], zero) + lower * part_s) * inv
                tm[c, k, body_rows, :] = part_t
                sm[c, k, body_rows, :] = part_s
                return upper, turn * inv, part_t, part_s

            over_levels(down, (zero, zero, zero, zero))

            def up(i, carry):
                below_t, below_s = carry
                k = levels - 1 - i
                gain = gain_a[k]
                below_t = tm[c, k, body_rows, :] + gain * below_t
                below_s = sm[c, k, body_rows, :] + gain * below_s
                tm[c, k, body_rows, :] = below_t
                sm[c, k, body_rows, :] = below_s
                return below_t, below_s

            over_levels(up, (zero, zero))
            return _

        def edges(columns, top_rows, bottom_rows):
            def level(k, packed):
                row = pl.ds(k, 1)
                out = []
                for pair, acc in zip(columns, packed):
                    for f, ref in pair:
                        slot = SLOT * f + k
                        both = pick(low_half, ref[0, k, body_rows, :], ref[tiles - 1, k, body_rows, :])
                        acc = pick(pair_of_lane == slot, roll(both, 2 * slot + 1), acc)
                    out.append(acc)
                for c in range(tiles):
                    for ref, dst in top_rows:
                        dst[c, row, :] = ref[c, k, pl.ds(PAD, 1), :]
                    for ref, dst in bottom_rows:
                        dst[c, row, :] = ref[c, k, pl.ds(PAD + rows - 1, 1), :]
                return tuple(out)

            return over_levels(level, (zero,) * len(columns), EDGE_UNROLL)

        wait_all(flow_load)
        cols_uv, cols_p, cols_ts, cols_us = split(cols)
        east_uv, east_p, east_ts = split(cols_e)
        west_uv, west_ts, west_us = split(cols_w)
        fr_u, fr_v, fr_p = split(first_row)
        lr_u, lr_v = split(last_row)
        rn_u, rn_v, rn_p = split(row_n)
        rs_u, rs_v = split(row_s)
        (packed,) = edges((((0, u), (1, v)),), ((u, fr_u), (v, fr_v)), ((u, lr_u), (v, lr_v)))
        cols_uv[...] = packed
        two = pl.ds(0, 2)
        ex_uv = remote(
            sem_uv,
            (first_row.at[two], row_n.at[two], SOUTH),
            (last_row, row_s, NORTH),
            (cols_uv, east_uv, WEST),
            (cols_uv, west_uv, EAST),
            (cols_uv.at[pl.ds(0, PAD), :], corner_nw, SOUTH_EAST),
            (cols_uv.at[pl.ds(rows - PAD, PAD), :], corner_se, NORTH_WEST),
        )
        start_all(ex_uv)

        rho_s, rho_t = 0.5 * BETA_S, 0.5 * ALPHA_T
        rho_0 = rho_t * T_REF - rho_s * S_REF

        def pressure_tile(c, _):
            k_cell = k_map[c, own, :]
            scale = (TIME_STEP * GRAVITY) * (depth_map[c, own, :] / jnp.maximum(k_cell, 1.0))

            def level(k, total):
                half = (rho_s * sm[c, k, body_rows, :] - rho_t * tm[c, k, body_rows, :]) + rho_0
                half = pick(real(k) < k_cell, half, zero)
                middle = total + half
                p[c, k, body_rows, :] = scale * middle
                return middle + half

            over_levels(level, zero)
            return _

        wait_all(tracer_load)
        lax.fori_loop(0, tiles, pressure_tile, 0)

        (packed,) = edges((((0, p),),), ((p, fr_p),), ())
        cols_p[...] = packed
        ex_p = remote(sem_p, (fr_p, rn_p, SOUTH), (cols_p, east_p, WEST))
        start_all(ex_p)

        wait_all(baro_load)
        rim_pack((eta_map, tu_map, tv_map), pk_e2, pk_w2)
        far_rows, far_corners = split(sem_far)
        baro_rows, baro_cols, baro_corners = split(sem_baro)
        far = row_rims(geo, far_rows, HALO, NEAR)
        far += corner_rims(pk_e1, pk_w1, rim_w1, rim_e1, far_corners, HALO, NEAR)
        far += row_rims(baro, baro_rows, HALO)
        far += column_rims(pk_e2, pk_w2, rim_w2, rim_e2, baro_cols)
        far += corner_rims(pk_e2, pk_w2, rim_w2, rim_e2, baro_corners, HALO)
        start_all(far)

        lax.fori_loop(0, tiles, tracer_tile, 0)
        fr_t4, fr_s4 = split(first_row4)
        lr_t4, lr_s4, lr_v4 = split(last_row4)
        rn_t4, rn_s4 = split(row_n4)
        rs_t4, rs_s4, rs_v4 = split(row_s4)
        (packed,) = edges((((0, tm), (1, sm)),), ((tm, fr_t4), (sm, fr_s4)), ((tm, lr_t4), (sm, lr_s4)))
        cols_ts[...] = packed
        ex_ts = remote(
            sem_ts,
            (cols_ts, east_ts, WEST),
            (cols_ts, west_ts, EAST),
            (first_row4, row_n4, SOUTH),
            (last_row4.at[two], row_s4.at[two], NORTH),
        )
        start_all(ex_ts)

        row_index = lax.axis_index("row")

        def wall(low, n, inside):
            @pl.when(jnp.logical_not(inside))
            def _():
                for c in range(ring):
                    k_map[c, pl.ds(low, n), :] = jnp.zeros((n, LANES), F32)

        def thickness(start, n):
            here = pl.ds(start, n)
            for c in range(ring):
                dz_map[c, here, :] = depth_map[c, here, :] / jnp.maximum(k_map[c, here, :], 1.0)

        def faces(start, n):
            here, north = pl.ds(start, n), pl.ds(start + 1, n)
            k_cell = [k_map[c, here, :] for c in range(ring)]
            dz = [dz_map[c, here, :] for c in range(ring)]
            k_east, dz_east = east(k_cell), east(dz)
            for c in range(ring):
                k_u = jnp.minimum(k_cell[c], k_east[c])
                k_v = jnp.minimum(k_cell[c], k_map[c, north, :])
                dz_u = 0.5 * (dz[c] + dz_east[c])
                dz_v = 0.5 * (dz[c] + dz_map[c, north, :])
                k_out[c, here, :] = k_cell[c]
                ku_map[c, here, :] = k_u
                kv_map[c, here, :] = k_v
                dzu_map[c, here, :] = dz_u
                dzv_map[c, here, :] = dz_v
                wet_map[c, here, :] = pick(k_cell[c] > 0, dt_sub, 0.0)
                hu_map[c, here, :] = dt_sub * (k_u * dz_u)
                hv_map[c, here, :] = dt_sub * (k_v * dz_v)

        def in_blocks(work, start, n, size=BLOCK):
            lax.fori_loop(0, n // size, lambda i, _: (work(pl.multiple_of(start + size * i, PAD), size), _)[1], 0)

        far_low, far_high, far_n = PAD, top + NEAR, HALO - NEAR
        wait_all(near)
        rim_unpack((k_map, depth_map), rim_w1, rim_e1, core - NEAR, rows + 2 * NEAR)
        wall(core - NEAR, NEAR, row_index > 0)
        wall(top, NEAR, row_index < n_rows - 1)
        in_blocks(thickness, core - NEAR, rows + 2 * NEAR)
        in_blocks(faces, core - PAD, rows + 2 * PAD)

        def mask_tile(c, _):
            for ref, count in ((u, ku_map), (v, kv_map)):
                k_face = count[c, own, :]

                def level(k, done, ref=ref, k_face=k_face):
                    ref[c, k, body_rows, :] = pick(real(k) < k_face, ref[c, k, body_rows, :], zero)
                    return done

                over_levels(level, 0)
            return _

        lax.fori_loop(0, tiles, mask_tile, 0)

        def fill(columns, norths, souths):
            def masked(x, k, count, tile, here):
                return x if count is None else pick(real(k) < count[tile, here, :], x, 0.0)

            def level(k, _):
                for ref, f, src, count in columns:
                    x = roll(src[...], LANES - 1 - 2 * (SLOT * f + k))
                    ref[halo_tile, k, body_rows, :] = masked(x, k, count, halo_tile, own)
                row = pl.ds(k, 1)
                for c in range(tiles):
                    for ref, src, count in norths:
                        x = masked(src[c, row, :], k, count, c, pl.ds(top, 1))
                        ref[c, k, pl.ds(PAD + rows, 1), :] = x
                    for ref, src, count in souths:
                        x = masked(src[c, row, :], k, count, c, pl.ds(core - 1, 1))
                        ref[c, k, pl.ds(PAD - 1, 1), :] = x
                return _

            over_levels(level, 0, EDGE_UNROLL)

        in_uv, in_ts = split(cols_in)
        wait_all(ex_uv)
        wait_all(ex_p)
        in_uv[...] = pick(odd, east_uv[...], west_uv[...])
        fill(
            ((u, 0, in_uv, ku_map), (v, 1, in_uv, kv_map), (p, 0, east_p, None)),
            ((u, rn_u, ku_map), (v, rn_v, kv_map), (p, rn_p, None)),
            ((u, rs_u, ku_map), (v, rs_v, kv_map)),
        )

        def corners(k, _):
            kf = real(k)
            x = roll(corner_nw[...], LANES - 1 - 2 * k)
            u[halo_tile, k, pl.ds(PAD + rows, PAD), :] = pick(kf < ku_map[halo_tile, pl.ds(top, PAD), :], x, 0.0)
            x = roll(corner_se[...], LANES - 1 - 2 * (SLOT + k))
            v[halo_tile, k, pl.ds(0, PAD), :] = pick(kf < kv_map[halo_tile, pl.ds(core - PAD, PAD), :], x, 0.0)
            return _

        over_levels(corners, 0, EDGE_UNROLL)

        quarter = 0.25 * TIME_STEP

        def momentum(k, _):
            tall, tall_north = pl.ds(0, PAD + rows), pl.ds(1, PAD + rows)
            here, north, south = body_rows, pl.ds(PAD + 1, rows), pl.ds(PAD - 1, rows)
            vv = [v[c, k, tall, :] for c in range(ring)]
            v_east = east(vv)
            for c in range(ring):
                cross[c, tall, :] = (vv[c] + v_east[c]) * (u[c, k, tall, :] + u[c, k, tall_north, :])
            uu = [u[c, k, here, :] for c in range(ring)]
            pp = [p[c, k, here, :] for c in range(ring)]
            centre = [x + y for x, y in zip(uu, west(uu))]
            centre = [scaled(quarter, x * x) + y for x, y in zip(centre, pp)]
            centre_east = east(centre)
            xx = [cross[c, here, :] for c in range(ring)]
            x_west = west(xx)
            for c in range(tiles):
                us[c, k, here, :] = uu[c] - (
                    (centre_east[c] - centre[c]) + scaled(quarter, xx[c] - cross[c, south, :])
                )
                vv = v[c, k, here, :]
                b_here = vv + v[c, k, north, :]
                b_south = vv + v[c, k, south, :]
                push = (b_here * b_here - b_south * b_south) + (xx[c] - x_west[c])
                vs[c, k, here, :] = vv - (scaled(quarter, push) + (p[c, k, north, :] - pp[c]))
            return _

        over_levels(momentum, 0)

        nil = jnp.zeros((SOLVE_ROWS, LANES), F32)
        parts = rows // SOLVE_ROWS

        def solve_part(c, i):
            r = pl.multiple_of(i * SOLVE_ROWS, PAD)
            flat, here = pl.ds(core + r, SOLVE_ROWS), pl.ds(PAD + r, SOLVE_ROWS)
            faces = []
            for count, dz in ((ku_map, dzu_map), (kv_map, dzv_map)):
                k_face = count[c, flat, :]
                safe = pick(k_face > 0, dz[c, flat, :], 1.0)
                faces.append((k_face, (TIME_STEP * VISC_KV) / (safe * safe)))

            def down(k, carry):
                kf = real(k)
                out = []
                for face, ref, gain, state in zip(faces, (us, vs), (gain_a, gain_b), carry):
                    k_face, couple = face
                    lower, keep, part = state
                    upper = pick(kf + 1.0 < k_face, couple, nil)
                    turn = 1.0 + lower * keep
                    inv = 1.0 / (turn + upper)
                    gain[k, pl.ds(0, SOLVE_ROWS), :] = upper * inv
                    part = (pick(kf < k_face, ref[c, k, here, :], nil) + lower * part) * inv
                    ref[c, k, here, :] = part
                    out.append((upper, turn * inv, part))
                return tuple(out)

            over_levels(down, ((nil,) * 3,) * 2)

            def up(j, carry):
                k = levels - 1 - j
                out = []
                for ref, old, gain, state in zip((us, vs), (u, v), (gain_a, gain_b), carry):
                    below, total, change = state
                    below = ref[c, k, here, :] + gain[k, pl.ds(0, SOLVE_ROWS), :] * below
                    ref[c, k, here, :] = below
                    out.append((below, total + below, change + (below - old[c, k, here, :])))
                return tuple(out)

            sums = over_levels(up, ((nil,) * 3,) * 2)
            for dz, total_map, force_map, state in zip((dzu_map, dzv_map), (su_map, sv_map), (fu_map, fv_map), sums):
                _, total, change = state
                total_map[c, flat, :] = dz[c, flat, :] * total
                force_map[c, flat, :] = dz[c, flat, :] * change * (1.0 / TIME_STEP)

        force_rows, force_cols, force_corners = split(sem_force)
        low, high, both = pl.ds(core, HALO), pl.ds(top - HALO, HALO), pl.ds(0, 2)

        def solve_tiles(first, step):
            def work(i, done):
                solve_part(first + step * (i // parts), i % parts)
                return done

            lax.fori_loop(0, 2 * parts, work, 0)
            sent = []
            for c in (first, first + step):
                sent += remote(
                    force_rows.at[both, pl.ds(2 * c, 2)],
                    (force.at[both, c, high, :], force.at[both, c, pl.ds(PAD, HALO), :], NORTH),
                    (force.at[both, c, low, :], force.at[both, c, pl.ds(top, HALO), :], SOUTH),
                )
            return sent

        ex3 = solve_tiles(0, tiles - 1)
        rim_pack((fu_map, fv_map), pk_e3, pk_w3)
        ex3 += column_rims(pk_e3, pk_w3, rim_w3, rim_e3, force_cols)
        ex3 += corner_rims(pk_e3, pk_w3, rim_w3, rim_e3, force_corners, HALO)
        start_all(ex3)
        late = solve_tiles(1, 1)
        start_all(late)
        ex3 += late

        (packed,) = edges((((0, us),),), (), ((vs, lr_v4),))
        cols_us[...] = pick(pair_of_lane == levels, roll(su_map[tiles - 1, own, :], 2 * levels + 1), packed)
        for c in range(tiles):
            lr_v4[c, pl.ds(levels, 1), :] = sv_map[c, pl.ds(top - 1, 1), :]
        ex_star = remote(sem_star, (cols_us, west_us, EAST), (lr_v4, rs_v4, NORTH))
        start_all(ex_star)

        wait_all(ex_ts)
        in_ts[...] = pick(odd, east_ts[...], west_ts[...])
        fill(
            ((tm, 0, in_ts, None), (sm, 1, in_ts, None)),
            ((tm, rn_t4, None), (sm, rn_s4, None)),
            ((tm, rs_t4, None), (sm, rs_s4, None)),
        )

        wait_all(far)
        for start in (far_low, far_high):
            rim_unpack((k_map, depth_map), rim_w1, rim_e1, start, far_n)
        wall(far_low, far_n, row_index > 0)
        wall(far_high, far_n, row_index < n_rows - 1)
        in_blocks(thickness, far_low, far_n, PAD)
        in_blocks(thickness, far_high, far_n, PAD)
        in_blocks(faces, PAD, HALO - PAD, PAD)
        in_blocks(faces, top + PAD, HALO - PAD, PAD)
        full_n = rows + 2 * HALO
        rim_unpack((eta_map, tu_map, tv_map), rim_w2, rim_e2, PAD, full_n)

        def start_fields(start, n):
            here = pl.ds(start, n)
            for ref, count in ((eta_map, k_out), (tu_map, ku_map), (tv_map, kv_map)):
                for c in range(ring):
                    ref[c, here, :] = pick(count[c, here, :] > 0, ref[c, here, :], 0.0)

        in_blocks(start_fields, PAD, full_n)
        tide_load.wait()

        wait_all(ex3)
        rim_unpack((fu_map, fv_map), rim_w3, rim_e3, PAD, full_n)

        def force_fields(start, n):
            here = pl.ds(start, n)
            for ref, count in ((fu_map, ku_map), (fv_map, kv_map)):
                for c in range(ring):
                    ref[c, here, :] = pick(count[c, here, :] > 0, dt_sub * ref[c, here, :], 0.0)

        in_blocks(force_fields, PAD, full_n)

        def subcycle(low, high):
            chunks = [(r, min(SUB_ROWS, high - r)) for r in range(low, high, SUB_ROWS)]

            def body(n, _):
                tide_u, tide_v = tide[0, n], tide[1, n]
                weight = weight_norm * ((n + 1) * (n_sub - n)).astype(F32)
                for r, n_r in chunks:
                    here, south = pl.ds(r, n_r), pl.ds(r - 1, n_r)
                    tu = [tu_map[c, here, :] for c in range(ring)]
                    tu_west = west(tu)
                    for c in range(ring):
                        spread = (tu[c] - tu_west[c]) + (tv_map[c, here, :] - tv_map[c, south, :])
                        eta_map[c, here, :] = eta_map[c, here, :] - wet_map[c, here, :] * spread
                for r, n_r in chunks:
                    here, north = pl.ds(r, n_r), pl.ds(r + 1, n_r)
                    eta = [eta_map[c, here, :] for c in range(ring)]
                    eta_east = east(eta)
                    averaged = r + n_r > core - 1 and r < top
                    for c in range(ring):
                        drive = hu_map[c, here, :] * (tide_u - scaled(GRAVITY, eta_east[c] - eta[c]))
                        tu = tu_map[c, here, :] + (drive + fu_map[c, here, :])
                        tu_map[c, here, :] = tu
                        drive = hv_map[c, here, :] * (tide_v - scaled(GRAVITY, eta_map[c, north, :] - eta[c]))
                        tv = tv_map[c, here, :] + (drive + fv_map[c, here, :])
                        tv_map[c, here, :] = tv
                        if averaged:
                            mu_map[c, here, :] = mu_map[c, here, :] + weight * tu
                            if c < tiles:
                                mv_map[c, here, :] = mv_map[c, here, :] + weight * tv
                return _

            return body

        begin, margin = 0, 0
        while begin < n_sub:
            end = n_sub if margin + PAD >= HALO else min(n_sub, n_sub - (HALO - margin - PAD))
            if end > begin:
                lax.fori_loop(begin, end, subcycle(PAD + margin, flat_rows - PAD - margin), 0)
                begin = end
            margin += PAD

        for ref, out in zip((eta_map, tu_map, tv_map), split(baro_out)):
            for c in range(tiles):
                out[c] = ref[c, own, :]

        wait_all(ex_star)
        fill(((us, 0, west_us, None),), (), ((vs, rs_v4, None),))
        su_map[halo_tile, own, :] = roll(west_us[...], LANES - 1 - 2 * levels)
        for c in range(tiles):
            sv_map[c, pl.ds(core - 1, 1), :] = rs_v4[c, pl.ds(levels, 1), :]
        cu_map, cv_map = split(corr)
        for out, mean_map, total_map, count, dz, n, here in (
            (cu_map, mu_map, su_map, ku_map, dzu_map, ring, own),
            (cv_map, mv_map, sv_map, kv_map, dzv_map, tiles, pl.ds(core - PAD, rows + PAD)),
        ):
            for c in range(n):
                depth = count[c, here, :] * dz[c, here, :]
                safe = pick(depth > 0, depth, 1.0)
                out[c, here, :] = (mean_map[c, here, :] - total_map[c, here, :]) / safe

    group = 4

    def back(us, vs, tm, sm, baro_in, corr, counts, eta_o, tu_o, tv_o, u_o, v_o, t_o, s_o, flux):
        k_map, ku_map, kv_map = split(counts)
        cu_map, cv_map = split(corr)
        fluxes = split(flux)
        for ref, out in zip(split(baro_in), (eta_o, tu_o, tv_o)):
            for c in range(tiles):
                out[:, pl.ds(c * LANES, LANES)] = ref[c]
        half = 0.5 * TIME_STEP

        def level(i, _):
            k = jnp.minimum(pl.program_id(0) * group + i, levels - 1)
            kf = k.astype(F32)
            for r in range(0, PAD + rows, PAD):
                here, north = pl.ds(r, PAD), pl.ds(r + 1, PAD)
                flat = pl.ds(r + core - PAD, PAD)
                for c in range(tiles):
                    vv = pick(kf < kv_map[c, flat, :], vs[c, k, here, :] + cv_map[c, flat, :], 0.0)
                    if r >= PAD:
                        v_o[i, pl.ds(r - PAD, PAD), pl.ds(c * LANES, LANES)] = vv
                    vv = half * vv
                    for ref, store in zip((tm, sm), fluxes):
                        store[c, here, :] = vv * (ref[c, k, here, :] + ref[c, k, north, :])
            for r in range(PAD, PAD + rows, BACK_ROWS):
                here, south = pl.ds(r, BACK_ROWS), pl.ds(r - 1, BACK_ROWS)
                flat = pl.ds(r - PAD + core, BACK_ROWS)
                out_rows = pl.ds(r - PAD, BACK_ROWS)
                uu = []
                for c in range(ring):
                    x = pick(kf < ku_map[c, flat, :], us[c, k, here, :] + cu_map[c, flat, :], 0.0)
                    if c < tiles:
                        u_o[i, out_rows, pl.ds(c * LANES, LANES)] = x
                    uu.append(half * x)
                for ref, store, out in zip((tm, sm), fluxes, (t_o, s_o)):
                    tt = [ref[c, k, here, :] for c in range(ring)]
                    fx = [x * (y + z) for x, y, z in zip(uu, tt, east(tt))]
                    fx_west = west(fx)
                    for c in range(tiles):
                        spread = (fx[c] - fx_west[c]) + (store[c, here, :] - store[c, south, :])
                        new = pick(kf < k_map[c, flat, :], tt[c] - spread, 0.0)
                        out[i, out_rows, pl.ds(c * LANES, LANES)] = new
            return _

        lax.fori_loop(0, group, level, 0)

    vmem = lambda *shape: pltpu.VMEM(shape, F32)
    flat = lambda n: vmem(n, ring, flat_rows, LANES)
    line = lambda n: vmem(n, tiles, SLOT, LANES)
    cube_buf = vmem(ring, levels, ext_rows, LANES)
    gain_buf = vmem(levels, rows, LANES)
    pack_buf = vmem(3, rows, LANES)
    rim_buf = vmem(3, rows + 2 * HALO, LANES)
    col_buf, corner_buf = vmem(rows, LANES), vmem(PAD, LANES)
    dma = lambda *shape: pltpu.SemaphoreType.DMA(shape)
    shared = [cube_buf, vmem(tiles, levels, ext_rows, LANES), cube_buf, cube_buf, vmem(3, tiles, rows, LANES), flat(2), flat(3)]
    routes = 6
    any_spec = pl.BlockSpec(memory_space=pl.ANY)
    vmem_spec = pl.BlockSpec(memory_space=pltpu.VMEM)
    front_call = pl.pallas_call(
        front,
        name="front",
        out_shape=shared,
        in_specs=[any_spec] * 10,
        out_specs=[vmem_spec] * len(shared),
        scratch_shapes=[
            cube_buf, cube_buf, cube_buf, gain_buf, vmem(levels, SOLVE_ROWS, LANES),
            vmem(ring, ext_rows, LANES), pltpu.VMEM((tiles, rows, LANES), jnp.int32),
            flat(2), flat(3), flat(3), flat(2), flat(3), flat(2), flat(2),
            pack_buf, pack_buf, rim_buf, rim_buf,
            vmem(4, rows, LANES), pack_buf, pack_buf, vmem(2, rows, LANES), line(3), line(2),
            line(3), line(2), corner_buf, corner_buf, line(2), line(3), line(2), line(3),
            pltpu.SMEM((2, n_sub), F32),
            dma(4, tiles), dma(5, tiles), pltpu.SemaphoreType.DMA,
            dma(3, 2, 4), dma(2, 2, 4), dma(3, 2, 4), dma(2, routes), dma(2, 2), dma(2, 4), dma(3, 2, 2 * tiles), dma(2, 2),
        ],
        compiler_params=pltpu.CompilerParams(
            collective_id=0, has_side_effects=True, vmem_limit_bytes=32 * MIB
        ),
    )
    plane_out = pl.BlockSpec((rows, cols), lambda i: (0, 0))
    cube_out = pl.BlockSpec((group, rows, cols), lambda i: (i, 0, 0))
    plane_shape = jax.ShapeDtypeStruct((rows, cols), F32)
    cube_shape = jax.ShapeDtypeStruct((levels, rows, cols), F32)
    back_call = pl.pallas_call(
        back,
        name="back",
        grid=(pl.cdiv(levels, group),),
        out_shape=[plane_shape] * 3 + [cube_shape] * 4,
        in_specs=[vmem_spec] * len(shared),
        out_specs=[plane_out] * 3 + [cube_out] * 4,
        scratch_shapes=[vmem(2, tiles, ext_rows, LANES)],
        compiler_params=pltpu.CompilerParams(vmem_limit_bytes=8 * MIB),
    )
    return front_call, back_call


def solution(mesh):
    def local_step(vel_u, vel_v, temperature, salinity, sea_level, trans_u, trans_v, bathymetry, kmt_levels, tide_force):
        levels, rows, cols = vel_u.shape
        front_call, back_call = kernels(mesh, levels, rows, cols, tide_force.shape[0])
        shared = front_call(
            vel_u, vel_v, temperature, salinity, sea_level, trans_u, trans_v, bathymetry, kmt_levels, tide_force.T
        )
        return tuple(back_call(*shared))

    spec_cube = P(None, "row", "col")
    spec_plane = P("row", "col")
    return jax.shard_map(
        local_step,
        mesh=mesh,
        in_specs=(spec_cube,) * 4 + (spec_plane,) * 5 + (P(None, None),),
        out_specs=(spec_plane,) * 3 + (spec_cube,) * 4,
        check_vma=False,
    )
```

```python
import jax
import jax.numpy as jnp
from jax import lax
from jax.experimental import pallas as pl
from jax.experimental.pallas import tpu as pltpu
from jax.sharding import PartitionSpec as P

GRAVITY = 1.0
TIME_STEP = 4.0
ALPHA_T = 0.02
BETA_S = 0.015
T_REF = 1.0
S_REF = 1.0
VISC_KV = 0.001
DIFF_KT = 0.0005

LANES = 128
HALO = 32
PAD = 8
NEAR = 16
F32 = jnp.float32
NORTH, SOUTH, EAST, WEST = (1, 0), (-1, 0), (0, 1), (0, -1)
NORTH_EAST, NORTH_WEST, SOUTH_EAST, SOUTH_WEST = (1, 1), (1, -1), (-1, 1), (-1, -1)
COMPASS = (NORTH, SOUTH, EAST, WEST, NORTH_EAST, NORTH_WEST, SOUTH_EAST, SOUTH_WEST)
SLOT = 32
BLOCK = 16
SOLVE_ROWS = 32
SUB_ROWS = 32
UNROLL = 2
EDGE_UNROLL = 3
FLOW_UNROLL = 4
MIB = 2**20


def kernels(mesh, levels, rows, cols, n_sub):
    n_cols, n_rows = mesh.shape["col"], mesh.shape["row"]
    tiles = cols // LANES
    ring = tiles + 1
    halo_tile = tiles
    ext_rows = rows + 2 * PAD
    flat_rows = rows + 2 * HALO + 2 * PAD
    core = PAD + HALO
    top = core + rows
    body_rows = pl.ds(PAD, rows)
    own = pl.ds(core, rows)
    dt_sub = TIME_STEP / n_sub
    weight_norm = 6.0 / (n_sub * (n_sub + 1) * (n_sub + 2))

    def lane_iota(n):
        return lax.broadcasted_iota(jnp.int32, (n, LANES), 1)

    def roll(x, shift):
        return pltpu.roll(x, shift, 1)

    def east(parts):
        last = lane_iota(parts[0].shape[0]) == LANES - 1
        moved = [roll(x, LANES - 1) for x in parts]
        return [pick(last, moved[(c + 1) % ring], moved[c]) for c in range(ring)]

    def west(parts):
        first = lane_iota(parts[0].shape[0]) == 0
        moved = [roll(x, 1) for x in parts]
        return [pick(first, moved[(c - 1) % ring], moved[c]) for c in range(ring)]

    def split(ref):
        return [ref.at[f] for f in range(ref.shape[0])]

    def scaled(factor, x):
        return x if factor == 1.0 else factor * x

    def real(k):
        return float(k) if isinstance(k, int) else k.astype(F32)

    def over_levels(body, carry, unroll=UNROLL):
        def trip(i, carry):
            for j in range(unroll):
                carry = body(unroll * i + j, carry)
            return carry

        carry = lax.fori_loop(0, levels // unroll, trip, carry)
        for k in range(levels - levels % unroll, levels):
            carry = body(k, carry)
        return carry

    def pick(condition, x, other):
        if jnp.ndim(condition) == 0:
            return jnp.where(condition, x, other)
        shape = condition.shape
        x = x if jnp.ndim(x) else jnp.full(shape, x, F32)
        other = other if jnp.ndim(other) else jnp.full(shape, other, F32)
        return lax.select(condition, x, other)

    def blank():
        return jnp.zeros((rows, LANES), F32)

    def neighbour(way):
        d_row, d_col = way
        row = lax.rem(lax.axis_index("row") + (d_row + n_rows), n_rows)
        col = lax.rem(lax.axis_index("col") + (d_col + n_cols), n_cols)
        return {"row": row, "col": col}

    def remote(sems, *routes):
        sent, arrived = split(sems)
        return [
            pltpu.make_async_remote_copy(
                src_ref=src,
                dst_ref=dst,
                send_sem=sent.at[index],
                recv_sem=arrived.at[index],
                device_id=neighbour(way),
                device_id_type=pl.DeviceIdType.MESH,
            )
            for index, (src, dst, way) in enumerate(routes)
        ]

    def start_all(copies):
        for copy in copies:
            copy.start()

    def wait_all(copies):
        for copy in copies:
            copy.wait()

    def rim_pack(maps, pack_east, pack_west):
        slot = lane_iota(rows) // HALO
        last, first = blank(), blank()
        for f, ref in enumerate(maps):
            last = pick(slot == f, roll(ref[tiles - 1, own, :], (HALO * f + HALO) % LANES), last)
            first = pick(slot == f, roll(ref[0, own, :], HALO * f), first)
        pack_east[...] = last
        pack_west[...] = first

    def row_rims(main, sems, reach, skip=0):
        every, inner, n = pl.ds(0, main.shape[0]), pl.ds(0, tiles), reach - skip
        return remote(
            sems,
            (main.at[every, inner, pl.ds(top - reach, n), :], main.at[every, inner, pl.ds(core - reach, n), :], NORTH),
            (main.at[every, inner, pl.ds(core + skip, n), :], main.at[every, inner, pl.ds(top + skip, n), :], SOUTH),
        )

    def column_rims(pack_east, pack_west, from_west, from_east, sems):
        own_rows = pl.ds(HALO, rows)
        return remote(sems, (pack_east, from_west.at[own_rows, :], EAST), (pack_west, from_east.at[own_rows, :], WEST))

    def corner_rims(pack_east, pack_west, from_west, from_east, sems, reach, skip=0):
        n = reach - skip
        p_high, p_low = pl.ds(rows - reach, n), pl.ds(skip, n)
        d_low, d_high = pl.ds(HALO - reach, n), pl.ds(HALO + rows + skip, n)
        return remote(
            sems,
            (pack_east.at[p_high, :], from_west.at[d_low, :], NORTH_EAST),
            (pack_west.at[p_high, :], from_east.at[d_low, :], NORTH_WEST),
            (pack_east.at[p_low, :], from_west.at[d_high, :], SOUTH_EAST),
            (pack_west.at[p_low, :], from_east.at[d_high, :], SOUTH_WEST),
        )

    def rim_unpack(maps, from_west, from_east, start, n):
        easterly = lane_iota(n) < LANES // 2
        here = pl.ds(start - PAD, n)
        for f, ref in enumerate(maps):
            e = roll(from_east[here, :], (LANES - HALO * f) % LANES)
            w = roll(from_west[here, :], LANES - HALO - HALO * f)
            ref[halo_tile, pl.ds(start, n), :] = pick(easterly, e, w)

    def front(
        u_hbm, v_hbm, t_hbm, s_hbm, eta_hbm, tu_hbm, tv_hbm, depth_hbm, kmt_hbm, tide_hbm,
        us, vs, tm, sm, baro_out, corr, counts,
        u, v, p, gain_a, gain_b, cross, kmt_int, geo, thick, baro, force, coef, mean, depth_sum,
        pk_e, pk_w, rim_w, rim_e, cols, cols_e, cols_w, cols_in, first_row, last_row,
        row_n, row_s, corner_nw, corner_se, first_row4, last_row4, row_n4, row_s4, tide,
        load_sems, plane_sems, tide_sem, sem_near, sem_far, sem_baro, sem_uv, sem_p, sem_ts, sem_force, sem_star,
    ):
        k_map, depth_map = split(geo)
        eta_map, tu_map, tv_map = split(baro)
        dz_map, dzu_map, dzv_map = split(thick)
        k_out, ku_map, kv_map = split(counts)
        hu_map, hv_map = split(coef)
        fu_map, fv_map = split(force)
        mu_map, mv_map = split(mean)
        su_map, sv_map = split(depth_sum)
        pk_e1, pk_e2, pk_e3 = split(pk_e)
        pk_w1, pk_w2, pk_w3 = split(pk_w)
        rim_e1, rim_e2, rim_e3 = split(rim_e)
        rim_w1, rim_w2, rim_w3 = split(rim_w)
        zero = blank()
        lane = lane_iota(rows)
        low_half = lane < LANES // 2
        pair_of_lane, odd = lane // 2, lane % 2 == 1

        barrier = pltpu.get_barrier_semaphore()
        for way in COMPASS:
            pl.semaphore_signal(barrier, device_id=neighbour(way), device_id_type=pl.DeviceIdType.MESH)

        def plane_load(sems, src, dst):
            return [
                pltpu.make_async_copy(src.at[:, pl.ds(c * LANES, LANES)], dst(c), sems.at[c]) for c in range(tiles)
            ]

        def cube_tile(sems, src, dst, c):
            lanes = pl.ds(pl.multiple_of(c * LANES, LANES), LANES)
            return pltpu.make_async_copy(src.at[:, :, lanes], dst.at[c, :, body_rows, :], sems.at[c])

        def cube_load(sems, src, dst):
            return [cube_tile(sems, src, dst, c) for c in range(tiles)]

        sem_k, sem_h, sem_e, sem_tu, sem_tv = split(plane_sems)
        sem_t, sem_s, sem_u, sem_v = split(load_sems)
        geo_load = plane_load(sem_k, kmt_hbm, lambda c: kmt_int.at[c]) + plane_load(
            sem_h, depth_hbm, lambda c: depth_map.at[c, own, :]
        )
        baro_load = (
            plane_load(sem_e, eta_hbm, lambda c: eta_map.at[c, own, :])
            + plane_load(sem_tu, tu_hbm, lambda c: tu_map.at[c, own, :])
            + plane_load(sem_tv, tv_hbm, lambda c: tv_map.at[c, own, :])
        )
        tracer_load = []
        for c in range(tiles):
            tracer_load += [cube_tile(sem_t, t_hbm, tm, c), cube_tile(sem_s, s_hbm, sm, c)]
        flow_load = cube_load(sem_u, u_hbm, u) + cube_load(sem_v, v_hbm, v)
        tide_load = pltpu.make_async_copy(tide_hbm, tide, tide_sem)
        start_all(geo_load)
        start_all(tracer_load)
        start_all(flow_load)
        start_all(baro_load)
        tide_load.start()

        zero_rows = jnp.zeros((PAD, LANES), F32)
        for ref in (k_map, depth_map, dz_map, eta_map, tu_map, tv_map):
            for c in range(ring):
                ref[c, pl.ds(0, PAD), :] = zero_rows
                ref[c, pl.ds(flat_rows - PAD, PAD), :] = zero_rows
        for ref in (mu_map, mv_map):
            for c in range(ring):
                ref[c] = jnp.zeros((flat_rows, LANES), F32)

        wait_all(geo_load)
        for c in range(tiles):
            k_map[c, own, :] = kmt_int[c].astype(F32)
        rim_pack((k_map, depth_map), pk_e1, pk_w1)
        pl.semaphore_wait(barrier, len(COMPASS))
        near_rows, near_cols, near_corners = split(sem_near)
        near = row_rims(geo, near_rows, NEAR)
        near += column_rims(pk_e1, pk_w1, rim_w1, rim_e1, near_cols)
        near += corner_rims(pk_e1, pk_w1, rim_w1, rim_e1, near_corners, NEAR)
        start_all(near)

        rho_s, rho_t = 0.5 * BETA_S, 0.5 * ALPHA_T
        rho_0 = rho_t * T_REF - rho_s * S_REF

        def pressure_tile(c, _):
            k_cell = k_map[c, own, :]
            scale = (TIME_STEP * GRAVITY) * (depth_map[c, own, :] / jnp.maximum(k_cell, 1.0))

            def level(k, total):
                half = (rho_s * sm[c, k, body_rows, :] - rho_t * tm[c, k, body_rows, :]) + rho_0
                half = pick(real(k) < k_cell, half, zero)
                middle = total + half
                p[c, k, body_rows, :] = scale * middle
                return middle + half

            over_levels(level, zero)
            return _


        def tracer_tile(c, _):
            k_cell = k_map[c, own, :]
            dz = depth_map[c, own, :] / jnp.maximum(k_cell, 1.0)
            safe = pick(k_cell > 0, dz, 1.0)
            couple = (TIME_STEP * DIFF_KT) / (safe * safe)

            def down(k, carry):
                lower, keep, part_t, part_s = carry
                kf = real(k)
                wet = kf < k_cell
                upper = pick(kf + 1.0 < k_cell, couple, zero)
                turn = 1.0 + lower * keep
                inv = 1.0 / (turn + upper)
                gain_a[k] = upper * inv
                part_t = (pick(wet, tm[c, k, body_rows, :], zero) + lower * part_t) * inv
                part_s = (pick(wet, sm[c, k, body_rows, :], zero) + lower * part_s) * inv
                tm[c, k, body_rows, :] = part_t
                sm[c, k, body_rows, :] = part_s
                return upper, turn * inv, part_t, part_s

            over_levels(down, (zero, zero, zero, zero))

            def up(i, carry):
                below_t, below_s = carry
                k = levels - 1 - i
                gain = gain_a[k]
                below_t = tm[c, k, body_rows, :] + gain * below_t
                below_s = sm[c, k, body_rows, :] + gain * below_s
                tm[c, k, body_rows, :] = below_t
                sm[c, k, body_rows, :] = below_s
                return below_t, below_s

            over_levels(up, (zero, zero))
            return _

        def arrived(c):
            cube_tile(sem_t, t_hbm, tm, c).wait()
            cube_tile(sem_s, s_hbm, sm, c).wait()

        def both_passes(c, done):
            arrived(c)
            pressure_tile(c, 0)
            tracer_tile(c, 0)
            return done

        def pressure_pass(c, done):
            arrived(c)
            pressure_tile(c, 0)
            return done

        lax.fori_loop(0, tiles // 2, both_passes, 0)
        lax.fori_loop(tiles // 2, tiles, pressure_pass, 0)

        def edges(columns, top_rows, bottom_rows):
            def level(k, packed):
                row = pl.ds(k, 1)
                out = []
                for pair, acc in zip(columns, packed):
                    for f, ref in pair:
                        slot = SLOT * f + k
                        both = pick(low_half, ref[0, k, body_rows, :], ref[tiles - 1, k, body_rows, :])
                        acc = pick(pair_of_lane == slot, roll(both, 2 * slot + 1), acc)
                    out.append(acc)
                for c in range(tiles):
                    for ref, dst in top_rows:
                        dst[c, row, :] = ref[c, k, pl.ds(PAD, 1), :]
                    for ref, dst in bottom_rows:
                        dst[c, row, :] = ref[c, k, pl.ds(PAD + rows - 1, 1), :]
                return tuple(out)

            return over_levels(level, (zero,) * len(columns), EDGE_UNROLL)

        wait_all(flow_load)
        cols_uv, cols_p, cols_ts, cols_us = split(cols)
        east_uv, east_p, east_ts = split(cols_e)
        west_uv, west_ts, west_us = split(cols_w)
        fr_u, fr_v, fr_p = split(first_row)
        lr_u, lr_v = split(last_row)
        rn_u, rn_v, rn_p = split(row_n)
        rs_u, rs_v = split(row_s)
        (packed,) = edges((((0, u), (1, v)),), ((u, fr_u), (v, fr_v)), ((u, lr_u), (v, lr_v)))
        cols_uv[...] = packed
        two = pl.ds(0, 2)
        ex_uv = remote(
            sem_uv,
            (first_row.at[two], row_n.at[two], SOUTH),
            (last_row, row_s, NORTH),
            (cols_uv, east_uv, WEST),
            (cols_uv, west_uv, EAST),
            (cols_uv.at[pl.ds(0, PAD), :], corner_nw, SOUTH_EAST),
            (cols_uv.at[pl.ds(rows - PAD, PAD), :], corner_se, NORTH_WEST),
        )
        start_all(ex_uv)

        (packed,) = edges((((0, p),),), ((p, fr_p),), ())
        cols_p[...] = packed
        ex_p = remote(sem_p, (fr_p, rn_p, SOUTH), (cols_p, east_p, WEST))
        start_all(ex_p)

        wait_all(baro_load)
        rim_pack((eta_map, tu_map, tv_map), pk_e2, pk_w2)
        far_rows, far_corners = split(sem_far)
        baro_rows, baro_cols, baro_corners = split(sem_baro)
        far = row_rims(geo, far_rows, HALO, NEAR)
        far += corner_rims(pk_e1, pk_w1, rim_w1, rim_e1, far_corners, HALO, NEAR)
        far += row_rims(baro, baro_rows, HALO)
        far += column_rims(pk_e2, pk_w2, rim_w2, rim_e2, baro_cols)
        far += corner_rims(pk_e2, pk_w2, rim_w2, rim_e2, baro_corners, HALO)
        start_all(far)

        lax.fori_loop(tiles // 2, tiles, tracer_tile, 0)
        fr_t4, fr_s4 = split(first_row4)
        lr_t4, lr_s4, lr_v4 = split(last_row4)
        rn_t4, rn_s4 = split(row_n4)
        rs_t4, rs_s4, rs_v4 = split(row_s4)
        (packed,) = edges((((0, tm), (1, sm)),), ((tm, fr_t4), (sm, fr_s4)), ((tm, lr_t4), (sm, lr_s4)))
        cols_ts[...] = packed
        ex_ts = remote(
            sem_ts,
            (cols_ts, east_ts, WEST),
            (cols_ts, west_ts, EAST),
            (first_row4, row_n4, SOUTH),
            (last_row4.at[two], row_s4.at[two], NORTH),
        )
        start_all(ex_ts)

        row_index = lax.axis_index("row")

        def wall(low, n, inside):
            @pl.when(jnp.logical_not(inside))
            def _():
                for c in range(ring):
                    k_map[c, pl.ds(low, n), :] = jnp.zeros((n, LANES), F32)

        def thickness(start, n):
            here = pl.ds(start, n)
            for c in range(ring):
                dz_map[c, here, :] = depth_map[c, here, :] / jnp.maximum(k_map[c, here, :], 1.0)

        def faces(start, n):
            here, north = pl.ds(start, n), pl.ds(start + 1, n)
            k_cell = [k_map[c, here, :] for c in range(ring)]
            dz = [dz_map[c, here, :] for c in range(ring)]
            k_east, dz_east = east(k_cell), east(dz)
            for c in range(ring):
                k_u = jnp.minimum(k_cell[c], k_east[c])
                k_v = jnp.minimum(k_cell[c], k_map[c, north, :])
                dz_u = 0.5 * (dz[c] + dz_east[c])
                dz_v = 0.5 * (dz[c] + dz_map[c, north, :])
                k_out[c, here, :] = k_cell[c]
                ku_map[c, here, :] = k_u
                kv_map[c, here, :] = k_v
                dzu_map[c, here, :] = dz_u
                dzv_map[c, here, :] = dz_v
                hu_map[c, here, :] = (dt_sub * dt_sub) * (k_u * dz_u)
                hv_map[c, here, :] = (dt_sub * dt_sub) * (k_v * dz_v)

        def in_blocks(work, start, n, size=BLOCK):
            lax.fori_loop(0, n // size, lambda i, _: (work(pl.multiple_of(start + size * i, PAD), size), _)[1], 0)

        far_low, far_high, far_n = PAD, top + NEAR, HALO - NEAR
        wait_all(near)
        rim_unpack((k_map, depth_map), rim_w1, rim_e1, core - NEAR, rows + 2 * NEAR)
        wall(core - NEAR, NEAR, row_index > 0)
        wall(top, NEAR, row_index < n_rows - 1)
        in_blocks(thickness, core - NEAR, rows + 2 * NEAR)
        in_blocks(faces, core - PAD, rows + 2 * PAD)

        def mask_tile(c, _):
            for ref, count in ((u, ku_map), (v, kv_map)):
                k_face = count[c, own, :]

                def level(k, done, ref=ref, k_face=k_face):
                    ref[c, k, body_rows, :] = pick(real(k) < k_face, ref[c, k, body_rows, :], zero)
                    return done

                over_levels(level, 0)
            return _

        lax.fori_loop(0, tiles, mask_tile, 0)

        def fill(columns, norths, souths):
            def masked(x, k, count, tile, here):
                return x if count is None else pick(real(k) < count[tile, here, :], x, 0.0)

            def level(k, _):
                for ref, f, src, count in columns:
                    x = roll(src[...], LANES - 1 - 2 * (SLOT * f + k))
                    ref[halo_tile, k, body_rows, :] = masked(x, k, count, halo_tile, own)
                row = pl.ds(k, 1)
                for c in range(tiles):
                    for ref, src, count in norths:
                        x = masked(src[c, row, :], k, count, c, pl.ds(top, 1))
                        ref[c, k, pl.ds(PAD + rows, 1), :] = x
                    for ref, src, count in souths:
                        x = masked(src[c, row, :], k, count, c, pl.ds(core - 1, 1))
                        ref[c, k, pl.ds(PAD - 1, 1), :] = x
                return _

            over_levels(level, 0, EDGE_UNROLL)

        in_uv, in_ts = split(cols_in)
        wait_all(ex_uv)
        wait_all(ex_p)
        in_uv[...] = pick(odd, east_uv[...], west_uv[...])
        fill(
            ((u, 0, in_uv, ku_map), (v, 1, in_uv, kv_map), (p, 0, east_p, None)),
            ((u, rn_u, ku_map), (v, rn_v, kv_map), (p, rn_p, None)),
            ((u, rs_u, ku_map), (v, rs_v, kv_map)),
        )

        def corners(k, _):
            kf = real(k)
            x = roll(corner_nw[...], LANES - 1 - 2 * k)
            u[halo_tile, k, pl.ds(PAD + rows, PAD), :] = pick(kf < ku_map[halo_tile, pl.ds(top, PAD), :], x, 0.0)
            x = roll(corner_se[...], LANES - 1 - 2 * (SLOT + k))
            v[halo_tile, k, pl.ds(0, PAD), :] = pick(kf < kv_map[halo_tile, pl.ds(core - PAD, PAD), :], x, 0.0)
            return _

        over_levels(corners, 0, EDGE_UNROLL)

        quarter = 0.25 * TIME_STEP

        def momentum(k, _):
            tall, tall_north = pl.ds(0, PAD + rows), pl.ds(1, PAD + rows)
            here, north, south = body_rows, pl.ds(PAD + 1, rows), pl.ds(PAD - 1, rows)
            vv = [v[c, k, tall, :] for c in range(ring)]
            v_east = east(vv)
            for c in range(ring):
                cross[c, tall, :] = (vv[c] + v_east[c]) * (u[c, k, tall, :] + u[c, k, tall_north, :])
            uu = [u[c, k, here, :] for c in range(ring)]
            pp = [p[c, k, here, :] for c in range(ring)]
            centre = [x + y for x, y in zip(uu, west(uu))]
            centre = [scaled(quarter, x * x) + y for x, y in zip(centre, pp)]
            centre_east = east(centre)
            xx = [cross[c, here, :] for c in range(ring)]
            x_west = west(xx)
            for c in range(tiles):
                us[c, k, here, :] = uu[c] - (
                    (centre_east[c] - centre[c]) + scaled(quarter, xx[c] - cross[c, south, :])
                )
                vv = v[c, k, here, :]
                b_here = vv + v[c, k, north, :]
                b_south = vv + v[c, k, south, :]
                push = (b_here * b_here - b_south * b_south) + (xx[c] - x_west[c])
                vs[c, k, here, :] = vv - (scaled(quarter, push) + (p[c, k, north, :] - pp[c]))
            return _

        over_levels(momentum, 0, FLOW_UNROLL)

        nil = jnp.zeros((SOLVE_ROWS, LANES), F32)
        parts = rows // SOLVE_ROWS

        def solve_part(c, i):
            r = pl.multiple_of(i * SOLVE_ROWS, PAD)
            flat, here = pl.ds(core + r, SOLVE_ROWS), pl.ds(PAD + r, SOLVE_ROWS)
            faces = []
            for count, dz in ((ku_map, dzu_map), (kv_map, dzv_map)):
                k_face = count[c, flat, :]
                safe = pick(k_face > 0, dz[c, flat, :], 1.0)
                faces.append((k_face, (TIME_STEP * VISC_KV) / (safe * safe)))

            def down(k, carry):
                kf = real(k)
                out = []
                for face, ref, gain, state in zip(faces, (us, vs), (gain_a, gain_b), carry):
                    k_face, couple = face
                    lower, keep, part = state
                    upper = pick(kf + 1.0 < k_face, couple, nil)
                    turn = 1.0 + lower * keep
                    inv = 1.0 / (turn + upper)
                    gain[k, pl.ds(0, SOLVE_ROWS), :] = upper * inv
                    part = (pick(kf < k_face, ref[c, k, here, :], nil) + lower * part) * inv
                    ref[c, k, here, :] = part
                    out.append((upper, turn * inv, part))
                return tuple(out)

            over_levels(down, ((nil,) * 3,) * 2)

            def up(j, carry):
                k = levels - 1 - j
                out = []
                for ref, old, gain, state in zip((us, vs), (u, v), (gain_a, gain_b), carry):
                    below, total, change = state
                    below = ref[c, k, here, :] + gain[k, pl.ds(0, SOLVE_ROWS), :] * below
                    ref[c, k, here, :] = below
                    out.append((below, total + below, change + (below - old[c, k, here, :])))
                return tuple(out)

            sums = over_levels(up, ((nil,) * 3,) * 2)
            for dz, total_map, force_map, state in zip((dzu_map, dzv_map), (su_map, sv_map), (fu_map, fv_map), sums):
                _, total, change = state
                total_map[c, flat, :] = dz[c, flat, :] * total
                force_map[c, flat, :] = dz[c, flat, :] * change * (1.0 / TIME_STEP)

        force_rows, force_cols, force_corners = split(sem_force)
        low, high, both = pl.ds(core, HALO), pl.ds(top - HALO, HALO), pl.ds(0, 2)

        def solve_tiles(first, step):
            def work(i, done):
                solve_part(first + step * (i // parts), i % parts)
                return done

            lax.fori_loop(0, 2 * parts, work, 0)
            sent = []
            for c in (first, first + step):
                sent += remote(
                    force_rows.at[both, pl.ds(2 * c, 2)],
                    (force.at[both, c, high, :], force.at[both, c, pl.ds(PAD, HALO), :], NORTH),
                    (force.at[both, c, low, :], force.at[both, c, pl.ds(top, HALO), :], SOUTH),
                )
            return sent

        ex3 = solve_tiles(0, tiles - 1)
        rim_pack((fu_map, fv_map), pk_e3, pk_w3)
        ex3 += column_rims(pk_e3, pk_w3, rim_w3, rim_e3, force_cols)
        ex3 += corner_rims(pk_e3, pk_w3, rim_w3, rim_e3, force_corners, HALO)
        start_all(ex3)
        late = solve_tiles(1, 1)
        start_all(late)
        ex3 += late

        (packed,) = edges((((0, us),),), (), ((vs, lr_v4),))
        cols_us[...] = pick(pair_of_lane == levels, roll(su_map[tiles - 1, own, :], 2 * levels + 1), packed)
        for c in range(tiles):
            lr_v4[c, pl.ds(levels, 1), :] = sv_map[c, pl.ds(top - 1, 1), :]
        ex_star = remote(sem_star, (cols_us, west_us, EAST), (lr_v4, rs_v4, NORTH))
        start_all(ex_star)

        wait_all(ex_ts)
        in_ts[...] = pick(odd, east_ts[...], west_ts[...])
        fill(
            ((tm, 0, in_ts, None), (sm, 1, in_ts, None)),
            ((tm, rn_t4, None), (sm, rn_s4, None)),
            ((tm, rs_t4, None), (sm, rs_s4, None)),
        )

        wait_all(far)
        for start in (far_low, far_high):
            rim_unpack((k_map, depth_map), rim_w1, rim_e1, start, far_n)
        wall(far_low, far_n, row_index > 0)
        wall(far_high, far_n, row_index < n_rows - 1)
        in_blocks(thickness, far_low, far_n, PAD)
        in_blocks(thickness, far_high, far_n, PAD)
        in_blocks(faces, PAD, HALO - PAD, PAD)
        in_blocks(faces, top + PAD, HALO - PAD, PAD)
        full_n = rows + 2 * HALO
        rim_unpack((eta_map, tu_map, tv_map), rim_w2, rim_e2, PAD, full_n)

        def start_fields(start, n):
            here = pl.ds(start, n)
            for ref, count, unit in ((eta_map, k_out, 1.0), (tu_map, ku_map, dt_sub), (tv_map, kv_map, dt_sub)):
                for c in range(ring):
                    ref[c, here, :] = pick(count[c, here, :] > 0, scaled(unit, ref[c, here, :]), 0.0)

        in_blocks(start_fields, PAD, full_n)
        tide_load.wait()

        wait_all(ex3)
        rim_unpack((fu_map, fv_map), rim_w3, rim_e3, PAD, full_n)

        def force_fields(start, n):
            here = pl.ds(start, n)
            for ref, count in ((fu_map, ku_map), (fv_map, kv_map)):
                for c in range(ring):
                    ref[c, here, :] = pick(count[c, here, :] > 0, (dt_sub * dt_sub) * ref[c, here, :], 0.0)

        in_blocks(force_fields, PAD, full_n)

        def subcycle(low, high):
            chunks = [(r, min(SUB_ROWS, high - r)) for r in range(low, high, SUB_ROWS)]

            def body(n, _):
                tide_u, tide_v = tide[0, n], tide[1, n]
                weight = (weight_norm / dt_sub) * ((n + 1) * (n_sub - n)).astype(F32)
                for r, n_r in chunks:
                    here, south = pl.ds(r, n_r), pl.ds(r - 1, n_r)
                    tu = [tu_map[c, here, :] for c in range(ring)]
                    tu_west = west(tu)
                    for c in range(ring):
                        spread = (tu[c] - tu_west[c]) + (tv_map[c, here, :] - tv_map[c, south, :])
                        eta_map[c, here, :] = eta_map[c, here, :] - spread
                for r, n_r in chunks:
                    here, north = pl.ds(r, n_r), pl.ds(r + 1, n_r)
                    eta = [eta_map[c, here, :] for c in range(ring)]
                    eta_east = east(eta)
                    averaged = r + n_r > core - 1 and r < top
                    for c in range(ring):
                        drive = hu_map[c, here, :] * (tide_u - scaled(GRAVITY, eta_east[c] - eta[c]))
                        tu = tu_map[c, here, :] + (drive + fu_map[c, here, :])
                        tu_map[c, here, :] = tu
                        drive = hv_map[c, here, :] * (tide_v - scaled(GRAVITY, eta_map[c, north, :] - eta[c]))
                        tv = tv_map[c, here, :] + (drive + fv_map[c, here, :])
                        tv_map[c, here, :] = tv
                        if averaged:
                            mu_map[c, here, :] = mu_map[c, here, :] + weight * tu
                            if c < tiles:
                                mv_map[c, here, :] = mv_map[c, here, :] + weight * tv
                return _

            return body

        begin, margin = 0, 0
        while begin < n_sub:
            end = n_sub if margin + PAD >= HALO else min(n_sub, n_sub - (HALO - margin - PAD))
            if end > begin:
                lax.fori_loop(begin, end, subcycle(PAD + margin, flat_rows - PAD - margin), 0)
                begin = end
            margin += PAD

        for ref, out, unit in zip((eta_map, tu_map, tv_map), split(baro_out), (1.0, 1.0 / dt_sub, 1.0 / dt_sub)):
            for c in range(tiles):
                out[c] = scaled(unit, ref[c, own, :])

        wait_all(ex_star)
        fill(((us, 0, west_us, None),), (), ((vs, rs_v4, None),))
        su_map[halo_tile, own, :] = roll(west_us[...], LANES - 1 - 2 * levels)
        for c in range(tiles):
            sv_map[c, pl.ds(core - 1, 1), :] = rs_v4[c, pl.ds(levels, 1), :]
        cu_map, cv_map = split(corr)
        for out, mean_map, total_map, count, dz, n, here in (
            (cu_map, mu_map, su_map, ku_map, dzu_map, ring, own),
            (cv_map, mv_map, sv_map, kv_map, dzv_map, tiles, pl.ds(core - PAD, rows + PAD)),
        ):
            for c in range(n):
                depth = count[c, here, :] * dz[c, here, :]
                safe = pick(depth > 0, depth, 1.0)
                out[c, here, :] = (mean_map[c, here, :] - total_map[c, here, :]) / safe

    group = 4

    def back(us, vs, tm, sm, baro_in, corr, counts, eta_o, tu_o, tv_o, u_o, v_o, t_o, s_o, flux):
        k_map, ku_map, kv_map = split(counts)
        cu_map, cv_map = split(corr)
        fluxes = split(flux)
        for ref, out in zip(split(baro_in), (eta_o, tu_o, tv_o)):
            for c in range(tiles):
                out[:, pl.ds(c * LANES, LANES)] = ref[c]
        half = 0.5 * TIME_STEP

        def level(i, _):
            k = jnp.minimum(pl.program_id(0) * group + i, levels - 1)
            kf = k.astype(F32)
            for r in range(0, PAD + rows, PAD):
                here, north = pl.ds(r, PAD), pl.ds(r + 1, PAD)
                flat = pl.ds(r + core - PAD, PAD)
                for c in range(tiles):
                    vv = pick(kf < kv_map[c, flat, :], vs[c, k, here, :] + cv_map[c, flat, :], 0.0)
                    if r >= PAD:
                        v_o[i, pl.ds(r - PAD, PAD), pl.ds(c * LANES, LANES)] = vv
                    vv = half * vv
                    for ref, store in zip((tm, sm), fluxes):
                        store[c, here, :] = vv * (ref[c, k, here, :] + ref[c, k, north, :])
            here, south, flat = body_rows, pl.ds(PAD - 1, rows), own
            tracers = [[ref[c, k, here, :] for c in range(ring)] for ref in (tm, sm)]
            easts = [east(x) for x in tracers]
            uu = []
            for c in range(ring):
                x = pick(kf < ku_map[c, flat, :], us[c, k, here, :] + cu_map[c, flat, :], 0.0)
                if c < tiles:
                    u_o[i, :, pl.ds(c * LANES, LANES)] = x
                uu.append(half * x)
            fluxes_x = [[x * (y + z) for x, y, z in zip(uu, own_t, east_t)] for own_t, east_t in zip(tracers, easts)]
            wests = [west(x) for x in fluxes_x]
            for own_t, fx, fx_west, store, out in zip(tracers, fluxes_x, wests, fluxes, (t_o, s_o)):
                for c in range(tiles):
                    spread = (fx[c] - fx_west[c]) + (store[c, here, :] - store[c, south, :])
                    out[i, :, pl.ds(c * LANES, LANES)] = pick(kf < k_map[c, flat, :], own_t[c] - spread, 0.0)
            return _

        lax.fori_loop(0, group, level, 0)

    vmem = lambda *shape: pltpu.VMEM(shape, F32)
    flat = lambda n: vmem(n, ring, flat_rows, LANES)
    line = lambda n: vmem(n, tiles, SLOT, LANES)
    cube_buf = vmem(ring, levels, ext_rows, LANES)
    gain_buf = vmem(levels, rows, LANES)
    pack_buf = vmem(3, rows, LANES)
    rim_buf = vmem(3, rows + 2 * HALO, LANES)
    col_buf, corner_buf = vmem(rows, LANES), vmem(PAD, LANES)
    dma = lambda *shape: pltpu.SemaphoreType.DMA(shape)
    shared = [cube_buf, vmem(tiles, levels, ext_rows, LANES), cube_buf, cube_buf, vmem(3, tiles, rows, LANES), flat(2), flat(3)]
    routes = 6
    any_spec = pl.BlockSpec(memory_space=pl.ANY)
    vmem_spec = pl.BlockSpec(memory_space=pltpu.VMEM)
    front_call = pl.pallas_call(
        front,
        name="front",
        out_shape=shared,
        in_specs=[any_spec] * 10,
        out_specs=[vmem_spec] * len(shared),
        scratch_shapes=[
            cube_buf, cube_buf, cube_buf, gain_buf, vmem(levels, SOLVE_ROWS, LANES),
            vmem(ring, ext_rows, LANES), pltpu.VMEM((tiles, rows, LANES), jnp.int32),
            flat(2), flat(3), flat(3), flat(2), flat(2), flat(2), flat(2),
            pack_buf, pack_buf, rim_buf, rim_buf,
            vmem(4, rows, LANES), pack_buf, pack_buf, vmem(2, rows, LANES), line(3), line(2),
            line(3), line(2), corner_buf, corner_buf, line(2), line(3), line(2), line(3),
            pltpu.SMEM((2, n_sub), F32),
            dma(4, tiles), dma(5, tiles), pltpu.SemaphoreType.DMA,
            dma(3, 2, 4), dma(2, 2, 4), dma(3, 2, 4), dma(2, routes), dma(2, 2), dma(2, 4), dma(3, 2, 2 * tiles), dma(2, 2),
        ],
        compiler_params=pltpu.CompilerParams(
            collective_id=0, has_side_effects=True, vmem_limit_bytes=32 * MIB
        ),
    )
    plane_out = pl.BlockSpec((rows, cols), lambda i: (0, 0))
    cube_out = pl.BlockSpec((group, rows, cols), lambda i: (i, 0, 0))
    plane_shape = jax.ShapeDtypeStruct((rows, cols), F32)
    cube_shape = jax.ShapeDtypeStruct((levels, rows, cols), F32)
    back_call = pl.pallas_call(
        back,
        name="back",
        grid=(pl.cdiv(levels, group),),
        out_shape=[plane_shape] * 3 + [cube_shape] * 4,
        in_specs=[vmem_spec] * len(shared),
        out_specs=[plane_out] * 3 + [cube_out] * 4,
        scratch_shapes=[vmem(2, tiles, ext_rows, LANES)],
        compiler_params=pltpu.CompilerParams(vmem_limit_bytes=8 * MIB),
    )
    return front_call, back_call


def solution(mesh):
    def local_step(vel_u, vel_v, temperature, salinity, sea_level, trans_u, trans_v, bathymetry, kmt_levels, tide_force):
        levels, rows, cols = vel_u.shape
        front_call, back_call = kernels(mesh, levels, rows, cols, tide_force.shape[0])
        shared = front_call(
            vel_u, vel_v, temperature, salinity, sea_level, trans_u, trans_v, bathymetry, kmt_levels, tide_force.T
        )
        return tuple(back_call(*shared))

    spec_cube = P(None, "row", "col")
    spec_plane = P("row", "col")
    return jax.shard_map(
        local_step,
        mesh=mesh,
        in_specs=(spec_cube,) * 4 + (spec_plane,) * 5 + (P(None, None),),
        out_specs=(spec_plane,) * 3 + (spec_cube,) * 4,
        check_vma=False,
    )
```

```python
import jax
import jax.numpy as jnp
from jax import lax
from jax.experimental import pallas as pl
from jax.experimental.pallas import tpu as pltpu
from jax.sharding import PartitionSpec as P

GRAVITY = 1.0
TIME_STEP = 4.0
ALPHA_T = 0.02
BETA_S = 0.015
T_REF = 1.0
S_REF = 1.0
VISC_KV = 0.001
DIFF_KT = 0.0005

LANES = 128
HALO = 32
PAD = 8
NEAR = 16
F32 = jnp.float32
NORTH, SOUTH, EAST, WEST = (1, 0), (-1, 0), (0, 1), (0, -1)
NORTH_EAST, NORTH_WEST, SOUTH_EAST, SOUTH_WEST = (1, 1), (1, -1), (-1, 1), (-1, -1)
COMPASS = (NORTH, SOUTH, EAST, WEST, NORTH_EAST, NORTH_WEST, SOUTH_EAST, SOUTH_WEST)
SLOT = 32
BLOCK = 16
SOLVE_ROWS = 32
SUB_ROWS = 32
UNROLL = 2
EDGE_UNROLL = 3
FLOW_UNROLL = 4
MIB = 2**20


def kernels(mesh, levels, rows, cols, n_sub):
    n_cols, n_rows = mesh.shape["col"], mesh.shape["row"]
    tiles = cols // LANES
    ring = tiles + 1
    halo_tile = tiles
    ext_rows = rows + 2 * PAD
    flat_rows = rows + 2 * HALO + 2 * PAD
    core = PAD + HALO
    top = core + rows
    body_rows = pl.ds(PAD, rows)
    own = pl.ds(core, rows)
    dt_sub = TIME_STEP / n_sub
    weight_norm = 6.0 / (n_sub * (n_sub + 1) * (n_sub + 2))

    def lane_iota(n):
        return lax.broadcasted_iota(jnp.int32, (n, LANES), 1)

    def roll(x, shift):
        return pltpu.roll(x, shift, 1)

    def east(parts):
        last = lane_iota(parts[0].shape[0]) == LANES - 1
        moved = [roll(x, LANES - 1) for x in parts]
        return [pick(last, moved[(c + 1) % ring], moved[c]) for c in range(ring)]

    def west(parts):
        first = lane_iota(parts[0].shape[0]) == 0
        moved = [roll(x, 1) for x in parts]
        return [pick(first, moved[(c - 1) % ring], moved[c]) for c in range(ring)]

    def split(ref):
        return [ref.at[f] for f in range(ref.shape[0])]

    def scaled(factor, x):
        return x if factor == 1.0 else factor * x

    def real(k):
        return float(k) if isinstance(k, int) else k.astype(F32)

    def over_levels(body, carry, unroll=UNROLL):
        def trip(i, carry):
            for j in range(unroll):
                carry = body(unroll * i + j, carry)
            return carry

        carry = lax.fori_loop(0, levels // unroll, trip, carry)
        for k in range(levels - levels % unroll, levels):
            carry = body(k, carry)
        return carry

    def pick(condition, x, other):
        if jnp.ndim(condition) == 0:
            return jnp.where(condition, x, other)
        shape = condition.shape
        x = x if jnp.ndim(x) else jnp.full(shape, x, F32)
        other = other if jnp.ndim(other) else jnp.full(shape, other, F32)
        return lax.select(condition, x, other)

    def blank():
        return jnp.zeros((rows, LANES), F32)

    def neighbour(way):
        d_row, d_col = way
        row = lax.rem(lax.axis_index("row") + (d_row + n_rows), n_rows)
        col = lax.rem(lax.axis_index("col") + (d_col + n_cols), n_cols)
        return {"row": row, "col": col}

    def remote(sems, *routes):
        sent, arrived = split(sems)
        return [
            pltpu.make_async_remote_copy(
                src_ref=src,
                dst_ref=dst,
                send_sem=sent.at[index],
                recv_sem=arrived.at[index],
                device_id=neighbour(way),
                device_id_type=pl.DeviceIdType.MESH,
            )
            for index, (src, dst, way) in enumerate(routes)
        ]

    def start_all(copies):
        for copy in copies:
            copy.start()

    def wait_all(copies):
        for copy in copies:
            copy.wait()

    def rim_pack(maps, pack_east, pack_west):
        slot = lane_iota(rows) // HALO
        last, first = blank(), blank()
        for f, ref in enumerate(maps):
            last = pick(slot == f, roll(ref[tiles - 1, own, :], (HALO * f + HALO) % LANES), last)
            first = pick(slot == f, roll(ref[0, own, :], HALO * f), first)
        pack_east[...] = last
        pack_west[...] = first

    def row_rims(main, sems, reach, skip=0):
        every, inner, n = pl.ds(0, main.shape[0]), pl.ds(0, tiles), reach - skip
        return remote(
            sems,
            (main.at[every, inner, pl.ds(top - reach, n), :], main.at[every, inner, pl.ds(core - reach, n), :], NORTH),
            (main.at[every, inner, pl.ds(core + skip, n), :], main.at[every, inner, pl.ds(top + skip, n), :], SOUTH),
        )

    def column_rims(pack_east, pack_west, from_west, from_east, sems):
        own_rows = pl.ds(HALO, rows)
        return remote(sems, (pack_east, from_west.at[own_rows, :], EAST), (pack_west, from_east.at[own_rows, :], WEST))

    def corner_rims(pack_east, pack_west, from_west, from_east, sems, reach, skip=0):
        n = reach - skip
        p_high, p_low = pl.ds(rows - reach, n), pl.ds(skip, n)
        d_low, d_high = pl.ds(HALO - reach, n), pl.ds(HALO + rows + skip, n)
        return remote(
            sems,
            (pack_east.at[p_high, :], from_west.at[d_low, :], NORTH_EAST),
            (pack_west.at[p_high, :], from_east.at[d_low, :], NORTH_WEST),
            (pack_east.at[p_low, :], from_west.at[d_high, :], SOUTH_EAST),
            (pack_west.at[p_low, :], from_east.at[d_high, :], SOUTH_WEST),
        )

    def rim_unpack(maps, from_west, from_east, start, n):
        easterly = lane_iota(n) < LANES // 2
        here = pl.ds(start - PAD, n)
        for f, ref in enumerate(maps):
            e = roll(from_east[here, :], (LANES - HALO * f) % LANES)
            w = roll(from_west[here, :], LANES - HALO - HALO * f)
            ref[halo_tile, pl.ds(start, n), :] = pick(easterly, e, w)

    def front(
        u_hbm, v_hbm, t_hbm, s_hbm, eta_hbm, tu_hbm, tv_hbm, depth_hbm, kmt_hbm, tide_hbm,
        us, vs, tm, sm, baro_out, corr, counts,
        u, v, p, gain_a, gain_b, cross, kmt_int, geo, thick, baro, force, coef, mean, depth_sum,
        pk_e, pk_w, rim_w, rim_e, cols, cols_e, cols_w, cols_in, first_row, last_row,
        row_n, row_s, corner_nw, corner_se, first_row4, last_row4, row_n4, row_s4, tide,
        load_sems, plane_sems, tide_sem, sem_near, sem_far, sem_baro, sem_uv, sem_p, sem_ts, sem_force, sem_star,
    ):
        k_map, depth_map = split(geo)
        eta_map, tu_map, tv_map = split(baro)
        dz_map, dzu_map, dzv_map = split(thick)
        k_out, ku_map, kv_map = split(counts)
        hu_map, hv_map = split(coef)
        fu_map, fv_map = split(force)
        mu_map, mv_map = split(mean)
        su_map, sv_map = split(depth_sum)
        pk_e1, pk_e2, pk_e3 = split(pk_e)
        pk_w1, pk_w2, pk_w3 = split(pk_w)
        rim_e1, rim_e2, rim_e3 = split(rim_e)
        rim_w1, rim_w2, rim_w3 = split(rim_w)
        zero = blank()
        lane = lane_iota(rows)
        low_half = lane < LANES // 2
        pair_of_lane, odd = lane // 2, lane % 2 == 1

        barrier = pltpu.get_barrier_semaphore()
        for way in COMPASS:
            pl.semaphore_signal(barrier, device_id=neighbour(way), device_id_type=pl.DeviceIdType.MESH)

        def plane_load(sems, src, dst):
            return [
                pltpu.make_async_copy(src.at[:, pl.ds(c * LANES, LANES)], dst(c), sems.at[c]) for c in range(tiles)
            ]

        def cube_tile(sems, src, dst, c):
            lanes = pl.ds(pl.multiple_of(c * LANES, LANES), LANES)
            return pltpu.make_async_copy(src.at[:, :, lanes], dst.at[c, :, body_rows, :], sems.at[c])

        def cube_load(sems, src, dst):
            return [cube_tile(sems, src, dst, c) for c in range(tiles)]

        sem_k, sem_h, sem_e, sem_tu, sem_tv = split(plane_sems)
        sem_t, sem_s, sem_u, sem_v = split(load_sems)
        geo_load = plane_load(sem_k, kmt_hbm, lambda c: kmt_int.at[c]) + plane_load(
            sem_h, depth_hbm, lambda c: depth_map.at[c, own, :]
        )
        baro_load = (
            plane_load(sem_e, eta_hbm, lambda c: eta_map.at[c, own, :])
            + plane_load(sem_tu, tu_hbm, lambda c: tu_map.at[c, own, :])
            + plane_load(sem_tv, tv_hbm, lambda c: tv_map.at[c, own, :])
        )
        tracer_load = []
        for c in range(tiles):
            tracer_load += [cube_tile(sem_t, t_hbm, tm, c), cube_tile(sem_s, s_hbm, sm, c)]
        flow_load = cube_load(sem_u, u_hbm, u) + cube_load(sem_v, v_hbm, v)
        tide_load = pltpu.make_async_copy(tide_hbm, tide, tide_sem)
        start_all(geo_load)
        start_all(tracer_load)
        start_all(flow_load)
        start_all(baro_load)
        tide_load.start()

        zero_rows = jnp.zeros((PAD, LANES), F32)
        for ref in (k_map, depth_map, dz_map, eta_map, tu_map, tv_map):
            for c in range(ring):
                ref[c, pl.ds(0, PAD), :] = zero_rows
                ref[c, pl.ds(flat_rows - PAD, PAD), :] = zero_rows
        for ref in (mu_map, mv_map):
            for c in range(ring):
                ref[c] = jnp.zeros((flat_rows, LANES), F32)

        wait_all(geo_load)
        for c in range(tiles):
            k_map[c, own, :] = kmt_int[c].astype(F32)
        rim_pack((k_map, depth_map), pk_e1, pk_w1)

        rho_s, rho_t = 0.5 * BETA_S, 0.5 * ALPHA_T
        rho_0 = rho_t * T_REF - rho_s * S_REF

        def pressure_tile(c, _):
            k_cell = k_map[c, own, :]
            scale = (TIME_STEP * GRAVITY) * (depth_map[c, own, :] / jnp.maximum(k_cell, 1.0))

            def level(k, total):
                half = (rho_s * sm[c, k, body_rows, :] - rho_t * tm[c, k, body_rows, :]) + rho_0
                half = pick(real(k) < k_cell, half, zero)
                middle = total + half
                p[c, k, body_rows, :] = scale * middle
                return middle + half

            over_levels(level, zero)
            return _


        def tracer_tile(c, _):
            k_cell = k_map[c, own, :]
            dz = depth_map[c, own, :] / jnp.maximum(k_cell, 1.0)
            safe = pick(k_cell > 0, dz, 1.0)
            couple = (TIME_STEP * DIFF_KT) / (safe * safe)

            def down(k, carry):
                lower, keep, part_t, part_s = carry
                kf = real(k)
                wet = kf < k_cell
                upper = pick(kf + 1.0 < k_cell, couple, zero)
                turn = 1.0 + lower * keep
                inv = 1.0 / (turn + upper)
                gain_a[k] = upper * inv
                part_t = (pick(wet, tm[c, k, body_rows, :], zero) + lower * part_t) * inv
                part_s = (pick(wet, sm[c, k, body_rows, :], zero) + lower * part_s) * inv
                tm[c, k, body_rows, :] = part_t
                sm[c, k, body_rows, :] = part_s
                return upper, turn * inv, part_t, part_s

            over_levels(down, (zero, zero, zero, zero))

            def up(i, carry):
                below_t, below_s = carry
                k = levels - 1 - i
                gain = gain_a[k]
                below_t = tm[c, k, body_rows, :] + gain * below_t
                below_s = sm[c, k, body_rows, :] + gain * below_s
                tm[c, k, body_rows, :] = below_t
                sm[c, k, body_rows, :] = below_s
                return below_t, below_s

            over_levels(up, (zero, zero))
            return _

        def arrived(c):
            cube_tile(sem_t, t_hbm, tm, c).wait()
            cube_tile(sem_s, s_hbm, sm, c).wait()

        def both_passes(c, done):
            arrived(c)
            pressure_tile(c, 0)
            tracer_tile(c, 0)
            return done

        def pressure_pass(c, done):
            arrived(c)
            pressure_tile(c, 0)
            return done

        lax.fori_loop(0, tiles // 2, both_passes, 0)
        lax.fori_loop(tiles // 2, tiles, pressure_pass, 0)

        pl.semaphore_wait(barrier, len(COMPASS))
        near_rows, near_cols, near_corners = split(sem_near)
        near = row_rims(geo, near_rows, NEAR)
        near += column_rims(pk_e1, pk_w1, rim_w1, rim_e1, near_cols)
        near += corner_rims(pk_e1, pk_w1, rim_w1, rim_e1, near_corners, NEAR)
        start_all(near)

        def edges(columns, top_rows, bottom_rows):
            def level(k, packed):
                row = pl.ds(k, 1)
                out = []
                for pair, acc in zip(columns, packed):
                    for f, ref in pair:
                        slot = SLOT * f + k
                        both = pick(low_half, ref[0, k, body_rows, :], ref[tiles - 1, k, body_rows, :])
                        acc = pick(pair_of_lane == slot, roll(both, 2 * slot + 1), acc)
                    out.append(acc)
                for c in range(tiles):
                    for ref, dst in top_rows:
                        dst[c, row, :] = ref[c, k, pl.ds(PAD, 1), :]
                    for ref, dst in bottom_rows:
                        dst[c, row, :] = ref[c, k, pl.ds(PAD + rows - 1, 1), :]
                return tuple(out)

            return over_levels(level, (zero,) * len(columns), EDGE_UNROLL)

        wait_all(flow_load)
        cols_uv, cols_p, cols_ts, cols_us = split(cols)
        east_uv, east_p, east_ts = split(cols_e)
        west_uv, west_ts, west_us = split(cols_w)
        fr_u, fr_v, fr_p = split(first_row)
        lr_u, lr_v = split(last_row)
        rn_u, rn_v, rn_p = split(row_n)
        rs_u, rs_v = split(row_s)
        (packed,) = edges((((0, u), (1, v)),), ((u, fr_u), (v, fr_v)), ((u, lr_u), (v, lr_v)))
        cols_uv[...] = packed
        two = pl.ds(0, 2)
        ex_uv = remote(
            sem_uv,
            (first_row.at[two], row_n.at[two], SOUTH),
            (last_row, row_s, NORTH),
            (cols_uv, east_uv, WEST),
            (cols_uv, west_uv, EAST),
            (cols_uv.at[pl.ds(0, PAD), :], corner_nw, SOUTH_EAST),
            (cols_uv.at[pl.ds(rows - PAD, PAD), :], corner_se, NORTH_WEST),
        )
        start_all(ex_uv)

        (packed,) = edges((((0, p),),), ((p, fr_p),), ())
        cols_p[...] = packed
        ex_p = remote(sem_p, (fr_p, rn_p, SOUTH), (cols_p, east_p, WEST))
        start_all(ex_p)

        wait_all(baro_load)
        rim_pack((eta_map, tu_map, tv_map), pk_e2, pk_w2)
        far_rows, far_corners = split(sem_far)
        baro_rows, baro_cols, baro_corners = split(sem_baro)
        far = row_rims(geo, far_rows, HALO, NEAR)
        far += corner_rims(pk_e1, pk_w1, rim_w1, rim_e1, far_corners, HALO, NEAR)
        far += row_rims(baro, baro_rows, HALO)
        far += column_rims(pk_e2, pk_w2, rim_w2, rim_e2, baro_cols)
        far += corner_rims(pk_e2, pk_w2, rim_w2, rim_e2, baro_corners, HALO)
        start_all(far)

        lax.fori_loop(tiles // 2, tiles, tracer_tile, 0)
        fr_t4, fr_s4 = split(first_row4)
        lr_t4, lr_s4, lr_v4 = split(last_row4)
        rn_t4, rn_s4 = split(row_n4)
        rs_t4, rs_s4, rs_v4 = split(row_s4)
        (packed,) = edges((((0, tm), (1, sm)),), ((tm, fr_t4), (sm, fr_s4)), ((tm, lr_t4), (sm, lr_s4)))
        cols_ts[...] = packed
        ex_ts = remote(
            sem_ts,
            (cols_ts, east_ts, WEST),
            (cols_ts, west_ts, EAST),
            (first_row4, row_n4, SOUTH),
            (last_row4.at[two], row_s4.at[two], NORTH),
        )
        start_all(ex_ts)

        row_index = lax.axis_index("row")

        def wall(low, n, inside):
            @pl.when(jnp.logical_not(inside))
            def _():
                for c in range(ring):
                    k_map[c, pl.ds(low, n), :] = jnp.zeros((n, LANES), F32)

        def thickness(start, n):
            here = pl.ds(start, n)
            for c in range(ring):
                dz_map[c, here, :] = depth_map[c, here, :] / jnp.maximum(k_map[c, here, :], 1.0)

        def faces(start, n):
            here, north = pl.ds(start, n), pl.ds(start + 1, n)
            k_cell = [k_map[c, here, :] for c in range(ring)]
            dz = [dz_map[c, here, :] for c in range(ring)]
            k_east, dz_east = east(k_cell), east(dz)
            for c in range(ring):
                k_u = jnp.minimum(k_cell[c], k_east[c])
                k_v = jnp.minimum(k_cell[c], k_map[c, north, :])
                dz_u = 0.5 * (dz[c] + dz_east[c])
                dz_v = 0.5 * (dz[c] + dz_map[c, north, :])
                k_out[c, here, :] = k_cell[c]
                ku_map[c, here, :] = k_u
                kv_map[c, here, :] = k_v
                dzu_map[c, here, :] = dz_u
                dzv_map[c, here, :] = dz_v
                hu_map[c, here, :] = (dt_sub * dt_sub) * (k_u * dz_u)
                hv_map[c, here, :] = (dt_sub * dt_sub) * (k_v * dz_v)

        def in_blocks(work, start, n, size=BLOCK):
            lax.fori_loop(0, n // size, lambda i, _: (work(pl.multiple_of(start + size * i, PAD), size), _)[1], 0)

        far_low, far_high, far_n = PAD, top + NEAR, HALO - NEAR
        wait_all(near)
        rim_unpack((k_map, depth_map), rim_w1, rim_e1, core - NEAR, rows + 2 * NEAR)
        wall(core - NEAR, NEAR, row_index > 0)
        wall(top, NEAR, row_index < n_rows - 1)
        in_blocks(thickness, core - NEAR, rows + 2 * NEAR)
        in_blocks(faces, core - PAD, rows + 2 * PAD)

        def mask_tile(c, _):
            for ref, count in ((u, ku_map), (v, kv_map)):
                k_face = count[c, own, :]

                def level(k, done, ref=ref, k_face=k_face):
                    ref[c, k, body_rows, :] = pick(real(k) < k_face, ref[c, k, body_rows, :], zero)
                    return done

                over_levels(level, 0)
            return _

        lax.fori_loop(0, tiles, mask_tile, 0)

        def fill(columns, norths, souths):
            def masked(x, k, count, tile, here):
                return x if count is None else pick(real(k) < count[tile, here, :], x, 0.0)

            def level(k, _):
                for ref, f, src, count in columns:
                    x = roll(src[...], LANES - 1 - 2 * (SLOT * f + k))
                    ref[halo_tile, k, body_rows, :] = masked(x, k, count, halo_tile, own)
                row = pl.ds(k, 1)
                for c in range(tiles):
                    for ref, src, count in norths:
                        x = masked(src[c, row, :], k, count, c, pl.ds(top, 1))
                        ref[c, k, pl.ds(PAD + rows, 1), :] = x
                    for ref, src, count in souths:
                        x = masked(src[c, row, :], k, count, c, pl.ds(core - 1, 1))
                        ref[c, k, pl.ds(PAD - 1, 1), :] = x
                return _

            over_levels(level, 0, EDGE_UNROLL)

        in_uv, in_ts = split(cols_in)
        wait_all(ex_uv)
        wait_all(ex_p)
        in_uv[...] = pick(odd, east_uv[...], west_uv[...])
        fill(
            ((u, 0, in_uv, ku_map), (v, 1, in_uv, kv_map), (p, 0, east_p, None)),
            ((u, rn_u, ku_map), (v, rn_v, kv_map), (p, rn_p, None)),
            ((u, rs_u, ku_map), (v, rs_v, kv_map)),
        )

        def corners(k, _):
            kf = real(k)
            x = roll(corner_nw[...], LANES - 1 - 2 * k)
            u[halo_tile, k, pl.ds(PAD + rows, PAD), :] = pick(kf < ku_map[halo_tile, pl.ds(top, PAD), :], x, 0.0)
            x = roll(corner_se[...], LANES - 1 - 2 * (SLOT + k))
            v[halo_tile, k, pl.ds(0, PAD), :] = pick(kf < kv_map[halo_tile, pl.ds(core - PAD, PAD), :], x, 0.0)
            return _

        over_levels(corners, 0, EDGE_UNROLL)

        quarter = 0.25 * TIME_STEP

        def momentum(k, _):
            tall, tall_north = pl.ds(0, PAD + rows), pl.ds(1, PAD + rows)
            here, north, south = body_rows, pl.ds(PAD + 1, rows), pl.ds(PAD - 1, rows)
            vv = [v[c, k, tall, :] for c in range(ring)]
            v_east = east(vv)
            for c in range(ring):
                cross[c, tall, :] = (vv[c] + v_east[c]) * (u[c, k, tall, :] + u[c, k, tall_north, :])
            uu = [u[c, k, here, :] for c in range(ring)]
            pp = [p[c, k, here, :] for c in range(ring)]
            centre = [x + y for x, y in zip(uu, west(uu))]
            centre = [scaled(quarter, x * x) + y for x, y in zip(centre, pp)]
            centre_east = east(centre)
            xx = [cross[c, here, :] for c in range(ring)]
            x_west = west(xx)
            for c in range(tiles):
                us[c, k, here, :] = uu[c] - (
                    (centre_east[c] - centre[c]) + scaled(quarter, xx[c] - cross[c, south, :])
                )
                vv = v[c, k, here, :]
                b_here = vv + v[c, k, north, :]
                b_south = vv + v[c, k, south, :]
                push = (b_here * b_here - b_south * b_south) + (xx[c] - x_west[c])
                vs[c, k, here, :] = vv - (scaled(quarter, push) + (p[c, k, north, :] - pp[c]))
            return _

        over_levels(momentum, 0, FLOW_UNROLL)

        nil = jnp.zeros((SOLVE_ROWS, LANES), F32)
        parts = rows // SOLVE_ROWS

        def solve_part(c, i):
            r = pl.multiple_of(i * SOLVE_ROWS, PAD)
            flat, here = pl.ds(core + r, SOLVE_ROWS), pl.ds(PAD + r, SOLVE_ROWS)
            faces = []
            for count, dz in ((ku_map, dzu_map), (kv_map, dzv_map)):
                k_face = count[c, flat, :]
                safe = pick(k_face > 0, dz[c, flat, :], 1.0)
                faces.append((k_face, (TIME_STEP * VISC_KV) / (safe * safe)))

            def down(k, carry):
                kf = real(k)
                out = []
                for face, ref, gain, state in zip(faces, (us, vs), (gain_a, gain_b), carry):
                    k_face, couple = face
                    lower, keep, part = state
                    upper = pick(kf + 1.0 < k_face, couple, nil)
                    turn = 1.0 + lower * keep
                    inv = 1.0 / (turn + upper)
                    gain[k, pl.ds(0, SOLVE_ROWS), :] = upper * inv
                    part = (pick(kf < k_face, ref[c, k, here, :], nil) + lower * part) * inv
                    ref[c, k, here, :] = part
                    out.append((upper, turn * inv, part))
                return tuple(out)

            over_levels(down, ((nil,) * 3,) * 2)

            def up(j, carry):
                k = levels - 1 - j
                out = []
                for ref, old, gain, state in zip((us, vs), (u, v), (gain_a, gain_b), carry):
                    below, total, change = state
                    below = ref[c, k, here, :] + gain[k, pl.ds(0, SOLVE_ROWS), :] * below
                    ref[c, k, here, :] = below
                    out.append((below, total + below, change + (below - old[c, k, here, :])))
                return tuple(out)

            sums = over_levels(up, ((nil,) * 3,) * 2)
            for dz, total_map, force_map, state in zip((dzu_map, dzv_map), (su_map, sv_map), (fu_map, fv_map), sums):
                _, total, change = state
                total_map[c, flat, :] = dz[c, flat, :] * total
                force_map[c, flat, :] = dz[c, flat, :] * change * (1.0 / TIME_STEP)

        force_rows, force_cols, force_corners = split(sem_force)
        low, high, both = pl.ds(core, HALO), pl.ds(top - HALO, HALO), pl.ds(0, 2)

        def solve_tiles(first, step):
            def work(i, done):
                solve_part(first + step * (i // parts), i % parts)
                return done

            lax.fori_loop(0, 2 * parts, work, 0)
            sent = []
            for c in (first, first + step):
                sent += remote(
                    force_rows.at[both, pl.ds(2 * c, 2)],
                    (force.at[both, c, high, :], force.at[both, c, pl.ds(PAD, HALO), :], NORTH),
                    (force.at[both, c, low, :], force.at[both, c, pl.ds(top, HALO), :], SOUTH),
                )
            return sent

        ex3 = solve_tiles(0, tiles - 1)
        rim_pack((fu_map, fv_map), pk_e3, pk_w3)
        ex3 += column_rims(pk_e3, pk_w3, rim_w3, rim_e3, force_cols)
        ex3 += corner_rims(pk_e3, pk_w3, rim_w3, rim_e3, force_corners, HALO)
        start_all(ex3)
        late = solve_tiles(1, 1)
        start_all(late)
        ex3 += late

        (packed,) = edges((((0, us),),), (), ((vs, lr_v4),))
        cols_us[...] = pick(pair_of_lane == levels, roll(su_map[tiles - 1, own, :], 2 * levels + 1), packed)
        for c in range(tiles):
            lr_v4[c, pl.ds(levels, 1), :] = sv_map[c, pl.ds(top - 1, 1), :]
        ex_star = remote(sem_star, (cols_us, west_us, EAST), (lr_v4, rs_v4, NORTH))
        start_all(ex_star)

        wait_all(ex_ts)
        in_ts[...] = pick(odd, east_ts[...], west_ts[...])
        fill(
            ((tm, 0, in_ts, None), (sm, 1, in_ts, None)),
            ((tm, rn_t4, None), (sm, rn_s4, None)),
            ((tm, rs_t4, None), (sm, rs_s4, None)),
        )

        wait_all(far)
        for start in (far_low, far_high):
            rim_unpack((k_map, depth_map), rim_w1, rim_e1, start, far_n)
        wall(far_low, far_n, row_index > 0)
        wall(far_high, far_n, row_index < n_rows - 1)
        in_blocks(thickness, far_low, far_n, PAD)
        in_blocks(thickness, far_high, far_n, PAD)
        in_blocks(faces, PAD, HALO - PAD, PAD)
        in_blocks(faces, top + PAD, HALO - PAD, PAD)
        full_n = rows + 2 * HALO
        rim_unpack((eta_map, tu_map, tv_map), rim_w2, rim_e2, PAD, full_n)

        def start_fields(start, n):
            here = pl.ds(start, n)
            for ref, count, unit in ((eta_map, k_out, 1.0), (tu_map, ku_map, dt_sub), (tv_map, kv_map, dt_sub)):
                for c in range(ring):
                    ref[c, here, :] = pick(count[c, here, :] > 0, scaled(unit, ref[c, here, :]), 0.0)

        in_blocks(start_fields, PAD, full_n)
        tide_load.wait()

        wait_all(ex3)
        rim_unpack((fu_map, fv_map), rim_w3, rim_e3, PAD, full_n)

        def force_fields(start, n):
            here = pl.ds(start, n)
            for ref, count in ((fu_map, ku_map), (fv_map, kv_map)):
                for c in range(ring):
                    ref[c, here, :] = pick(count[c, here, :] > 0, (dt_sub * dt_sub) * ref[c, here, :], 0.0)

        in_blocks(force_fields, PAD, full_n)

        def subcycle(low, high):
            chunks = [(r, min(SUB_ROWS, high - r)) for r in range(low, high, SUB_ROWS)]

            def body(n, _):
                tide_u, tide_v = tide[0, n], tide[1, n]
                weight = (weight_norm / dt_sub) * ((n + 1) * (n_sub - n)).astype(F32)
                for r, n_r in chunks:
                    here, south = pl.ds(r, n_r), pl.ds(r - 1, n_r)
                    tu = [tu_map[c, here, :] for c in range(ring)]
                    tu_west = west(tu)
                    for c in range(ring):
                        spread = (tu[c] - tu_west[c]) + (tv_map[c, here, :] - tv_map[c, south, :])
                        eta_map[c, here, :] = eta_map[c, here, :] - spread
                for r, n_r in chunks:
                    here, north = pl.ds(r, n_r), pl.ds(r + 1, n_r)
                    eta = [eta_map[c, here, :] for c in range(ring)]
                    eta_east = east(eta)
                    averaged = r + n_r > core - 1 and r < top
                    for c in range(ring):
                        drive = hu_map[c, here, :] * (tide_u - scaled(GRAVITY, eta_east[c] - eta[c]))
                        tu = tu_map[c, here, :] + (drive + fu_map[c, here, :])
                        tu_map[c, here, :] = tu
                        drive = hv_map[c, here, :] * (tide_v - scaled(GRAVITY, eta_map[c, north, :] - eta[c]))
                        tv = tv_map[c, here, :] + (drive + fv_map[c, here, :])
                        tv_map[c, here, :] = tv
                        if averaged:
                            mu_map[c, here, :] = mu_map[c, here, :] + weight * tu
                            if c < tiles:
                                mv_map[c, here, :] = mv_map[c, here, :] + weight * tv
                return _

            return body

        begin, margin = 0, 0
        while begin < n_sub:
            end = n_sub if margin + PAD >= HALO else min(n_sub, n_sub - (HALO - margin - PAD))
            if end > begin:
                lax.fori_loop(begin, end, subcycle(PAD + margin, flat_rows - PAD - margin), 0)
                begin = end
            margin += PAD

        for ref, out, unit in zip((eta_map, tu_map, tv_map), split(baro_out), (1.0, 1.0 / dt_sub, 1.0 / dt_sub)):
            for c in range(tiles):
                out[c] = scaled(unit, ref[c, own, :])

        wait_all(ex_star)
        fill(((us, 0, west_us, None),), (), ((vs, rs_v4, None),))
        su_map[halo_tile, own, :] = roll(west_us[...], LANES - 1 - 2 * levels)
        for c in range(tiles):
            sv_map[c, pl.ds(core - 1, 1), :] = rs_v4[c, pl.ds(levels, 1), :]
        cu_map, cv_map = split(corr)
        for out, mean_map, total_map, count, dz, n, here in (
            (cu_map, mu_map, su_map, ku_map, dzu_map, ring, own),
            (cv_map, mv_map, sv_map, kv_map, dzv_map, tiles, pl.ds(core - PAD, rows + PAD)),
        ):
            for c in range(n):
                depth = count[c, here, :] * dz[c, here, :]
                safe = pick(depth > 0, depth, 1.0)
                out[c, here, :] = (mean_map[c, here, :] - total_map[c, here, :]) / safe

    group = 4

    def back(us, vs, tm, sm, baro_in, corr, counts, eta_o, tu_o, tv_o, u_o, v_o, t_o, s_o, flux):
        k_map, ku_map, kv_map = split(counts)
        cu_map, cv_map = split(corr)
        fluxes = split(flux)
        for ref, out in zip(split(baro_in), (eta_o, tu_o, tv_o)):
            for c in range(tiles):
                out[:, pl.ds(c * LANES, LANES)] = ref[c]
        half = 0.5 * TIME_STEP

        def level(i, _):
            k = jnp.minimum(pl.program_id(0) * group + i, levels - 1)
            kf = k.astype(F32)
            for r in range(0, PAD + rows, PAD):
                here, north = pl.ds(r, PAD), pl.ds(r + 1, PAD)
                flat = pl.ds(r + core - PAD, PAD)
                for c in range(tiles):
                    vv = pick(kf < kv_map[c, flat, :], vs[c, k, here, :] + cv_map[c, flat, :], 0.0)
                    if r >= PAD:
                        v_o[i, pl.ds(r - PAD, PAD), pl.ds(c * LANES, LANES)] = vv
                    vv = half * vv
                    for ref, store in zip((tm, sm), fluxes):
                        store[c, here, :] = vv * (ref[c, k, here, :] + ref[c, k, north, :])
            here, south, flat = body_rows, pl.ds(PAD - 1, rows), own
            tracers = [[ref[c, k, here, :] for c in range(ring)] for ref in (tm, sm)]
            easts = [east(x) for x in tracers]
            uu = []
            for c in range(ring):
                x = pick(kf < ku_map[c, flat, :], us[c, k, here, :] + cu_map[c, flat, :], 0.0)
                if c < tiles:
                    u_o[i, :, pl.ds(c * LANES, LANES)] = x
                uu.append(half * x)
            fluxes_x = [[x * (y + z) for x, y, z in zip(uu, own_t, east_t)] for own_t, east_t in zip(tracers, easts)]
            wests = [west(x) for x in fluxes_x]
            for own_t, fx, fx_west, store, out in zip(tracers, fluxes_x, wests, fluxes, (t_o, s_o)):
                for c in range(tiles):
                    spread = (fx[c] - fx_west[c]) + (store[c, here, :] - store[c, south, :])
                    out[i, :, pl.ds(c * LANES, LANES)] = pick(kf < k_map[c, flat, :], own_t[c] - spread, 0.0)
            return _

        lax.fori_loop(0, group, level, 0)

    vmem = lambda *shape: pltpu.VMEM(shape, F32)
    flat = lambda n: vmem(n, ring, flat_rows, LANES)
    line = lambda n: vmem(n, tiles, SLOT, LANES)
    cube_buf = vmem(ring, levels, ext_rows, LANES)
    gain_buf = vmem(levels, rows, LANES)
    pack_buf = vmem(3, rows, LANES)
    rim_buf = vmem(3, rows + 2 * HALO, LANES)
    col_buf, corner_buf = vmem(rows, LANES), vmem(PAD, LANES)
    dma = lambda *shape: pltpu.SemaphoreType.DMA(shape)
    shared = [cube_buf, vmem(tiles, levels, ext_rows, LANES), cube_buf, cube_buf, vmem(3, tiles, rows, LANES), flat(2), flat(3)]
    routes = 6
    any_spec = pl.BlockSpec(memory_space=pl.ANY)
    vmem_spec = pl.BlockSpec(memory_space=pltpu.VMEM)
    front_call = pl.pallas_call(
        front,
        name="front",
        out_shape=shared,
        in_specs=[any_spec] * 10,
        out_specs=[vmem_spec] * len(shared),
        scratch_shapes=[
            cube_buf, cube_buf, cube_buf, gain_buf, vmem(levels, SOLVE_ROWS, LANES),
            vmem(ring, ext_rows, LANES), pltpu.VMEM((tiles, rows, LANES), jnp.int32),
            flat(2), flat(3), flat(3), flat(2), flat(2), flat(2), flat(2),
            pack_buf, pack_buf, rim_buf, rim_buf,
            vmem(4, rows, LANES), pack_buf, pack_buf, vmem(2, rows, LANES), line(3), line(2),
            line(3), line(2), corner_buf, corner_buf, line(2), line(3), line(2), line(3),
            pltpu.SMEM((2, n_sub), F32),
            dma(4, tiles), dma(5, tiles), pltpu.SemaphoreType.DMA,
            dma(3, 2, 4), dma(2, 2, 4), dma(3, 2, 4), dma(2, routes), dma(2, 2), dma(2, 4), dma(3, 2, 2 * tiles), dma(2, 2),
        ],
        compiler_params=pltpu.CompilerParams(
            collective_id=0, has_side_effects=True, vmem_limit_bytes=32 * MIB
        ),
    )
    plane_out = pl.BlockSpec((rows, cols), lambda i: (0, 0))
    cube_out = pl.BlockSpec((group, rows, cols), lambda i: (i, 0, 0))
    plane_shape = jax.ShapeDtypeStruct((rows, cols), F32)
    cube_shape = jax.ShapeDtypeStruct((levels, rows, cols), F32)
    back_call = pl.pallas_call(
        back,
        name="back",
        grid=(pl.cdiv(levels, group),),
        out_shape=[plane_shape] * 3 + [cube_shape] * 4,
        in_specs=[vmem_spec] * len(shared),
        out_specs=[plane_out] * 3 + [cube_out] * 4,
        scratch_shapes=[vmem(2, tiles, ext_rows, LANES)],
        compiler_params=pltpu.CompilerParams(vmem_limit_bytes=8 * MIB),
    )
    return front_call, back_call


def solution(mesh):
    def local_step(vel_u, vel_v, temperature, salinity, sea_level, trans_u, trans_v, bathymetry, kmt_levels, tide_force):
        levels, rows, cols = vel_u.shape
        front_call, back_call = kernels(mesh, levels, rows, cols, tide_force.shape[0])
        shared = front_call(
            vel_u, vel_v, temperature, salinity, sea_level, trans_u, trans_v, bathymetry, kmt_levels, tide_force.T
        )
        return tuple(back_call(*shared))

    spec_cube = P(None, "row", "col")
    spec_plane = P("row", "col")
    return jax.shard_map(
        local_step,
        mesh=mesh,
        in_specs=(spec_cube,) * 4 + (spec_plane,) * 5 + (P(None, None),),
        out_specs=(spec_plane,) * 3 + (spec_cube,) * 4,
        check_vma=False,
    )
```

```python
import jax
import jax.numpy as jnp
from jax import lax
from jax.experimental import pallas as pl
from jax.experimental.pallas import tpu as pltpu
from jax.sharding import PartitionSpec as P

GRAVITY = 1.0
TIME_STEP = 4.0
ALPHA_T = 0.02
BETA_S = 0.015
T_REF = 1.0
S_REF = 1.0
VISC_KV = 0.001
DIFF_KT = 0.0005

LANES = 128
HALO = 32
PAD = 8
NEAR = 16
F32 = jnp.float32
NORTH, SOUTH, EAST, WEST = (1, 0), (-1, 0), (0, 1), (0, -1)
NORTH_EAST, NORTH_WEST, SOUTH_EAST, SOUTH_WEST = (1, 1), (1, -1), (-1, 1), (-1, -1)
COMPASS = (NORTH, SOUTH, EAST, WEST, NORTH_EAST, NORTH_WEST, SOUTH_EAST, SOUTH_WEST)
SLOT = 32
BLOCK = 16
SOLVE_ROWS = 32
SUB_ROWS = 32
UNROLL = 2
EDGE_UNROLL = 5
FLOW_UNROLL = 3
MIB = 2**20


def kernels(mesh, levels, rows, cols, n_sub):
    n_cols, n_rows = mesh.shape["col"], mesh.shape["row"]
    tiles = cols // LANES
    ring = tiles + 1
    halo_tile = tiles
    ext_rows = rows + 2 * PAD
    flat_rows = rows + 2 * HALO + 2 * PAD
    core = PAD + HALO
    top = core + rows
    body_rows = pl.ds(PAD, rows)
    own = pl.ds(core, rows)
    dt_sub = TIME_STEP / n_sub
    weight_norm = 6.0 / (n_sub * (n_sub + 1) * (n_sub + 2))

    def lane_iota(n):
        return lax.broadcasted_iota(jnp.int32, (n, LANES), 1)

    def roll(x, shift):
        return pltpu.roll(x, shift, 1)

    def east(parts):
        last = lane_iota(parts[0].shape[0]) == LANES - 1
        moved = [roll(x, LANES - 1) for x in parts]
        return [pick(last, moved[(c + 1) % ring], moved[c]) for c in range(ring)]

    def west(parts):
        first = lane_iota(parts[0].shape[0]) == 0
        moved = [roll(x, 1) for x in parts]
        return [pick(first, moved[(c - 1) % ring], moved[c]) for c in range(ring)]

    def split(ref):
        return [ref.at[f] for f in range(ref.shape[0])]

    def scaled(factor, x):
        return x if factor == 1.0 else factor * x

    def real(k):
        return float(k) if isinstance(k, int) else k.astype(F32)

    def over_levels(body, carry, unroll=UNROLL):
        def trip(i, carry):
            for j in range(unroll):
                carry = body(unroll * i + j, carry)
            return carry

        carry = lax.fori_loop(0, levels // unroll, trip, carry)
        for k in range(levels - levels % unroll, levels):
            carry = body(k, carry)
        return carry

    def pick(condition, x, other):
        if jnp.ndim(condition) == 0:
            return jnp.where(condition, x, other)
        shape = condition.shape
        x = x if jnp.ndim(x) else jnp.full(shape, x, F32)
        other = other if jnp.ndim(other) else jnp.full(shape, other, F32)
        return lax.select(condition, x, other)

    def blank():
        return jnp.zeros((rows, LANES), F32)

    def neighbour(way):
        d_row, d_col = way
        row = lax.rem(lax.axis_index("row") + (d_row + n_rows), n_rows)
        col = lax.rem(lax.axis_index("col") + (d_col + n_cols), n_cols)
        return {"row": row, "col": col}

    def remote(sems, *routes):
        sent, arrived = split(sems)
        return [
            pltpu.make_async_remote_copy(
                src_ref=src,
                dst_ref=dst,
                send_sem=sent.at[index],
                recv_sem=arrived.at[index],
                device_id=neighbour(way),
                device_id_type=pl.DeviceIdType.MESH,
            )
            for index, (src, dst, way) in enumerate(routes)
        ]

    def start_all(copies):
        for copy in copies:
            copy.start()

    def wait_all(copies):
        for copy in copies:
            copy.wait()

    def rim_pack(maps, pack_east, pack_west):
        slot = lane_iota(rows) // HALO
        last, first = blank(), blank()
        for f, ref in enumerate(maps):
            last = pick(slot == f, roll(ref[tiles - 1, own, :], (HALO * f + HALO) % LANES), last)
            first = pick(slot == f, roll(ref[0, own, :], HALO * f), first)
        pack_east[...] = last
        pack_west[...] = first

    def row_rims(main, sems, reach, skip=0):
        every, inner, n = pl.ds(0, main.shape[0]), pl.ds(0, tiles), reach - skip
        return remote(
            sems,
            (main.at[every, inner, pl.ds(top - reach, n), :], main.at[every, inner, pl.ds(core - reach, n), :], NORTH),
            (main.at[every, inner, pl.ds(core + skip, n), :], main.at[every, inner, pl.ds(top + skip, n), :], SOUTH),
        )

    def column_rims(pack_east, pack_west, from_west, from_east, sems):
        own_rows = pl.ds(HALO, rows)
        return remote(sems, (pack_east, from_west.at[own_rows, :], EAST), (pack_west, from_east.at[own_rows, :], WEST))

    def corner_rims(pack_east, pack_west, from_west, from_east, sems, reach, skip=0):
        n = reach - skip
        p_high, p_low = pl.ds(rows - reach, n), pl.ds(skip, n)
        d_low, d_high = pl.ds(HALO - reach, n), pl.ds(HALO + rows + skip, n)
        return remote(
            sems,
            (pack_east.at[p_high, :], from_west.at[d_low, :], NORTH_EAST),
            (pack_west.at[p_high, :], from_east.at[d_low, :], NORTH_WEST),
            (pack_east.at[p_low, :], from_west.at[d_high, :], SOUTH_EAST),
            (pack_west.at[p_low, :], from_east.at[d_high, :], SOUTH_WEST),
        )

    def rim_unpack(maps, from_west, from_east, start, n):
        easterly = lane_iota(n) < LANES // 2
        here = pl.ds(start - PAD, n)
        for f, ref in enumerate(maps):
            e = roll(from_east[here, :], (LANES - HALO * f) % LANES)
            w = roll(from_west[here, :], LANES - HALO - HALO * f)
            ref[halo_tile, pl.ds(start, n), :] = pick(easterly, e, w)

    def front(
        u_hbm, v_hbm, t_hbm, s_hbm, eta_hbm, tu_hbm, tv_hbm, depth_hbm, kmt_hbm, tide_hbm,
        us, vs, tm, sm, baro_out, corr, counts,
        u, v, p, gain_a, gain_b, cross, kmt_int, geo, thick, baro, force, coef, mean, depth_sum,
        pk_e, pk_w, rim_w, rim_e, cols, cols_e, cols_w, cols_in, first_row, last_row,
        row_n, row_s, corner_nw, corner_se, first_row4, last_row4, row_n4, row_s4, tide,
        load_sems, plane_sems, tide_sem, sem_near, sem_far, sem_baro, sem_uv, sem_p, sem_ts, sem_force, sem_star,
    ):
        k_map, depth_map = split(geo)
        eta_map, tu_map, tv_map = split(baro)
        dz_map, dzu_map, dzv_map = split(thick)
        k_out, ku_map, kv_map = split(counts)
        hu_map, hv_map = split(coef)
        fu_map, fv_map = split(force)
        mu_map, mv_map = split(mean)
        su_map, sv_map = split(depth_sum)
        pk_e1, pk_e2, pk_e3 = split(pk_e)
        pk_w1, pk_w2, pk_w3 = split(pk_w)
        rim_e1, rim_e2, rim_e3 = split(rim_e)
        rim_w1, rim_w2, rim_w3 = split(rim_w)
        zero = blank()
        lane = lane_iota(rows)
        low_half = lane < LANES // 2
        pair_of_lane, odd = lane // 2, lane % 2 == 1

        barrier = pltpu.get_barrier_semaphore()
        for way in COMPASS:
            pl.semaphore_signal(barrier, device_id=neighbour(way), device_id_type=pl.DeviceIdType.MESH)

        def plane_load(sems, src, dst):
            return [
                pltpu.make_async_copy(src.at[:, pl.ds(c * LANES, LANES)], dst(c), sems.at[c]) for c in range(tiles)
            ]

        def cube_tile(sems, src, dst, c):
            lanes = pl.ds(pl.multiple_of(c * LANES, LANES), LANES)
            return pltpu.make_async_copy(src.at[:, :, lanes], dst.at[c, :, body_rows, :], sems.at[c])

        def cube_load(sems, src, dst):
            return [cube_tile(sems, src, dst, c) for c in range(tiles)]

        sem_k, sem_h, sem_e, sem_tu, sem_tv = split(plane_sems)
        sem_t, sem_s, sem_u, sem_v = split(load_sems)
        geo_load = plane_load(sem_k, kmt_hbm, lambda c: kmt_int.at[c]) + plane_load(
            sem_h, depth_hbm, lambda c: depth_map.at[c, own, :]
        )
        baro_load = (
            plane_load(sem_e, eta_hbm, lambda c: eta_map.at[c, own, :])
            + plane_load(sem_tu, tu_hbm, lambda c: tu_map.at[c, own, :])
            + plane_load(sem_tv, tv_hbm, lambda c: tv_map.at[c, own, :])
        )
        tracer_load = []
        for c in range(tiles):
            tracer_load += [cube_tile(sem_t, t_hbm, tm, c), cube_tile(sem_s, s_hbm, sm, c)]
        flow_load = cube_load(sem_u, u_hbm, u) + cube_load(sem_v, v_hbm, v)
        tide_load = pltpu.make_async_copy(tide_hbm, tide, tide_sem)
        start_all(geo_load)
        start_all(tracer_load)
        start_all(flow_load)
        start_all(baro_load)
        tide_load.start()

        zero_rows = jnp.zeros((PAD, LANES), F32)
        for ref in (k_map, depth_map, dz_map, eta_map, tu_map, tv_map):
            for c in range(ring):
                ref[c, pl.ds(0, PAD), :] = zero_rows
                ref[c, pl.ds(flat_rows - PAD, PAD), :] = zero_rows
        for ref in (mu_map, mv_map):
            for c in range(ring):
                ref[c] = jnp.zeros((flat_rows, LANES), F32)

        wait_all(geo_load)
        for c in range(tiles):
            k_map[c, own, :] = kmt_int[c].astype(F32)
        rim_pack((k_map, depth_map), pk_e1, pk_w1)

        rho_s, rho_t = 0.5 * BETA_S, 0.5 * ALPHA_T
        rho_0 = rho_t * T_REF - rho_s * S_REF

        def pressure_tile(c, _):
            k_cell = k_map[c, own, :]
            scale = (TIME_STEP * GRAVITY) * (depth_map[c, own, :] / jnp.maximum(k_cell, 1.0))

            def level(k, total):
                half = (rho_s * sm[c, k, body_rows, :] - rho_t * tm[c, k, body_rows, :]) + rho_0
                half = pick(real(k) < k_cell, half, zero)
                middle = total + half
                p[c, k, body_rows, :] = scale * middle
                return middle + half

            over_levels(level, zero)
            return _


        def tracer_tile(c, _):
            k_cell = k_map[c, own, :]
            dz = depth_map[c, own, :] / jnp.maximum(k_cell, 1.0)
            safe = pick(k_cell > 0, dz, 1.0)
            couple = (TIME_STEP * DIFF_KT) / (safe * safe)

            def down(k, carry):
                lower, keep, part_t, part_s = carry
                kf = real(k)
                wet = kf < k_cell
                upper = pick(kf + 1.0 < k_cell, couple, zero)
                turn = 1.0 + lower * keep
                inv = 1.0 / (turn + upper)
                gain_a[k] = upper * inv
                part_t = (pick(wet, tm[c, k, body_rows, :], zero) + lower * part_t) * inv
                part_s = (pick(wet, sm[c, k, body_rows, :], zero) + lower * part_s) * inv
                tm[c, k, body_rows, :] = part_t
                sm[c, k, body_rows, :] = part_s
                return upper, turn * inv, part_t, part_s

            over_levels(down, (zero, zero, zero, zero))

            def up(i, carry):
                below_t, below_s = carry
                k = levels - 1 - i
                gain = gain_a[k]
                below_t = tm[c, k, body_rows, :] + gain * below_t
                below_s = sm[c, k, body_rows, :] + gain * below_s
                tm[c, k, body_rows, :] = below_t
                sm[c, k, body_rows, :] = below_s
                return below_t, below_s

            over_levels(up, (zero, zero))
            return _

        def arrived(c):
            cube_tile(sem_t, t_hbm, tm, c).wait()
            cube_tile(sem_s, s_hbm, sm, c).wait()

        def both_passes(c, done):
            arrived(c)
            pressure_tile(c, 0)
            tracer_tile(c, 0)
            return done

        def pressure_pass(c, done):
            arrived(c)
            pressure_tile(c, 0)
            return done

        lax.fori_loop(0, tiles // 2, both_passes, 0)
        lax.fori_loop(tiles // 2, tiles, pressure_pass, 0)

        pl.semaphore_wait(barrier, len(COMPASS))
        near_rows, near_cols, near_corners = split(sem_near)
        near = row_rims(geo, near_rows, NEAR)
        near += column_rims(pk_e1, pk_w1, rim_w1, rim_e1, near_cols)
        near += corner_rims(pk_e1, pk_w1, rim_w1, rim_e1, near_corners, NEAR)
        start_all(near)

        def edges(columns, top_rows, bottom_rows):
            def level(k, packed):
                row = pl.ds(k, 1)
                out = []
                for pair, acc in zip(columns, packed):
                    for f, ref in pair:
                        slot = SLOT * f + k
                        both = pick(low_half, ref[0, k, body_rows, :], ref[tiles - 1, k, body_rows, :])
                        acc = pick(pair_of_lane == slot, roll(both, 2 * slot + 1), acc)
                    out.append(acc)
                for c in range(tiles):
                    for ref, dst in top_rows:
                        dst[c, row, :] = ref[c, k, pl.ds(PAD, 1), :]
                    for ref, dst in bottom_rows:
                        dst[c, row, :] = ref[c, k, pl.ds(PAD + rows - 1, 1), :]
                return tuple(out)

            return over_levels(level, (zero,) * len(columns), EDGE_UNROLL)

        wait_all(flow_load)
        cols_uv, cols_p, cols_ts, cols_us = split(cols)
        east_uv, east_p, east_ts = split(cols_e)
        west_uv, west_ts, west_us = split(cols_w)
        fr_u, fr_v, fr_p = split(first_row)
        lr_u, lr_v = split(last_row)
        rn_u, rn_v, rn_p = split(row_n)
        rs_u, rs_v = split(row_s)
        (packed,) = edges((((0, u), (1, v)),), ((u, fr_u), (v, fr_v)), ((u, lr_u), (v, lr_v)))
        cols_uv[...] = packed
        two = pl.ds(0, 2)
        ex_uv = remote(
            sem_uv,
            (first_row.at[two], row_n.at[two], SOUTH),
            (last_row, row_s, NORTH),
            (cols_uv, east_uv, WEST),
            (cols_uv, west_uv, EAST),
            (cols_uv.at[pl.ds(0, PAD), :], corner_nw, SOUTH_EAST),
            (cols_uv.at[pl.ds(rows - PAD, PAD), :], corner_se, NORTH_WEST),
        )
        start_all(ex_uv)

        (packed,) = edges((((0, p),),), ((p, fr_p),), ())
        cols_p[...] = packed
        ex_p = remote(sem_p, (fr_p, rn_p, SOUTH), (cols_p, east_p, WEST))
        start_all(ex_p)

        wait_all(baro_load)
        rim_pack((eta_map, tu_map, tv_map), pk_e2, pk_w2)
        far_rows, far_corners = split(sem_far)
        baro_rows, baro_cols, baro_corners = split(sem_baro)
        far = row_rims(geo, far_rows, HALO, NEAR)
        far += corner_rims(pk_e1, pk_w1, rim_w1, rim_e1, far_corners, HALO, NEAR)
        far += row_rims(baro, baro_rows, HALO)
        far += column_rims(pk_e2, pk_w2, rim_w2, rim_e2, baro_cols)
        far += corner_rims(pk_e2, pk_w2, rim_w2, rim_e2, baro_corners, HALO)
        start_all(far)

        lax.fori_loop(tiles // 2, tiles, tracer_tile, 0)
        fr_t4, fr_s4 = split(first_row4)
        lr_t4, lr_s4, lr_v4 = split(last_row4)
        rn_t4, rn_s4 = split(row_n4)
        rs_t4, rs_s4, rs_v4 = split(row_s4)
        (packed,) = edges((((0, tm), (1, sm)),), ((tm, fr_t4), (sm, fr_s4)), ((tm, lr_t4), (sm, lr_s4)))
        cols_ts[...] = packed
        ex_ts = remote(
            sem_ts,
            (cols_ts, east_ts, WEST),
            (cols_ts, west_ts, EAST),
            (first_row4, row_n4, SOUTH),
            (last_row4.at[two], row_s4.at[two], NORTH),
        )
        start_all(ex_ts)

        row_index = lax.axis_index("row")

        def wall(low, n, inside):
            @pl.when(jnp.logical_not(inside))
            def _():
                for c in range(ring):
                    k_map[c, pl.ds(low, n), :] = jnp.zeros((n, LANES), F32)

        def thickness(start, n):
            here = pl.ds(start, n)
            for c in range(ring):
                dz_map[c, here, :] = depth_map[c, here, :] / jnp.maximum(k_map[c, here, :], 1.0)

        def faces(start, n):
            here, north = pl.ds(start, n), pl.ds(start + 1, n)
            k_cell = [k_map[c, here, :] for c in range(ring)]
            dz = [dz_map[c, here, :] for c in range(ring)]
            k_east, dz_east = east(k_cell), east(dz)
            for c in range(ring):
                k_u = jnp.minimum(k_cell[c], k_east[c])
                k_v = jnp.minimum(k_cell[c], k_map[c, north, :])
                dz_u = 0.5 * (dz[c] + dz_east[c])
                dz_v = 0.5 * (dz[c] + dz_map[c, north, :])
                k_out[c, here, :] = k_cell[c]
                ku_map[c, here, :] = k_u
                kv_map[c, here, :] = k_v
                dzu_map[c, here, :] = dz_u
                dzv_map[c, here, :] = dz_v
                hu_map[c, here, :] = (dt_sub * dt_sub) * (k_u * dz_u)
                hv_map[c, here, :] = (dt_sub * dt_sub) * (k_v * dz_v)

        def in_blocks(work, start, n, size=BLOCK):
            lax.fori_loop(0, n // size, lambda i, _: (work(pl.multiple_of(start + size * i, PAD), size), _)[1], 0)

        far_low, far_high, far_n = PAD, top + NEAR, HALO - NEAR
        wait_all(near)
        rim_unpack((k_map, depth_map), rim_w1, rim_e1, core - NEAR, rows + 2 * NEAR)
        wall(core - NEAR, NEAR, row_index > 0)
        wall(top, NEAR, row_index < n_rows - 1)
        in_blocks(thickness, core - NEAR, rows + 2 * NEAR)
        in_blocks(faces, core - PAD, rows + 2 * PAD)

        def mask_tile(c, _):
            for ref, count in ((u, ku_map), (v, kv_map)):
                k_face = count[c, own, :]

                def level(k, done, ref=ref, k_face=k_face):
                    ref[c, k, body_rows, :] = pick(real(k) < k_face, ref[c, k, body_rows, :], zero)
                    return done

                over_levels(level, 0)
            return _

        lax.fori_loop(0, tiles, mask_tile, 0)

        def fill(columns, norths, souths):
            def masked(x, k, count, tile, here):
                return x if count is None else pick(real(k) < count[tile, here, :], x, 0.0)

            def level(k, _):
                for ref, f, src, count in columns:
                    x = roll(src[...], LANES - 1 - 2 * (SLOT * f + k))
                    ref[halo_tile, k, body_rows, :] = masked(x, k, count, halo_tile, own)
                row = pl.ds(k, 1)
                for c in range(tiles):
                    for ref, src, count in norths:
                        x = masked(src[c, row, :], k, count, c, pl.ds(top, 1))
                        ref[c, k, pl.ds(PAD + rows, 1), :] = x
                    for ref, src, count in souths:
                        x = masked(src[c, row, :], k, count, c, pl.ds(core - 1, 1))
                        ref[c, k, pl.ds(PAD - 1, 1), :] = x
                return _

            over_levels(level, 0, EDGE_UNROLL)

        in_uv, in_ts = split(cols_in)
        wait_all(ex_uv)
        wait_all(ex_p)
        in_uv[...] = pick(odd, east_uv[...], west_uv[...])
        fill(
            ((u, 0, in_uv, ku_map), (v, 1, in_uv, kv_map), (p, 0, east_p, None)),
            ((u, rn_u, ku_map), (v, rn_v, kv_map), (p, rn_p, None)),
            ((u, rs_u, ku_map), (v, rs_v, kv_map)),
        )

        def corners(k, _):
            kf = real(k)
            x = roll(corner_nw[...], LANES - 1 - 2 * k)
            u[halo_tile, k, pl.ds(PAD + rows, PAD), :] = pick(kf < ku_map[halo_tile, pl.ds(top, PAD), :], x, 0.0)
            x = roll(corner_se[...], LANES - 1 - 2 * (SLOT + k))
            v[halo_tile, k, pl.ds(0, PAD), :] = pick(kf < kv_map[halo_tile, pl.ds(core - PAD, PAD), :], x, 0.0)
            return _

        over_levels(corners, 0, EDGE_UNROLL)

        quarter = 0.25 * TIME_STEP

        def momentum(k, _):
            tall, tall_north = pl.ds(0, PAD + rows), pl.ds(1, PAD + rows)
            here, north, south = body_rows, pl.ds(PAD + 1, rows), pl.ds(PAD - 1, rows)
            vv = [v[c, k, tall, :] for c in range(ring)]
            v_east = east(vv)
            for c in range(ring):
                cross[c, tall, :] = (vv[c] + v_east[c]) * (u[c, k, tall, :] + u[c, k, tall_north, :])
            uu = [u[c, k, here, :] for c in range(ring)]
            pp = [p[c, k, here, :] for c in range(ring)]
            centre = [x + y for x, y in zip(uu, west(uu))]
            centre = [scaled(quarter, x * x) + y for x, y in zip(centre, pp)]
            centre_east = east(centre)
            xx = [cross[c, here, :] for c in range(ring)]
            x_west = west(xx)
            for c in range(tiles):
                us[c, k, here, :] = uu[c] - (
                    (centre_east[c] - centre[c]) + scaled(quarter, xx[c] - cross[c, south, :])
                )
                vv = v[c, k, here, :]
                b_here = vv + v[c, k, north, :]
                b_south = vv + v[c, k, south, :]
                push = (b_here * b_here - b_south * b_south) + (xx[c] - x_west[c])
                vs[c, k, here, :] = vv - (scaled(quarter, push) + (p[c, k, north, :] - pp[c]))
            return _

        over_levels(momentum, 0, FLOW_UNROLL)

        nil = jnp.zeros((SOLVE_ROWS, LANES), F32)
        parts = rows // SOLVE_ROWS

        def solve_part(c, i):
            r = pl.multiple_of(i * SOLVE_ROWS, PAD)
            flat, here = pl.ds(core + r, SOLVE_ROWS), pl.ds(PAD + r, SOLVE_ROWS)
            faces = []
            for count, dz in ((ku_map, dzu_map), (kv_map, dzv_map)):
                k_face = count[c, flat, :]
                safe = pick(k_face > 0, dz[c, flat, :], 1.0)
                faces.append((k_face, (TIME_STEP * VISC_KV) / (safe * safe)))

            def down(k, carry):
                kf = real(k)
                out = []
                for face, ref, gain, state in zip(faces, (us, vs), (gain_a, gain_b), carry):
                    k_face, couple = face
                    lower, keep, part = state
                    upper = pick(kf + 1.0 < k_face, couple, nil)
                    turn = 1.0 + lower * keep
                    inv = 1.0 / (turn + upper)
                    gain[k, pl.ds(0, SOLVE_ROWS), :] = upper * inv
                    part = (pick(kf < k_face, ref[c, k, here, :], nil) + lower * part) * inv
                    ref[c, k, here, :] = part
                    out.append((upper, turn * inv, part))
                return tuple(out)

            over_levels(down, ((nil,) * 3,) * 2)

            def up(j, carry):
                k = levels - 1 - j
                out = []
                for ref, old, gain, state in zip((us, vs), (u, v), (gain_a, gain_b), carry):
                    below, total, change = state
                    below = ref[c, k, here, :] + gain[k, pl.ds(0, SOLVE_ROWS), :] * below
                    ref[c, k, here, :] = below
                    out.append((below, total + below, change + (below - old[c, k, here, :])))
                return tuple(out)

            sums = over_levels(up, ((nil,) * 3,) * 2)
            for dz, total_map, force_map, state in zip((dzu_map, dzv_map), (su_map, sv_map), (fu_map, fv_map), sums):
                _, total, change = state
                total_map[c, flat, :] = dz[c, flat, :] * total
                force_map[c, flat, :] = dz[c, flat, :] * change * (1.0 / TIME_STEP)

        force_rows, force_cols, force_corners = split(sem_force)
        low, high, both = pl.ds(core, HALO), pl.ds(top - HALO, HALO), pl.ds(0, 2)

        def solve_tiles(first, step):
            def work(i, done):
                solve_part(first + step * (i // parts), i % parts)
                return done

            lax.fori_loop(0, 2 * parts, work, 0)
            sent = []
            for c in (first, first + step):
                sent += remote(
                    force_rows.at[both, pl.ds(2 * c, 2)],
                    (force.at[both, c, high, :], force.at[both, c, pl.ds(PAD, HALO), :], NORTH),
                    (force.at[both, c, low, :], force.at[both, c, pl.ds(top, HALO), :], SOUTH),
                )
            return sent

        ex3 = solve_tiles(0, tiles - 1)
        rim_pack((fu_map, fv_map), pk_e3, pk_w3)
        ex3 += column_rims(pk_e3, pk_w3, rim_w3, rim_e3, force_cols)
        ex3 += corner_rims(pk_e3, pk_w3, rim_w3, rim_e3, force_corners, HALO)
        start_all(ex3)
        late = solve_tiles(1, 1)
        start_all(late)
        ex3 += late

        (packed,) = edges((((0, us),),), (), ((vs, lr_v4),))
        cols_us[...] = pick(pair_of_lane == levels, roll(su_map[tiles - 1, own, :], 2 * levels + 1), packed)
        for c in range(tiles):
            lr_v4[c, pl.ds(levels, 1), :] = sv_map[c, pl.ds(top - 1, 1), :]
        ex_star = remote(sem_star, (cols_us, west_us, EAST), (lr_v4, rs_v4, NORTH))
        start_all(ex_star)

        wait_all(ex_ts)
        in_ts[...] = pick(odd, east_ts[...], west_ts[...])
        fill(
            ((tm, 0, in_ts, None), (sm, 1, in_ts, None)),
            ((tm, rn_t4, None), (sm, rn_s4, None)),
            ((tm, rs_t4, None), (sm, rs_s4, None)),
        )

        wait_all(far)
        for start in (far_low, far_high):
            rim_unpack((k_map, depth_map), rim_w1, rim_e1, start, far_n)
        wall(far_low, far_n, row_index > 0)
        wall(far_high, far_n, row_index < n_rows - 1)
        in_blocks(thickness, far_low, far_n, PAD)
        in_blocks(thickness, far_high, far_n, PAD)
        in_blocks(faces, PAD, HALO - PAD, PAD)
        in_blocks(faces, top + PAD, HALO - PAD, PAD)
        full_n = rows + 2 * HALO
        rim_unpack((eta_map, tu_map, tv_map), rim_w2, rim_e2, PAD, full_n)

        def start_fields(start, n):
            here = pl.ds(start, n)
            for ref, count, unit in ((eta_map, k_out, 1.0), (tu_map, ku_map, dt_sub), (tv_map, kv_map, dt_sub)):
                for c in range(ring):
                    ref[c, here, :] = pick(count[c, here, :] > 0, scaled(unit, ref[c, here, :]), 0.0)

        in_blocks(start_fields, PAD, full_n)
        tide_load.wait()

        wait_all(ex3)
        rim_unpack((fu_map, fv_map), rim_w3, rim_e3, PAD, full_n)

        def force_fields(start, n):
            here = pl.ds(start, n)
            for ref, count in ((fu_map, ku_map), (fv_map, kv_map)):
                for c in range(ring):
                    ref[c, here, :] = pick(count[c, here, :] > 0, (dt_sub * dt_sub) * ref[c, here, :], 0.0)

        in_blocks(force_fields, PAD, full_n)

        def subcycle(low, high):
            chunks = [(r, min(SUB_ROWS, high - r)) for r in range(low, high, SUB_ROWS)]

            def body(n, _):
                tide_u, tide_v = tide[0, n], tide[1, n]
                weight = (weight_norm / dt_sub) * ((n + 1) * (n_sub - n)).astype(F32)
                for r, n_r in chunks:
                    here, south = pl.ds(r, n_r), pl.ds(r - 1, n_r)
                    tu = [tu_map[c, here, :] for c in range(ring)]
                    tu_west = west(tu)
                    for c in range(ring):
                        spread = (tu[c] - tu_west[c]) + (tv_map[c, here, :] - tv_map[c, south, :])
                        eta_map[c, here, :] = eta_map[c, here, :] - spread
                for r, n_r in chunks:
                    here, north = pl.ds(r, n_r), pl.ds(r + 1, n_r)
                    eta = [eta_map[c, here, :] for c in range(ring)]
                    eta_east = east(eta)
                    averaged = r + n_r > core - 1 and r < top
                    for c in range(ring):
                        drive = hu_map[c, here, :] * (tide_u - scaled(GRAVITY, eta_east[c] - eta[c]))
                        tu = tu_map[c, here, :] + (drive + fu_map[c, here, :])
                        tu_map[c, here, :] = tu
                        drive = hv_map[c, here, :] * (tide_v - scaled(GRAVITY, eta_map[c, north, :] - eta[c]))
                        tv = tv_map[c, here, :] + (drive + fv_map[c, here, :])
                        tv_map[c, here, :] = tv
                        if averaged:
                            mu_map[c, here, :] = mu_map[c, here, :] + weight * tu
                            if c < tiles:
                                mv_map[c, here, :] = mv_map[c, here, :] + weight * tv
                return _

            return body

        begin, margin = 0, 0
        while begin < n_sub:
            end = n_sub if margin + PAD >= HALO else min(n_sub, n_sub - (HALO - margin - PAD))
            if end > begin:
                lax.fori_loop(begin, end, subcycle(PAD + margin, flat_rows - PAD - margin), 0)
                begin = end
            margin += PAD

        for ref, out, unit in zip((eta_map, tu_map, tv_map), split(baro_out), (1.0, 1.0 / dt_sub, 1.0 / dt_sub)):
            for c in range(tiles):
                out[c] = scaled(unit, ref[c, own, :])

        wait_all(ex_star)
        fill(((us, 0, west_us, None),), (), ((vs, rs_v4, None),))
        su_map[halo_tile, own, :] = roll(west_us[...], LANES - 1 - 2 * levels)
        for c in range(tiles):
            sv_map[c, pl.ds(core - 1, 1), :] = rs_v4[c, pl.ds(levels, 1), :]
        cu_map, cv_map = split(corr)
        for out, mean_map, total_map, count, dz, n, here in (
            (cu_map, mu_map, su_map, ku_map, dzu_map, ring, own),
            (cv_map, mv_map, sv_map, kv_map, dzv_map, tiles, pl.ds(core - PAD, rows + PAD)),
        ):
            for c in range(n):
                depth = count[c, here, :] * dz[c, here, :]
                safe = pick(depth > 0, depth, 1.0)
                out[c, here, :] = (mean_map[c, here, :] - total_map[c, here, :]) / safe

    group = 4

    def back(us, vs, tm, sm, baro_in, corr, counts, eta_o, tu_o, tv_o, u_o, v_o, t_o, s_o, flux):
        k_map, ku_map, kv_map = split(counts)
        cu_map, cv_map = split(corr)
        fluxes = split(flux)
        for ref, out in zip(split(baro_in), (eta_o, tu_o, tv_o)):
            for c in range(tiles):
                out[:, pl.ds(c * LANES, LANES)] = ref[c]
        half = 0.5 * TIME_STEP

        def level(i, _):
            k = pl.program_id(0) * group + i
            kf = k.astype(F32)
            for r in range(0, PAD + rows, PAD):
                here, north = pl.ds(r, PAD), pl.ds(r + 1, PAD)
                flat = pl.ds(r + core - PAD, PAD)
                for c in range(tiles):
                    vv = pick(kf < kv_map[c, flat, :], vs[c, k, here, :] + cv_map[c, flat, :], 0.0)
                    if r >= PAD:
                        v_o[i, pl.ds(r - PAD, PAD), pl.ds(c * LANES, LANES)] = vv
                    vv = half * vv
                    for ref, store in zip((tm, sm), fluxes):
                        store[c, here, :] = vv * (ref[c, k, here, :] + ref[c, k, north, :])
            here, south, flat = body_rows, pl.ds(PAD - 1, rows), own
            tracers = [[ref[c, k, here, :] for c in range(ring)] for ref in (tm, sm)]
            easts = [east(x) for x in tracers]
            uu = []
            for c in range(ring):
                x = pick(kf < ku_map[c, flat, :], us[c, k, here, :] + cu_map[c, flat, :], 0.0)
                if c < tiles:
                    u_o[i, :, pl.ds(c * LANES, LANES)] = x
                uu.append(half * x)
            fluxes_x = [[x * (y + z) for x, y, z in zip(uu, own_t, east_t)] for own_t, east_t in zip(tracers, easts)]
            wests = [west(x) for x in fluxes_x]
            for own_t, fx, fx_west, store, out in zip(tracers, fluxes_x, wests, fluxes, (t_o, s_o)):
                for c in range(tiles):
                    spread = (fx[c] - fx_west[c]) + (store[c, here, :] - store[c, south, :])
                    out[i, :, pl.ds(c * LANES, LANES)] = pick(kf < k_map[c, flat, :], own_t[c] - spread, 0.0)
            return _

        left = jnp.minimum(group, levels - pl.program_id(0) * group)
        lax.fori_loop(0, left, level, 0)

    vmem = lambda *shape: pltpu.VMEM(shape, F32)
    flat = lambda n: vmem(n, ring, flat_rows, LANES)
    line = lambda n: vmem(n, tiles, SLOT, LANES)
    cube_buf = vmem(ring, levels, ext_rows, LANES)
    gain_buf = vmem(levels, rows, LANES)
    pack_buf = vmem(3, rows, LANES)
    rim_buf = vmem(3, rows + 2 * HALO, LANES)
    col_buf, corner_buf = vmem(rows, LANES), vmem(PAD, LANES)
    dma = lambda *shape: pltpu.SemaphoreType.DMA(shape)
    shared = [cube_buf, vmem(tiles, levels, ext_rows, LANES), cube_buf, cube_buf, vmem(3, tiles, rows, LANES), flat(2), flat(3)]
    routes = 6
    any_spec = pl.BlockSpec(memory_space=pl.ANY)
    vmem_spec = pl.BlockSpec(memory_space=pltpu.VMEM)
    front_call = pl.pallas_call(
        front,
        name="front",
        out_shape=shared,
        in_specs=[any_spec] * 10,
        out_specs=[vmem_spec] * len(shared),
        scratch_shapes=[
            cube_buf, cube_buf, cube_buf, gain_buf, vmem(levels, SOLVE_ROWS, LANES),
            vmem(ring, ext_rows, LANES), pltpu.VMEM((tiles, rows, LANES), jnp.int32),
            flat(2), flat(3), flat(3), flat(2), flat(2), flat(2), flat(2),
            pack_buf, pack_buf, rim_buf, rim_buf,
            vmem(4, rows, LANES), pack_buf, pack_buf, vmem(2, rows, LANES), line(3), line(2),
            line(3), line(2), corner_buf, corner_buf, line(2), line(3), line(2), line(3),
            pltpu.SMEM((2, n_sub), F32),
            dma(4, tiles), dma(5, tiles), pltpu.SemaphoreType.DMA,
            dma(3, 2, 4), dma(2, 2, 4), dma(3, 2, 4), dma(2, routes), dma(2, 2), dma(2, 4), dma(3, 2, 2 * tiles), dma(2, 2),
        ],
        compiler_params=pltpu.CompilerParams(
            collective_id=0, has_side_effects=True, vmem_limit_bytes=32 * MIB
        ),
    )
    plane_out = pl.BlockSpec((rows, cols), lambda i: (0, 0))
    cube_out = pl.BlockSpec((group, rows, cols), lambda i: (i, 0, 0))
    plane_shape = jax.ShapeDtypeStruct((rows, cols), F32)
    cube_shape = jax.ShapeDtypeStruct((levels, rows, cols), F32)
    back_call = pl.pallas_call(
        back,
        name="back",
        grid=(pl.cdiv(levels, group),),
        out_shape=[plane_shape] * 3 + [cube_shape] * 4,
        in_specs=[vmem_spec] * len(shared),
        out_specs=[plane_out] * 3 + [cube_out] * 4,
        scratch_shapes=[vmem(2, tiles, ext_rows, LANES)],
        compiler_params=pltpu.CompilerParams(vmem_limit_bytes=8 * MIB),
    )
    return front_call, back_call


def solution(mesh):
    def local_step(vel_u, vel_v, temperature, salinity, sea_level, trans_u, trans_v, bathymetry, kmt_levels, tide_force):
        levels, rows, cols = vel_u.shape
        front_call, back_call = kernels(mesh, levels, rows, cols, tide_force.shape[0])
        shared = front_call(
            vel_u, vel_v, temperature, salinity, sea_level, trans_u, trans_v, bathymetry, kmt_levels, tide_force.T
        )
        return tuple(back_call(*shared))

    spec_cube = P(None, "row", "col")
    spec_plane = P("row", "col")
    return jax.shard_map(
        local_step,
        mesh=mesh,
        in_specs=(spec_cube,) * 4 + (spec_plane,) * 5 + (P(None, None),),
        out_specs=(spec_plane,) * 3 + (spec_cube,) * 4,
        check_vma=False,
    )
```
